32 devices in a mesh: freq: 4 (over y, core), mesh: 8 (over z, x).
Axes of the slice: x: 2, y: 2, z: 4, core: 2. Of those that a mesh axis runs over, the one named last changes fastest.
Arguments:
- spectrum: float32 [2, 216, 32768], P(None, 'freq', 'mesh'), may hold values from -84 to 84
- time_weights: float32 [2, 432], P(None, 'freq'), may hold values from -0.625 to 0.625
- interp_weights: float32 [1024, 128, 128], P('mesh'), may hold values from -0.5 to 0.5
- group_block: int32 [1024], P('mesh'), may hold values from 0 to 255, as said below
- group_count: int32 [8], P('mesh'), may hold values from 64 to 128, as said below
- wave_state: float32 [4, 2, 524288], P('freq', None, 'mesh'), may hold values from -6 to 6
- neighbors: int32 [4, 4096], P(None, 'mesh'), may hold values from 0 to 575, as said below
- coupling: float32 [4, 524288], P(None, 'mesh'), may hold values from 0.02 to 0.2
Outputs:
- series: float32 [432, 32768], P('freq', 'mesh')
- new_state: float32 [4, 2, 524288], P('freq', None, 'mesh')
The draws below stay inside these ranges and needn't reach their ends.
Inputs may be any that keep to these rules, and one draw needn't show every extreme that they name: `group_block`: partition o owns blocks o * 32 to o * 32 + 31. Of one partition's 128 groups at most 16 name blocks of one owner, and each partition has an owner named by exactly 16 of its live groups. The live groups of partition m are its first group_count[m]; some partition has exactly 128. `neighbors`: for the cell row with local row index u, a value e names local row e - 32 of the row's own partition when it lies in 32 .. (69632) // 128 - 1, else a row of the neighbouring partition below or above; never the row itself.
All inputs are finite; a program needn't handle non-finite values.
Results may differ from the reference program's by a relative error of at most 0.0001.
Values sent between devices are 32-bit elements; how exact they have to be, the bound alone decides.
A program may use at most 64 MiB of HBM per device.

```python
import math
import jax
import jax.numpy as jnp
from jax import lax

NF = 216
NT = 432
BS = 128
B_DEV = 32
NB = 256
NP = 32768
FG_MAX = 128
GROUPS = 1024
C_DEV = 65536
CELLS = 524288
LANES = 128
HB = 4096
NEIGH = 4
WINDOWS = 4
N_FREQ = 4
N_MESH = 8


def group_plan(base_key):
    count_key = jax.random.fold_in(base_key, 7)
    heaviest = jax.random.randint(jax.random.fold_in(count_key, 1), (), 0, N_MESH)
    lighter = jax.random.randint(jax.random.fold_in(count_key, 2), (N_MESH,), FG_MAX // 2, FG_MAX + 1)
    partitions = jnp.arange(N_MESH, dtype=jnp.int32)
    counts = jnp.where(partitions == heaviest, FG_MAX, lighter).astype(jnp.int32)
    capacity = max(2, FG_MAX // N_MESH)

    def one_partition(partition, live_count):
        partition_key = jax.random.fold_in(base_key, 1000 + partition)
        leading = jax.random.randint(jax.random.fold_in(partition_key, 1), (), 0, N_MESH).astype(jnp.int32)
        others = jax.random.permutation(jax.random.fold_in(partition_key, 2), (N_MESH - 1) * capacity) // capacity
        others = jnp.where(others >= leading, others + 1, others).astype(jnp.int32)
        owners = jnp.concatenate([jnp.full((capacity,), leading, jnp.int32), others])[:FG_MAX]
        positions = jnp.arange(FG_MAX, dtype=jnp.int32)
        ranking = jax.random.permutation(jax.random.fold_in(partition_key, 3), FG_MAX).astype(jnp.int32)
        scores = jnp.where(positions < live_count, ranking, FG_MAX + positions)
        ordering = jnp.argsort(scores, stable=True)
        owners = owners[ordering]
        inside = jax.random.randint(jax.random.fold_in(partition_key, 4), (FG_MAX,), 0, B_DEV)
        return (owners * B_DEV + inside).astype(jnp.int32)
    blocks = jax.vmap(one_partition)(partitions, counts)
    return (blocks.reshape(N_MESH * FG_MAX), counts)


def draw_group_block(key, part):
    return group_plan(key)[0]


def draw_group_count(key, part):
    return group_plan(key)[1]


def draw_neighbors(key, part):
    halo_rows = HB // LANES
    rows_local = C_DEV // LANES
    local_rows = jnp.arange(CELLS // LANES, dtype=jnp.int32) % rows_local
    offsets = jax.random.randint(jax.random.fold_in(key, 21), (NEIGH, CELLS // LANES), -halo_rows, halo_rows)
    offsets = jnp.where(offsets >= 0, offsets + 1, offsets)
    return (halo_rows + local_rows[None, :] + offsets).astype(jnp.int32)


def block_scale(key, shape, pieces, smallest, largest):
    gain, own = 1.0, jax.random.fold_in(key, 6)
    for dim, parts in pieces:
        heights = jnp.exp(jax.random.uniform(jax.random.fold_in(own, dim), (parts,), jnp.float32, smallest / len(pieces), largest / len(pieces)))
        gain = gain * jnp.repeat(heights, shape[dim] // parts).reshape([-1 if axis == dim else 1 for axis in range(len(shape))])
    return gain


def normal_values(own_key, extent, scale, bound, cuts=(), kind=jnp.bfloat16):
    result = scale * jax.random.normal(own_key, extent, jnp.float32)
    if cuts:
        result = result * block_scale(own_key, extent, cuts, -0.22, 0.18)
    return jnp.clip(result, -bound, bound).astype(kind)


def setup_inputs(seed: int = 0) -> dict:
    seeds = jax.random.split(jax.random.key(seed), 9)
    spectrum = normal_values(seeds[0], (2, NF, NP), 14.0, 84.0, ((1, 4), (2, 8)), jnp.float32)
    time_weights = normal_values(seeds[1], (2, NT), (NT // N_FREQ) ** -0.5, 0.625, ((1, 4),), jnp.float32)
    interp_weights = normal_values(seeds[2], (GROUPS, BS, BS), BS ** -0.5, 0.5, ((0, 8),), jnp.float32)
    group_block = draw_group_block(jax.random.fold_in(seeds[8], 71), 0)
    group_count = draw_group_count(jax.random.fold_in(seeds[8], 71), 0)
    wave_state = normal_values(seeds[5], (WINDOWS, 2, CELLS), 1.0, 6.0, ((0, 4), (2, 8)), jnp.float32)
    neighbors = draw_neighbors(jax.random.fold_in(seeds[8], 71), 0)
    coupling = jnp.clip(jnp.exp(math.log(0.2) - 2.3025851 * jax.random.uniform(seeds[7], (NEIGH, CELLS), jnp.float32) ** block_scale(seeds[7], (NEIGH, CELLS), ((1, 8),), -0.2, 0.2)), 0.02, 0.2)
    return dict(spectrum=spectrum, time_weights=time_weights, interp_weights=interp_weights, group_block=group_block, group_count=group_count, wave_state=wave_state, neighbors=neighbors, coupling=coupling)


highest = lax.Precision.HIGHEST


def advance(previous, current, forcing, neighbors, coupling):
    halo_rows = HB // LANES
    row_count = CELLS // LANES
    rows_local = C_DEV // LANES
    cell_rows = current.reshape(row_count, LANES)
    extended = jnp.pad(cell_rows, ((halo_rows, halo_rows), (0, 0)))
    offsets = (jnp.arange(row_count, dtype=jnp.int32) // rows_local) * rows_local
    beside_all = extended[offsets[None, :] + neighbors].reshape(NEIGH, CELLS)
    spread = jnp.sum(coupling * (beside_all - current[None, :]), axis=0)
    return 2.0 * current - previous + spread + forcing


def reference(spectrum, time_weights, interp_weights, group_block, group_count, wave_state, neighbors, coupling):
    time_horizon = 2 * NF
    sample_times = jnp.arange(time_horizon, dtype=jnp.int32)
    angular_frequency = jnp.arange(NF, dtype=jnp.int32)
    phase_angles = ((sample_times[:, None] * angular_frequency[None, :]) % time_horizon).astype(jnp.float32)
    angles = phase_angles * (2.0 * math.pi / time_horizon)
    scales = jnp.where(angular_frequency == 0, 1.0, 2.0).astype(jnp.float32) / time_horizon
    basis_row_matrix = jnp.concatenate([jnp.cos(angles) * scales, -jnp.sin(angles) * scales], axis=1)
    series = jnp.dot(basis_row_matrix, spectrum.reshape(2 * NF, NP), precision=highest, preferred_element_type=jnp.float32)
    taper_window = time_horizon // N_FREQ
    live_mask = (jnp.arange(FG_MAX, dtype=jnp.int32)[None, :] < group_count[:, None]).reshape(GROUPS).astype(jnp.float32)
    blocks = series.reshape(time_horizon, NB, BS)
    states = []
    for window_index in range(N_FREQ):
        picked = blocks[window_index * taper_window:(window_index + 1) * taper_window][:, group_block, :]
        interpolated = jnp.einsum("rgp,gfp->rgf", picked, interp_weights, precision=highest)
        interpolated = interpolated * live_mask[None, :, None]
        weights_here = time_weights[:, window_index * taper_window:(window_index + 1) * taper_window]
        forcing = jnp.einsum("sr,rgf->sgf", weights_here, interpolated, precision=highest)
        forcing = forcing.reshape(2, N_MESH, FG_MAX * BS)
        forcing = jnp.pad(forcing, ((0, 0), (0, 0), (0, C_DEV - FG_MAX * BS))).reshape(2, CELLS)
        previous = wave_state[window_index, 0]
        current = wave_state[window_index, 1]
        stepped = advance(previous, current, forcing[0], neighbors, coupling)
        stepped_again = advance(current, stepped, forcing[1], neighbors, coupling)
        states.append(jnp.stack([stepped, stepped_again]))
    return series, jnp.stack(states)
```

```python
import functools
import math

import jax
import jax.numpy as jnp
import numpy as np
from jax import lax
from jax.experimental import pallas as pl
from jax.experimental.pallas import tpu as pltpu
from jax.sharding import PartitionSpec as P

LANE = 128
CORES = 2
HALO_CELLS = 4096
BLOCKS_PER_CHUNK = 4
EARLY = 2
HIGHEST = lax.Precision.HIGHEST
F32 = jnp.float32
BF16 = jnp.bfloat16


def pad8(n):
    return (n + 7) // 8 * 8


def split(x):
    high = x.astype(BF16)
    return high, (x - high.astype(F32)).astype(BF16)


def dot(a, b):
    return jnp.dot(a, b, preferred_element_type=F32)


def kernel(
    dims,
    count_smem,
    block_hbm,
    neigh_hbm,
    tw_hbm,
    basis_hbm,
    spec_hbm,
    weights_hbm,
    wave_hbm,
    coup_hbm,
    series,
    state,
    block_smem,
    neigh_smem,
    tw_own,
    basis_own,
    folded,
    own_spec,
    peer_spec,
    staged,
    lhs_high,
    lhs_low,
    cross_high,
    cross_low,
    raw,
    raw_peer,
    tw_all,
    outgoing,
    incoming,
    part,
    part_in,
    wall,
    picked,
    xt_high,
    xt_low,
    turned,
    weights,
    wave,
    coup,
    halo1,
    halo2,
    ext,
    gathered,
    spec_sem,
    swap_send,
    swap_recv,
    load_sem,
    tw_send,
    tw_recv,
    raw_send,
    raw_recv,
    pass_send,
    pass_recv,
    ser_send,
    ser_recv,
    part_send,
    part_recv,
    wall_send,
    wall_recv,
    halo_send,
    halo_recv,
):
    ny, nm, coefs, rows, chunks = dims
    groups = weights.shape[0]
    kp, rp = pad8(coefs), pad8(rows)
    m1 = ny * rp
    per = part.shape[1] // 2
    cell_rows = ext.shape[0] - 2 * halo1.shape[1] // 2
    halo = halo1.shape[1] // 2
    width = BLOCKS_PER_CHUNK * LANE
    seg = 2 * BLOCKS_PER_CHUNK

    freq = lax.axis_index("freq")
    me = lax.axis_index("mesh")
    chip, core = freq // CORES, freq % CORES
    partner = chip * CORES + (1 - core)

    def at_chip(d):
        return ((chip + d + ny) % ny) * CORES + core

    def peer(d):
        return (me + d + nm) % nm

    def remote(src, dst, send, recv, axis, target):
        return pltpu.make_async_remote_copy(
            src_ref=src,
            dst_ref=dst,
            send_sem=send,
            recv_sem=recv,
            device_id={axis: target},
            device_id_type=pl.DeviceIdType.MESH,
        )

    def load_spec(c):
        return pltpu.make_async_copy(
            spec_hbm.at[:, pl.ds(c * seg, seg), :], own_spec.at[c], spec_sem.at[c]
        )

    def swap(c):
        return remote(
            spec_hbm.at[:, pl.ds(c * seg, seg), :],
            peer_spec.at[c],
            swap_send.at[c],
            swap_recv.at[c],
            "freq",
            partner,
        )

    def send_tw(d):
        return remote(
            tw_own, tw_all.at[d - 1], tw_send.at[d - 1], tw_recv.at[d - 1], "freq", at_chip(-d)
        )

    def send_raw(d):
        return remote(
            spec_hbm.at[:, pl.ds((chunks - 1) * seg, seg), :],
            raw.at[d - 1],
            raw_send.at[d - 1],
            raw_recv.at[d - 1],
            "freq",
            at_chip(d),
        )

    def pass_raw(d):
        return remote(
            raw.at[d - 1],
            raw_peer.at[d - 1],
            pass_send.at[d - 1],
            pass_recv.at[d - 1],
            "freq",
            partner,
        )

    def send_series(d, c):
        return remote(
            outgoing.at[d - 1, c],
            incoming.at[d - 1, c],
            ser_send.at[d - 1, c],
            ser_recv.at[d - 1, c],
            "freq",
            at_chip(d),
        )

    def send_part(d):
        return remote(
            part.at[d],
            part_in.at[d - 1],
            part_send.at[d - 1],
            part_recv.at[d - 1],
            "freq",
            at_chip(d),
        )

    def send_wall(o):
        mine = pl.ds(pl.multiple_of(me * 2 * per, 8), 2 * per)
        return remote(
            wall.at[mine], wall.at[mine], wall_send.at[o - 1], wall_recv.at[o - 1], "mesh", peer(o)
        )

    def send_halo1(side):
        first = 0 if side else 2 * (cell_rows - halo)
        return remote(
            wave.at[pl.ds(first, 2 * halo)],
            halo1.at[side],
            halo_send.at[side],
            halo_recv.at[side],
            "mesh",
            peer(-1 if side else 1),
        )

    def send_halo2(side):
        first = halo if side else cell_rows
        return remote(
            ext.at[pl.ds(first, halo)],
            halo2.at[side],
            halo_send.at[2 + side],
            halo_recv.at[2 + side],
            "mesh",
            peer(-1 if side else 1),
        )

    def columns(c):
        return pl.ds(pl.multiple_of(c * width, width), width)

    load_wave = pltpu.make_async_copy(wave_hbm, wave, load_sem.at[0])
    load_coup = pltpu.make_async_copy(coup_hbm, coup, load_sem.at[1])
    load_weights = pltpu.make_async_copy(weights_hbm, weights, load_sem.at[2])

    load_tw = pltpu.make_async_copy(tw_hbm, tw_own, load_sem.at[4])
    load_basis = pltpu.make_async_copy(basis_hbm.at[freq], basis_own, load_sem.at[5])
    load_neigh = pltpu.make_async_copy(neigh_hbm, neigh_smem, load_sem.at[6])
    load_block = pltpu.make_async_copy(block_hbm, block_smem, load_sem.at[7])

    load_tw.start()
    load_basis.start()
    for c in range(chunks):
        load_spec(c).start()
    load_wave.start()
    load_neigh.start()
    load_block.start()

    barrier = pltpu.get_barrier_semaphore()
    pl.semaphore_signal(
        barrier, inc=1, device_id={"freq": partner}, device_id_type=pl.DeviceIdType.MESH
    )
    for d in range(1, ny):
        pl.semaphore_signal(
            barrier, inc=1, device_id={"freq": at_chip(d)}, device_id_type=pl.DeviceIdType.MESH
        )
    for o in range(1, nm):
        pl.semaphore_signal(
            barrier, inc=1, device_id={"mesh": peer(o)}, device_id_type=pl.DeviceIdType.MESH
        )
    pl.semaphore_wait(barrier, 1 + (ny - 1) + (nm - 1))

    swap(0).start()
    load_tw.wait()
    for d in range(1, ny):
        send_tw(d).start()
    for d in range(1, ny):
        send_raw(d).start()
    for c in range(1, chunks):
        swap(c).start()
    load_coup.start()
    load_weights.start()

    staged[...] = jnp.zeros_like(staged)
    folded[...] = jnp.zeros_like(folded)
    load_basis.wait()
    high, low = split(basis_own[0:m1, :])
    lhs_high[0:m1, :] = high
    lhs_low[0:m1, :] = low
    load_wave.wait()
    for side in range(2):
        send_halo1(side).start()

    own_rows = own_spec.reshape(chunks * coefs * seg, LANE)
    peer_rows = peer_spec.reshape(chunks * coefs * seg, LANE)

    raw_rows = raw.reshape(max(ny - 1, 1) * coefs * seg, LANE)
    raw_peer_rows = raw_peer.reshape(max(ny - 1, 1) * coefs * seg, LANE)

    def stage(sources, c):
        for p, source in enumerate(sources):
            for s in range(2):
                for j in range(BLOCKS_PER_CHUNK):
                    piece = source[pl.ds(c * (coefs * seg) + 2 * j + s, coefs, stride=seg), :]
                    base = (p * 2 + s) * kp
                    staged[base : base + coefs, j * LANE : (j + 1) * LANE] = piece
        return split(staged[...])

    def stage_chunk(c):
        load_spec(c).wait()
        swap(c).wait_recv()
        return stage((own_rows, peer_rows), c)

    def product(first, last, s_high, s_low):
        high = lhs_high[first:last, :]
        return dot(high, s_high) + dot(lhs_low[first:last, :], s_high) + dot(high, s_low)

    def keep_series(c, total):
        series[:, columns(c)] = total[0:rows]
        for d in range(1, ny):
            outgoing[d - 1, c] = total[d * rp : d * rp + rows]

    def keep_part(c, total):
        for d in range(ny):
            for s in range(2):
                row = 8 * d + s
                for j in range(BLOCKS_PER_CHUNK):
                    part[d, pl.ds(s * per + c * BLOCKS_PER_CHUNK + j, 1), :] = total[
                        row : row + 1, j * LANE : (j + 1) * LANE
                    ]

    m_all = m1 + 8 * ny
    s_high, s_low = stage_chunk(0)
    keep_series(0, product(0, m1, s_high, s_low))
    for d in range(1, ny):
        send_series(d, 0).start()
    for d in range(ny):
        if d:
            send_tw(d).wait_recv()
        tw = tw_all[d - 1] if d else tw_own[...]
        folded[8 * d : 8 * d + 2, :] = jnp.dot(
            tw,
            basis_own[d * rp : d * rp + rows, :],
            precision=HIGHEST,
            preferred_element_type=F32,
        )
    high, low = split(folded[...])
    lhs_high[m1:, :] = high
    lhs_low[m1:, :] = low
    keep_part(0, product(m1, m_all, s_high, s_low))

    def partial_chunk(c, carry):
        s_high, s_low = stage_chunk(c)
        total = product(0, m_all, s_high, s_low)
        keep_series(c, total)
        keep_part(c, total[m1:])

        @pl.when(c < EARLY)
        def _():
            for d in range(1, ny):
                send_series(d, c).start()

        return carry

    lax.fori_loop(1, chunks, partial_chunk, 0)
    for d in range(1, ny):
        send_part(d).start()

    def later(c, carry):
        for d in range(1, ny):
            send_series(d, c).start()
        return carry

    lax.fori_loop(EARLY, chunks - 1, later, 0)
    for d in range(1, ny):
        send_raw(d).wait_recv()
        pass_raw(d).start()

    wave_rows = 64

    def stage_current(b, carry):
        at = b * wave_rows
        ext[pl.ds(halo + at, wave_rows), :] = wave[pl.ds(2 * at + 1, wave_rows, stride=2), :]
        return carry

    lax.fori_loop(0, cell_rows // wave_rows, stage_current, 0)

    load_neigh.wait()
    load_block.wait()

    def gather():
        def tile(t, carry):
            for n in range(4):
                for i in range(8):
                    u = t * 8 + i
                    gathered[n, pl.ds(u, 1), :] = ext[pl.ds(neigh_smem[n, u], 1), :]
            return carry

        lax.fori_loop(0, cell_rows // 8, tile, 0)

    def spread_of(at, center):
        total = jnp.zeros((wave_rows, LANE), F32)
        for n in range(4):
            factor = coup[pl.ds(4 * at + n, wave_rows, stride=4), :]
            total += factor * (gathered[n, pl.ds(at, wave_rows), :] - center)
        return total

    inside_low = (jnp.zeros((halo, LANE), jnp.int32) + me) > 0
    inside_high = (jnp.zeros((halo, LANE), jnp.int32) + me) < nm - 1

    for side in range(2):
        send_halo1(side).wait_recv()
    ext[0:halo, :] = jnp.where(inside_low, halo1[0, pl.ds(1, halo, stride=2), :], 0.0)
    ext[halo + cell_rows :, :] = jnp.where(
        inside_high, halo1[1, pl.ds(1, halo, stride=2), :], 0.0
    )
    load_coup.wait()

    for d in range(1, ny):
        send_part(d).wait_recv()
    weighted = part[0]
    for d in range(1, ny):
        weighted += part_in[d - 1]
    wall[pl.ds(pl.multiple_of(me * 2 * per, 8), 2 * per), :] = weighted
    for o in range(1, nm):
        send_wall(o).start()

    gather()

    def first_step(b, carry):
        at = b * wave_rows
        center = ext[pl.ds(halo + at, wave_rows), :]
        previous = wave[pl.ds(2 * at, wave_rows, stride=2), :]
        state[pl.ds(2 * at, wave_rows, stride=2), :] = (
            2.0 * center - previous + spread_of(at, center)
        )
        return carry

    lax.fori_loop(0, cell_rows // wave_rows, first_step, 0)

    total = series[:, columns(chunks - 1)]
    for d in range(1, ny):
        high, low = split(basis_own[m1 + (d - 1) * rp : m1 + d * rp, :])
        cross_high[d - 1] = high
        cross_low[d - 1] = low
        pass_raw(d).wait_recv()
        s_high, s_low = stage((raw_rows, raw_peer_rows), d - 1)
        high = cross_high[d - 1]
        product_d = dot(high, s_high) + dot(cross_low[d - 1], s_high) + dot(high, s_low)
        total += product_d[0:rows]
    series[:, columns(chunks - 1)] = total

    for o in range(1, nm):
        send_wall(o).wait_recv()

    def pick(t, carry):
        for i in range(8):
            g = t * 8 + i
            block = block_smem[g]
            row = (block // per) * (2 * per) + block % per
            picked[pl.ds(g, 1), :] = wall[pl.ds(row, 1), :]
            picked[pl.ds(groups + g, 1), :] = wall[pl.ds(row + per, 1), :]
        return carry

    lax.fori_loop(0, groups // 8, pick, 0)
    high, low = split(picked[...].T)
    xt_high[0:LANE, :] = high
    xt_high[LANE:, :] = high
    xt_low[...] = low
    load_weights.wait()
    batch = 8
    lane = lax.broadcasted_iota(jnp.int32, (LANE, groups), 1)

    def interpolate(t, carry):
        block = weights[pl.ds(t * batch, batch)].reshape(batch * LANE, LANE)
        w_high, w_low = split(block)
        both = jnp.concatenate([w_high, w_low], axis=1)
        result = dot(both, xt_high[...]) + dot(w_high, xt_low[...])
        for s in range(2):
            column = turned[s]
            for i in range(batch):
                column = jnp.where(
                    lane == t * batch + i,
                    result[i * LANE : (i + 1) * LANE, s * groups : (s + 1) * groups],
                    column,
                )
            turned[s] = column
        return carry

    turned[...] = jnp.zeros_like(turned)
    lax.fori_loop(0, groups // batch, interpolate, 0)
    alive = lax.broadcasted_iota(jnp.int32, (groups, LANE), 0) < count_smem[0]
    push = [jnp.where(alive, turned[s].T, 0.0) for s in range(2)]

    top = pl.ds(0, groups, stride=2)
    state[top, :] = state[top, :] + push[0]

    def stage_stepped(b, carry):
        at = b * wave_rows
        ext[pl.ds(halo + at, wave_rows), :] = state[pl.ds(2 * at, wave_rows, stride=2), :]
        return carry

    lax.fori_loop(0, cell_rows // wave_rows, stage_stepped, 0)
    for side in range(2):
        send_halo2(side).start()
    for side in range(2):
        send_halo2(side).wait_recv()
    ext[0:halo, :] = jnp.where(inside_low, halo2[0], 0.0)
    ext[halo + cell_rows :, :] = jnp.where(inside_high, halo2[1], 0.0)
    gather()

    def second_step(b, carry):
        at = b * wave_rows
        center = ext[pl.ds(halo + at, wave_rows), :]
        previous = wave[pl.ds(2 * at + 1, wave_rows, stride=2), :]
        state[pl.ds(2 * at + 1, wave_rows, stride=2), :] = (
            2.0 * center - previous + spread_of(at, center)
        )
        return carry

    lax.fori_loop(0, cell_rows // wave_rows, second_step, 0)
    bottom = pl.ds(1, groups, stride=2)
    state[bottom, :] = state[bottom, :] + push[1]

    def finish(c, carry):
        total = series[:, columns(c)]
        for d in range(1, ny):
            send_series(d, c).wait_recv()
            total += incoming[d - 1, c]
        series[:, columns(c)] = total
        return carry

    lax.fori_loop(0, chunks - 1, finish, 0)

    def drain(c, carry):
        swap(c).wait_send()
        for d in range(1, ny):
            send_series(d, c).wait_send()
        return carry

    lax.fori_loop(0, chunks - 1, drain, 0)
    swap(chunks - 1).wait_send()
    for d in range(1, ny):
        send_raw(d).wait_send()
        pass_raw(d).wait_send()
        send_tw(d).wait_send()
        send_part(d).wait_send()
    for o in range(1, nm):
        send_wall(o).wait_send()
    for side in range(2):
        send_halo1(side).wait_send()
        send_halo2(side).wait_send()


def store(series, state, series_hbm, state_hbm, sem):
    copies = [
        pltpu.make_async_copy(series, series_hbm, sem.at[0]),
        pltpu.make_async_copy(state, state_hbm, sem.at[1]),
    ]
    for copy in copies:
        copy.start()
    for copy in copies:
        copy.wait()


def chip_basis(ny, coefs, rows, horizon):
    kp, rp = pad8(coefs), pad8(rows)
    freq = np.arange(ny * CORES).reshape(-1, 1, 1, 1, 1, 1)
    d, r, p, s, k = np.indices((2 * ny - 1, rp, CORES, 2, kp), sparse=True)
    chip, core = freq // CORES, freq % CORES
    source = chip - np.where(d < ny, 0, d - ny + 1)
    window = ((chip + np.where(d < ny, d, 0)) % ny) * CORES + core
    wave_number = (source % ny * CORES + (core + p) % CORES) * coefs + k
    angle = ((window * rows + r) * wave_number) % horizon * (2.0 * math.pi / horizon)
    scale = np.where(wave_number == 0, 1.0, 2.0) / horizon
    value = np.where(s == 0, np.cos(angle), -np.sin(angle)) * scale
    value = np.where((r < rows) & (k < coefs), value, 0.0)
    return value.reshape(ny * CORES, (2 * ny - 1) * rp, CORES * 2 * kp).astype(np.float32)


def local(
    ny,
    nm,
    spectrum,
    time_weights,
    interp_weights,
    group_block,
    group_count,
    wave_state,
    neighbors,
    coupling,
):
    coefs, points = spectrum.shape[1:]
    rows = time_weights.shape[1]
    horizon = rows * ny * CORES
    groups = interp_weights.shape[0]
    cell_rows = neighbors.shape[1]
    halo = HALO_CELLS // LANE
    blocks = points // LANE
    chunks = blocks // BLOCKS_PER_CHUNK
    kp, rp = pad8(coefs), pad8(rows)
    k_all, m_all = CORES * 2 * kp, ny * (rp + 8)
    seg = 2 * BLOCKS_PER_CHUNK
    width = BLOCKS_PER_CHUNK * LANE

    spec = spectrum.reshape(2, coefs, blocks, LANE).transpose(1, 2, 0, 3)
    spec = spec.reshape(coefs, 2 * blocks, LANE)
    wave = wave_state.reshape(2, cell_rows, LANE).transpose(1, 0, 2).reshape(2 * cell_rows, LANE)
    coup = coupling.reshape(4, cell_rows, LANE).transpose(1, 0, 2).reshape(4 * cell_rows, LANE)
    basis = jnp.asarray(chip_basis(ny, coefs, rows, horizon))

    vmem = lambda *shape: pltpu.VMEM(shape, F32)
    dma = lambda *shape: pltpu.SemaphoreType.DMA(shape)
    smem = pl.BlockSpec(memory_space=pltpu.SMEM)
    hbm = pl.BlockSpec(memory_space=pltpu.HBM)
    on_chip = pl.BlockSpec(memory_space=pltpu.VMEM)
    far = max(ny - 1, 1)
    pinned = [
        pltpu.with_memory_space_constraint(x, pltpu.HBM)
        for x in (
            group_block,
            neighbors,
            time_weights,
            basis,
            spec,
            interp_weights,
            wave,
            coup,
        )
    ]
    outs = (
        jax.ShapeDtypeStruct((rows, points), F32),
        jax.ShapeDtypeStruct((2 * cell_rows, LANE), F32),
    )
    series, state = pl.pallas_call(
        functools.partial(kernel, (ny, nm, coefs, rows, chunks)),
        out_shape=outs,
        in_specs=[smem] + [hbm] * 8,
        out_specs=(on_chip, on_chip),
        scratch_shapes=[
            pltpu.SMEM(group_block.shape, jnp.int32),
            pltpu.SMEM(neighbors.shape, jnp.int32),
            vmem(2, rows),
            vmem((2 * ny - 1) * rp, k_all),
            vmem(8 * ny, k_all),
            vmem(chunks, coefs, seg, LANE),
            vmem(chunks, coefs, seg, LANE),
            vmem(k_all, width),
            pltpu.VMEM((m_all, k_all), BF16),
            pltpu.VMEM((m_all, k_all), BF16),
            pltpu.VMEM((far, rp, k_all), BF16),
            pltpu.VMEM((far, rp, k_all), BF16),
            vmem(far, coefs, seg, LANE),
            vmem(far, coefs, seg, LANE),
            vmem(far, 2, rows),
            vmem(far, chunks, rows, width),
            vmem(far, chunks, rows, width),
            vmem(ny, 2 * blocks, LANE),
            vmem(far, 2 * blocks, LANE),
            vmem(nm * 2 * blocks, LANE),
            vmem(2 * groups, LANE),
            pltpu.VMEM((2 * LANE, 2 * groups), BF16),
            pltpu.VMEM((LANE, 2 * groups), BF16),
            vmem(2, LANE, groups),
            vmem(groups, LANE, LANE),
            vmem(2 * cell_rows, LANE),
            vmem(4 * cell_rows, LANE),
            vmem(2, 2 * halo, LANE),
            vmem(2, halo, LANE),
            vmem(cell_rows + 2 * halo, LANE),
            vmem(4, cell_rows, LANE),
            dma(chunks),
            dma(chunks),
            dma(chunks),
            dma(8),
            dma(far),
            dma(far),
            dma(far),
            dma(far),
            dma(far),
            dma(far),
            dma(far, chunks),
            dma(far, chunks),
            dma(far),
            dma(far),
            dma(max(nm - 1, 1)),
            dma(max(nm - 1, 1)),
            dma(4),
            dma(4),
        ],
        compiler_params=pltpu.CompilerParams(
            collective_id=0, has_side_effects=True, vmem_limit_bytes=40000 * 1024
        ),
        name="adjoint",
    )(group_count, *pinned)
    series, state = pl.pallas_call(
        store,
        out_shape=outs,
        in_specs=[pl.BlockSpec(memory_space=pl.ANY)] * 2,
        out_specs=(hbm, hbm),
        scratch_shapes=[dma(2)],
        compiler_params=pltpu.CompilerParams(vmem_limit_bytes=1024 * 1024),
        name="store",
    )(series, state)
    new_state = state.reshape(cell_rows, 2, LANE).transpose(1, 0, 2)
    return series, new_state.reshape(1, 2, cell_rows * LANE)


def solution(mesh):
    placed = (
        P(None, "freq", "mesh"),
        P(None, "freq"),
        P("mesh", None, None),
        P("mesh"),
        P("mesh"),
        P("freq", None, "mesh"),
        P(None, "mesh"),
        P(None, "mesh"),
    )
    ny = mesh.shape["freq"] // CORES
    return jax.shard_map(
        functools.partial(local, ny, mesh.shape["mesh"]),
        mesh=mesh,
        in_specs=placed,
        out_specs=(P("freq", "mesh"), P("freq", None, "mesh")),
        check_vma=False,
    )
```

```python
import functools
import math

import jax
import jax.numpy as jnp
import numpy as np
from jax import lax
from jax.experimental import pallas as pl
from jax.experimental.pallas import tpu as pltpu
from jax.sharding import PartitionSpec as P

LANE = 128
CORES = 2
HALO_CELLS = 4096
BLOCKS_PER_CHUNK = 4
EARLY = 2
HIGHEST = lax.Precision.HIGHEST
F32 = jnp.float32
BF16 = jnp.bfloat16


def pad8(n):
    return (n + 7) // 8 * 8


def split(x):
    high = x.astype(BF16)
    return high, (x - high.astype(F32)).astype(BF16)


def dot(a, b):
    return jnp.dot(a, b, preferred_element_type=F32)


def kernel(
    dims,
    count_smem,
    block_hbm,
    neigh_hbm,
    tw_hbm,
    basis_hbm,
    spec_hbm,
    weights_hbm,
    wave_hbm,
    coup_hbm,
    series,
    state,
    block_smem,
    neigh_smem,
    tw_own,
    basis_own,
    folded,
    own_spec,
    peer_spec,
    staged,
    lhs_high,
    lhs_low,
    cross_high,
    cross_low,
    raw,
    raw_peer,
    tw_all,
    outgoing,
    incoming,
    part,
    part_in,
    wall,
    picked,
    xt_high,
    xt_low,
    turned,
    weights,
    wave,
    coup,
    halo1,
    halo2,
    ext,
    gathered,
    spec_sem,
    swap_send,
    swap_recv,
    load_sem,
    tw_send,
    tw_recv,
    raw_send,
    raw_recv,
    pass_send,
    pass_recv,
    ser_send,
    ser_recv,
    part_send,
    part_recv,
    wall_send,
    wall_recv,
    halo_send,
    halo_recv,
    go,
    seen,
    peers_in,
    all_in,
):
    ny, nm, coefs, rows, chunks = dims
    groups = weights.shape[0]
    kp, rp = pad8(coefs), pad8(rows)
    m1 = ny * rp
    per = part.shape[1] // 2
    cell_rows = ext.shape[0] - 2 * halo1.shape[1] // 2
    halo = halo1.shape[1] // 2
    width = BLOCKS_PER_CHUNK * LANE
    seg = 2 * BLOCKS_PER_CHUNK

    freq = lax.axis_index("freq")
    me = lax.axis_index("mesh")
    chip, core = freq // CORES, freq % CORES
    partner = chip * CORES + (1 - core)

    def at_chip(d):
        return ((chip + d + ny) % ny) * CORES + core

    def peer(d):
        return (me + d + nm) % nm

    def remote(src, dst, send, recv, axis, target):
        return pltpu.make_async_remote_copy(
            src_ref=src,
            dst_ref=dst,
            send_sem=send,
            recv_sem=recv,
            device_id={axis: target},
            device_id_type=pl.DeviceIdType.MESH,
        )

    def load_spec(c):
        return pltpu.make_async_copy(
            spec_hbm.at[:, pl.ds(c * seg, seg), :], own_spec.at[c], spec_sem.at[c]
        )

    def swap(c):
        return remote(
            spec_hbm.at[:, pl.ds(c * seg, seg), :],
            peer_spec.at[c],
            swap_send.at[c],
            swap_recv.at[c],
            "freq",
            partner,
        )

    def send_tw(d):
        return remote(
            tw_own, tw_all.at[d - 1], tw_send.at[d - 1], tw_recv.at[d - 1], "freq", at_chip(-d)
        )

    def send_raw(d):
        return remote(
            own_spec.at[chunks - 1],
            raw.at[d - 1],
            raw_send.at[d - 1],
            raw_recv.at[d - 1],
            "freq",
            at_chip(d),
        )

    def pass_raw(d):
        return remote(
            raw.at[d - 1],
            raw_peer.at[d - 1],
            pass_send.at[d - 1],
            pass_recv.at[d - 1],
            "freq",
            partner,
        )

    def send_series(d, c):
        return remote(
            outgoing.at[d - 1, c],
            incoming.at[d - 1, c],
            ser_send.at[d - 1, c],
            ser_recv.at[d - 1, c],
            "freq",
            at_chip(d),
        )

    def send_part(d):
        return remote(
            part.at[d],
            part_in.at[d - 1],
            part_send.at[d - 1],
            part_recv.at[d - 1],
            "freq",
            at_chip(d),
        )

    def send_wall(o):
        mine = pl.ds(pl.multiple_of(me * 2 * per, 8), 2 * per)
        return remote(
            wall.at[mine], wall.at[mine], wall_send.at[o - 1], wall_recv.at[o - 1], "mesh", peer(o)
        )

    def send_halo1(side):
        first = 0 if side else 2 * (cell_rows - halo)
        return remote(
            wave.at[pl.ds(first, 2 * halo)],
            halo1.at[side],
            halo_send.at[side],
            halo_recv.at[side],
            "mesh",
            peer(-1 if side else 1),
        )

    def send_halo2(side):
        first = halo if side else cell_rows
        return remote(
            ext.at[pl.ds(first, halo)],
            halo2.at[side],
            halo_send.at[2 + side],
            halo_recv.at[2 + side],
            "mesh",
            peer(-1 if side else 1),
        )

    inside = (me > 0, me < nm - 1)

    def halo_each(copy, method):
        for side in range(2):
            there = inside[side] if method == "wait_recv" else inside[1 - side]
            pl.when(there)(getattr(copy(side), method))

    def columns(c):
        return pl.ds(pl.multiple_of(c * width, width), width)

    load_wave = pltpu.make_async_copy(wave_hbm, wave, load_sem.at[0])
    load_coup = pltpu.make_async_copy(coup_hbm, coup, load_sem.at[1])
    load_weights = pltpu.make_async_copy(weights_hbm, weights, load_sem.at[2])

    load_tw = pltpu.make_async_copy(tw_hbm, tw_own, load_sem.at[4])
    load_basis = pltpu.make_async_copy(basis_hbm.at[freq], basis_own, load_sem.at[5])
    load_neigh = pltpu.make_async_copy(neigh_hbm, neigh_smem, load_sem.at[6])
    load_block = pltpu.make_async_copy(block_hbm, block_smem, load_sem.at[7])

    load_tw.start()
    load_basis.start()
    for c in (chunks - 1, *range(chunks - 1)):
        load_spec(c).start()
    load_wave.start()
    load_neigh.start()
    load_block.start()

    barrier = pltpu.get_barrier_semaphore()
    first_core, first_chip = core == 0, chip == 0
    other_core, other_chip = core == 1, chip != 0

    def signal(sem, axis, target):
        pl.semaphore_signal(
            sem, inc=1, device_id={axis: target}, device_id_type=pl.DeviceIdType.MESH
        )

    @pl.when(first_core)
    def _():
        for d in range(1, ny):
            signal(barrier, "freq", at_chip(d))

    @pl.when(first_core == other_chip)
    def _():
        signal(barrier, "freq", partner)

    @pl.when(first_core & first_chip)
    def _():
        pl.semaphore_wait(barrier, ny)
        signal(go, "freq", partner)

    @pl.when(first_core & other_chip)
    def _():
        pl.semaphore_wait(barrier, ny - 1)

    @pl.when(other_core & other_chip)
    def _():
        pl.semaphore_wait(barrier, 1)
        signal(go, "freq", partner)

    load_tw.wait()
    load_spec(chunks - 1).wait()

    def send_first():
        for d in range(1, ny):
            send_tw(d).start()
            send_raw(d).start()

    pl.when(first_core)(send_first)

    @pl.when(first_core == other_chip)
    def _():
        pl.semaphore_wait(go, 1)

    for c in range(chunks):
        swap(c).start()

    @pl.when(first_core)
    def _():
        for d in range(1, ny):
            signal(seen.at[d - 1], "freq", at_chip(d))
        for d in range(1, ny):
            pl.semaphore_wait(seen.at[d - 1], 1)
        signal(peers_in, "freq", partner)

    @pl.when(other_core)
    def _():
        pl.semaphore_wait(peers_in, 1)
        send_first()

    @pl.when(other_core & first_chip)
    def _():
        for o in range(1, nm):
            signal(barrier, "mesh", peer(o))

    load_coup.start()
    load_weights.start()

    staged[...] = jnp.zeros_like(staged)
    folded[...] = jnp.zeros_like(folded)
    load_basis.wait()
    high, low = split(basis_own[0:m1, :])
    lhs_high[0:m1, :] = high
    lhs_low[0:m1, :] = low

    own_rows = own_spec.reshape(chunks * coefs * seg, LANE)
    peer_rows = peer_spec.reshape(chunks * coefs * seg, LANE)

    raw_rows = raw.reshape(max(ny - 1, 1) * coefs * seg, LANE)
    raw_peer_rows = raw_peer.reshape(max(ny - 1, 1) * coefs * seg, LANE)

    def stage(sources, c):
        for p, source in enumerate(sources):
            for s in range(2):
                for j in range(BLOCKS_PER_CHUNK):
                    piece = source[pl.ds(c * (coefs * seg) + 2 * j + s, coefs, stride=seg), :]
                    base = (p * 2 + s) * kp
                    staged[base : base + coefs, j * LANE : (j + 1) * LANE] = piece
        return split(staged[...])

    def stage_chunk(c):
        @pl.when(c < chunks - 1)
        def _():
            load_spec(c).wait()

        swap(c).wait_recv()
        return stage((own_rows, peer_rows), c)

    def product(first, last, s_high, s_low):
        high = lhs_high[first:last, :]
        return dot(high, s_high) + dot(lhs_low[first:last, :], s_high) + dot(high, s_low)

    def keep_series(c, total):
        series[:, columns(c)] = total[0:rows]
        for d in range(1, ny):
            outgoing[d - 1, c] = total[d * rp : d * rp + rows]

    def keep_part(c, total):
        for d in range(ny):
            for s in range(2):
                row = 8 * d + s
                for j in range(BLOCKS_PER_CHUNK):
                    part[d, pl.ds(s * per + c * BLOCKS_PER_CHUNK + j, 1), :] = total[
                        row : row + 1, j * LANE : (j + 1) * LANE
                    ]

    m_all = m1 + 8 * ny
    s_high, s_low = stage_chunk(0)
    keep_series(0, product(0, m1, s_high, s_low))
    for d in range(1, ny):
        send_series(d, 0).start()
    for d in range(ny):
        if d:
            send_tw(d).wait_recv()
        tw = tw_all[d - 1] if d else tw_own[...]
        folded[8 * d : 8 * d + 2, :] = jnp.dot(
            tw,
            basis_own[d * rp : d * rp + rows, :],
            precision=HIGHEST,
            preferred_element_type=F32,
        )
    high, low = split(folded[...])
    lhs_high[m1:, :] = high
    lhs_low[m1:, :] = low
    keep_part(0, product(m1, m_all, s_high, s_low))

    def partial_chunk(c, carry):
        s_high, s_low = stage_chunk(c)
        total = product(0, m_all, s_high, s_low)
        keep_series(c, total)
        keep_part(c, total[m1:])

        @pl.when(c < EARLY)
        def _():
            for d in range(1, ny):
                send_series(d, c).start()

        return carry

    lax.fori_loop(1, chunks, partial_chunk, 0)
    for d in range(1, ny):
        send_part(d).start()

    def later(c, carry):
        for d in range(1, ny):
            send_series(d, c).start()
        return carry

    lax.fori_loop(EARLY, chunks - 1, later, 0)

    @pl.when(other_core & first_chip)
    def _():
        pl.semaphore_wait(barrier, nm - 1)
        for d in range(ny):
            signal(all_in, "freq", d * CORES)
            if d:
                signal(all_in, "freq", d * CORES + 1)

    @pl.when(first_core | other_chip)
    def _():
        pl.semaphore_wait(all_in, 1)

    load_wave.wait()
    halo_each(send_halo1, "start")
    for d in range(1, ny):
        send_raw(d).wait_recv()
        pass_raw(d).start()

    wave_rows = 64

    def stage_current(b, carry):
        at = b * wave_rows
        ext[pl.ds(halo + at, wave_rows), :] = wave[pl.ds(2 * at + 1, wave_rows, stride=2), :]
        return carry

    lax.fori_loop(0, cell_rows // wave_rows, stage_current, 0)

    load_neigh.wait()
    load_block.wait()

    def gather():
        def tile(t, carry):
            for n in range(4):
                for i in range(8):
                    u = t * 8 + i
                    gathered[n, pl.ds(u, 1), :] = ext[pl.ds(neigh_smem[n, u], 1), :]
            return carry

        lax.fori_loop(0, cell_rows // 8, tile, 0)

    def spread_of(at, center):
        total = jnp.zeros((wave_rows, LANE), F32)
        for n in range(4):
            factor = coup[pl.ds(4 * at + n, wave_rows, stride=4), :]
            total += factor * (gathered[n, pl.ds(at, wave_rows), :] - center)
        return total

    inside_low = (jnp.zeros((halo, LANE), jnp.int32) + me) > 0
    inside_high = (jnp.zeros((halo, LANE), jnp.int32) + me) < nm - 1

    halo_each(send_halo1, "wait_recv")
    ext[0:halo, :] = jnp.where(inside_low, halo1[0, pl.ds(1, halo, stride=2), :], 0.0)
    ext[halo + cell_rows :, :] = jnp.where(
        inside_high, halo1[1, pl.ds(1, halo, stride=2), :], 0.0
    )
    load_coup.wait()

    for d in range(1, ny):
        send_part(d).wait_recv()
    weighted = part[0]
    for d in range(1, ny):
        weighted += part_in[d - 1]
    wall[pl.ds(pl.multiple_of(me * 2 * per, 8), 2 * per), :] = weighted
    for o in range(1, nm):
        send_wall(o).start()

    gather()

    def first_step(b, carry):
        at = b * wave_rows
        center = ext[pl.ds(halo + at, wave_rows), :]
        previous = wave[pl.ds(2 * at, wave_rows, stride=2), :]
        state[pl.ds(2 * at, wave_rows, stride=2), :] = (
            2.0 * center - previous + spread_of(at, center)
        )
        return carry

    lax.fori_loop(0, cell_rows // wave_rows, first_step, 0)

    total = series[:, columns(chunks - 1)]
    for d in range(1, ny):
        high, low = split(basis_own[m1 + (d - 1) * rp : m1 + d * rp, :])
        cross_high[d - 1] = high
        cross_low[d - 1] = low
        pass_raw(d).wait_recv()
        s_high, s_low = stage((raw_rows, raw_peer_rows), d - 1)
        high = cross_high[d - 1]
        product_d = dot(high, s_high) + dot(cross_low[d - 1], s_high) + dot(high, s_low)
        total += product_d[0:rows]
    series[:, columns(chunks - 1)] = total

    for o in range(1, nm):
        send_wall(o).wait_recv()

    def pick(t, carry):
        for i in range(8):
            g = t * 8 + i
            block = block_smem[g]
            row = (block // per) * (2 * per) + block % per
            picked[pl.ds(g, 1), :] = wall[pl.ds(row, 1), :]
            picked[pl.ds(groups + g, 1), :] = wall[pl.ds(row + per, 1), :]
        return carry

    lax.fori_loop(0, groups // 8, pick, 0)
    high, low = split(picked[...].T)
    xt_high[0:LANE, :] = high
    xt_high[LANE:, :] = high
    xt_low[...] = low
    load_weights.wait()
    batch = 8
    lane = lax.broadcasted_iota(jnp.int32, (LANE, groups), 1)

    def interpolate(t, carry):
        block = weights[pl.ds(t * batch, batch)].reshape(batch * LANE, LANE)
        w_high, w_low = split(block)
        both = jnp.concatenate([w_high, w_low], axis=1)
        result = dot(both, xt_high[...]) + dot(w_high, xt_low[...])
        for s in range(2):
            column = turned[s]
            for i in range(batch):
                column = jnp.where(
                    lane == t * batch + i,
                    result[i * LANE : (i + 1) * LANE, s * groups : (s + 1) * groups],
                    column,
                )
            turned[s] = column
        return carry

    turned[...] = jnp.zeros_like(turned)
    lax.fori_loop(0, groups // batch, interpolate, 0)
    alive = lax.broadcasted_iota(jnp.int32, (groups, LANE), 0) < count_smem[0]
    push = [jnp.where(alive, turned[s].T, 0.0) for s in range(2)]

    top = pl.ds(0, groups, stride=2)
    state[top, :] = state[top, :] + push[0]

    def stage_stepped(b, carry):
        at = b * wave_rows
        ext[pl.ds(halo + at, wave_rows), :] = state[pl.ds(2 * at, wave_rows, stride=2), :]
        return carry

    lax.fori_loop(0, cell_rows // wave_rows, stage_stepped, 0)
    halo_each(send_halo2, "start")
    halo_each(send_halo2, "wait_recv")
    ext[0:halo, :] = jnp.where(inside_low, halo2[0], 0.0)
    ext[halo + cell_rows :, :] = jnp.where(inside_high, halo2[1], 0.0)
    gather()

    def second_step(b, carry):
        at = b * wave_rows
        center = ext[pl.ds(halo + at, wave_rows), :]
        previous = wave[pl.ds(2 * at + 1, wave_rows, stride=2), :]
        state[pl.ds(2 * at + 1, wave_rows, stride=2), :] = (
            2.0 * center - previous + spread_of(at, center)
        )
        return carry

    lax.fori_loop(0, cell_rows // wave_rows, second_step, 0)
    bottom = pl.ds(1, groups, stride=2)
    state[bottom, :] = state[bottom, :] + push[1]

    def finish(c, carry):
        total = series[:, columns(c)]
        for d in range(1, ny):
            send_series(d, c).wait_recv()
            total += incoming[d - 1, c]
        series[:, columns(c)] = total
        return carry

    lax.fori_loop(0, chunks - 1, finish, 0)

    def drain(c, carry):
        swap(c).wait_send()
        for d in range(1, ny):
            send_series(d, c).wait_send()
        return carry

    lax.fori_loop(0, chunks - 1, drain, 0)
    swap(chunks - 1).wait_send()
    for d in range(1, ny):
        send_raw(d).wait_send()
        pass_raw(d).wait_send()
        send_tw(d).wait_send()
        send_part(d).wait_send()
    for o in range(1, nm):
        send_wall(o).wait_send()
    halo_each(send_halo1, "wait_send")
    halo_each(send_halo2, "wait_send")


def store(series, state, series_hbm, state_hbm, sem):
    copies = [
        pltpu.make_async_copy(series, series_hbm, sem.at[0]),
        pltpu.make_async_copy(state, state_hbm, sem.at[1]),
    ]
    for copy in copies:
        copy.start()
    for copy in copies:
        copy.wait()


def chip_basis(ny, coefs, rows, horizon):
    kp, rp = pad8(coefs), pad8(rows)
    freq = np.arange(ny * CORES).reshape(-1, 1, 1, 1, 1, 1)
    d, r, p, s, k = np.indices((2 * ny - 1, rp, CORES, 2, kp), sparse=True)
    chip, core = freq // CORES, freq % CORES
    source = chip - np.where(d < ny, 0, d - ny + 1)
    window = ((chip + np.where(d < ny, d, 0)) % ny) * CORES + core
    wave_number = (source % ny * CORES + (core + p) % CORES) * coefs + k
    angle = ((window * rows + r) * wave_number) % horizon * (2.0 * math.pi / horizon)
    scale = np.where(wave_number == 0, 1.0, 2.0) / horizon
    value = np.where(s == 0, np.cos(angle), -np.sin(angle)) * scale
    value = np.where((r < rows) & (k < coefs), value, 0.0)
    return value.reshape(ny * CORES, (2 * ny - 1) * rp, CORES * 2 * kp).astype(np.float32)


def local(
    ny,
    nm,
    spectrum,
    time_weights,
    interp_weights,
    group_block,
    group_count,
    wave_state,
    neighbors,
    coupling,
):
    coefs, points = spectrum.shape[1:]
    rows = time_weights.shape[1]
    horizon = rows * ny * CORES
    groups = interp_weights.shape[0]
    cell_rows = neighbors.shape[1]
    halo = HALO_CELLS // LANE
    blocks = points // LANE
    chunks = blocks // BLOCKS_PER_CHUNK
    kp, rp = pad8(coefs), pad8(rows)
    k_all, m_all = CORES * 2 * kp, ny * (rp + 8)
    seg = 2 * BLOCKS_PER_CHUNK
    width = BLOCKS_PER_CHUNK * LANE

    spec = spectrum.reshape(2, coefs, blocks, LANE).transpose(1, 2, 0, 3)
    spec = spec.reshape(coefs, 2 * blocks, LANE)
    wave = wave_state.reshape(2, cell_rows, LANE).transpose(1, 0, 2).reshape(2 * cell_rows, LANE)
    coup = coupling.reshape(4, cell_rows, LANE).transpose(1, 0, 2).reshape(4 * cell_rows, LANE)
    basis = jnp.asarray(chip_basis(ny, coefs, rows, horizon))

    vmem = lambda *shape: pltpu.VMEM(shape, F32)
    dma = lambda *shape: pltpu.SemaphoreType.DMA(shape)
    smem = pl.BlockSpec(memory_space=pltpu.SMEM)
    hbm = pl.BlockSpec(memory_space=pltpu.HBM)
    on_chip = pl.BlockSpec(memory_space=pltpu.VMEM)
    far = max(ny - 1, 1)
    pinned = [
        pltpu.with_memory_space_constraint(x, pltpu.HBM)
        for x in (
            group_block,
            neighbors,
            time_weights,
            basis,
            spec,
            interp_weights,
            wave,
            coup,
        )
    ]
    outs = (
        jax.ShapeDtypeStruct((rows, points), F32),
        jax.ShapeDtypeStruct((2 * cell_rows, LANE), F32),
    )
    series, state = pl.pallas_call(
        functools.partial(kernel, (ny, nm, coefs, rows, chunks)),
        out_shape=outs,
        in_specs=[smem] + [hbm] * 8,
        out_specs=(on_chip, on_chip),
        scratch_shapes=[
            pltpu.SMEM(group_block.shape, jnp.int32),
            pltpu.SMEM(neighbors.shape, jnp.int32),
            vmem(2, rows),
            vmem((2 * ny - 1) * rp, k_all),
            vmem(8 * ny, k_all),
            vmem(chunks, coefs, seg, LANE),
            vmem(chunks, coefs, seg, LANE),
            vmem(k_all, width),
            pltpu.VMEM((m_all, k_all), BF16),
            pltpu.VMEM((m_all, k_all), BF16),
            pltpu.VMEM((far, rp, k_all), BF16),
            pltpu.VMEM((far, rp, k_all), BF16),
            vmem(far, coefs, seg, LANE),
            vmem(far, coefs, seg, LANE),
            vmem(far, 2, rows),
            vmem(far, chunks, rows, width),
            vmem(far, chunks, rows, width),
            vmem(ny, 2 * blocks, LANE),
            vmem(far, 2 * blocks, LANE),
            vmem(nm * 2 * blocks, LANE),
            vmem(2 * groups, LANE),
            pltpu.VMEM((2 * LANE, 2 * groups), BF16),
            pltpu.VMEM((LANE, 2 * groups), BF16),
            vmem(2, LANE, groups),
            vmem(groups, LANE, LANE),
            vmem(2 * cell_rows, LANE),
            vmem(4 * cell_rows, LANE),
            vmem(2, 2 * halo, LANE),
            vmem(2, halo, LANE),
            vmem(cell_rows + 2 * halo, LANE),
            vmem(4, cell_rows, LANE),
            dma(chunks),
            dma(chunks),
            dma(chunks),
            dma(8),
            dma(far),
            dma(far),
            dma(far),
            dma(far),
            dma(far),
            dma(far),
            dma(far, chunks),
            dma(far, chunks),
            dma(far),
            dma(far),
            dma(max(nm - 1, 1)),
            dma(max(nm - 1, 1)),
            dma(4),
            dma(4),
            pltpu.SemaphoreType.REGULAR,
            pltpu.SemaphoreType.REGULAR((far,)),
            pltpu.SemaphoreType.REGULAR,
            pltpu.SemaphoreType.REGULAR,
        ],
        compiler_params=pltpu.CompilerParams(
            collective_id=0, has_side_effects=True, vmem_limit_bytes=40000 * 1024
        ),
        name="adjoint",
    )(group_count, *pinned)
    series, state = pl.pallas_call(
        store,
        out_shape=outs,
        in_specs=[pl.BlockSpec(memory_space=pl.ANY)] * 2,
        out_specs=(hbm, hbm),
        scratch_shapes=[dma(2)],
        compiler_params=pltpu.CompilerParams(vmem_limit_bytes=1024 * 1024),
        name="store",
    )(series, state)
    new_state = state.reshape(cell_rows, 2, LANE).transpose(1, 0, 2)
    return series, new_state.reshape(1, 2, cell_rows * LANE)


def solution(mesh):
    placed = (
        P(None, "freq", "mesh"),
        P(None, "freq"),
        P("mesh", None, None),
        P("mesh"),
        P("mesh"),
        P("freq", None, "mesh"),
        P(None, "mesh"),
        P(None, "mesh"),
    )
    ny = mesh.shape["freq"] // CORES
    return jax.shard_map(
        functools.partial(local, ny, mesh.shape["mesh"]),
        mesh=mesh,
        in_specs=placed,
        out_specs=(P("freq", "mesh"), P("freq", None, "mesh")),
        check_vma=False,
    )
```

```python
import functools
import math

import jax
import jax.numpy as jnp
import numpy as np
from jax import lax
from jax.experimental import pallas as pl
from jax.experimental.pallas import tpu as pltpu
from jax.sharding import PartitionSpec as P

LANE = 128
CORES = 2
HALO_CELLS = 4096
BLOCKS_PER_CHUNK = 4
RAW = 2
PAIR = 2
HIGHEST = lax.Precision.HIGHEST
F32 = jnp.float32
BF16 = jnp.bfloat16


def pad(n, to):
    return (n + to - 1) // to * to


def split(x):
    high = x.astype(BF16)
    return high, (x - high.astype(F32)).astype(BF16)


def dot(a, b):
    return jnp.dot(a, b, preferred_element_type=F32)


def kernel(
    dims,
    count_smem,
    block_hbm,
    neigh_hbm,
    tw_hbm,
    basis_hbm,
    spec_hbm,
    weights_hbm,
    wave_hbm,
    coup_hbm,
    series,
    state,
    block_smem,
    neigh_smem,
    tw_own,
    basis_own,
    folded,
    own_spec,
    peer_spec,
    staged,
    lhs_high,
    lhs_low,
    cross_high,
    cross_low,
    raw,
    raw_peer,
    tw_all,
    outgoing,
    incoming,
    part,
    part_in,
    wall,
    picked,
    asked,
    turned,
    weights,
    lined,
    wave,
    coup,
    halo1,
    halo2,
    ext,
    gathered,
    spec_sem,
    swap_send,
    swap_recv,
    load_sem,
    tw_send,
    tw_recv,
    raw_send,
    raw_recv,
    pass_send,
    pass_recv,
    ser_send,
    ser_recv,
    part_send,
    part_recv,
    wall_send,
    wall_recv,
    halo_send,
    halo_recv,
    go,
    seen,
    peers_in,
    all_in,
):
    ny, nm, coefs, rows, chunks = dims
    groups = weights.shape[0]
    kp, rp, fb = pad(coefs, 8), pad(rows, 8), pad(rows, 16)
    rb = fb + 16
    m1 = ny * rp
    per = part.shape[2]
    cell_rows = ext.shape[0] - 2 * halo1.shape[1] // 2
    halo = halo1.shape[1] // 2
    width = BLOCKS_PER_CHUNK * LANE
    seg = 2 * BLOCKS_PER_CHUNK
    summed = chunks - RAW
    whole_rows = rows // 8 * 8
    rest = rows - whole_rows

    freq = lax.axis_index("freq")
    me = lax.axis_index("mesh")
    chip, core = freq // CORES, freq % CORES
    partner = chip * CORES + (1 - core)

    def at_chip(d):
        return ((chip + d + ny) % ny) * CORES + core

    def peer(d):
        return (me + d + nm) % nm

    def remote(src, dst, send, recv, axis, target):
        return pltpu.make_async_remote_copy(
            src_ref=src,
            dst_ref=dst,
            send_sem=send,
            recv_sem=recv,
            device_id={axis: target},
            device_id_type=pl.DeviceIdType.MESH,
        )

    def load_spec(c):
        return pltpu.make_async_copy(
            spec_hbm.at[:, pl.ds(c * seg, seg), :],
            own_spec.at[c],
            spec_sem.at[1 if c >= summed else 0],
        )

    def loaded(first, count, sem):
        span = own_spec.at[pl.ds(first, count)]
        return pltpu.make_async_copy(span, span, spec_sem.at[sem])

    def swap(c):
        return remote(
            spec_hbm.at[:, pl.ds(c * seg, seg), :],
            peer_spec.at[c],
            swap_send.at[0],
            swap_recv.at[c // PAIR],
            "freq",
            partner,
        )

    def swapped(first, count):
        span = peer_spec.at[pl.ds(first, count)]
        return remote(span, span, swap_send.at[0], swap_recv.at[first // PAIR], "freq", partner)

    def send_tw(d):
        return remote(
            tw_own, tw_all.at[d - 1], tw_send.at[d - 1], tw_recv.at[d - 1], "freq", at_chip(-d)
        )

    def send_raw(d):
        return remote(
            own_spec.at[pl.ds(summed, RAW)],
            raw.at[d - 1],
            raw_send.at[d - 1],
            raw_recv.at[d - 1],
            "freq",
            at_chip(d),
        )

    def pass_raw(d):
        return remote(
            raw.at[d - 1],
            raw_peer.at[d - 1],
            pass_send.at[d - 1],
            pass_recv.at[d - 1],
            "freq",
            partner,
        )

    def send_series(d, first, count):
        span = pl.ds(first, count)
        return remote(
            outgoing.at[d - 1, span],
            incoming.at[d - 1, span],
            ser_send.at[d - 1],
            ser_recv.at[d - 1, jnp.where(first == summed - 1, 1, 0)],
            "freq",
            at_chip(d),
        )

    def send_part(d):
        return remote(
            part.at[d, :, pl.ds(0, summed * BLOCKS_PER_CHUNK), :],
            part_in.at[d - 1],
            part_send.at[d - 1],
            part_recv.at[d - 1],
            "freq",
            at_chip(d),
        )

    def send_wall(o):
        mine = wall.at[:, pl.ds(pl.multiple_of(me * per, 8), per), :]
        return remote(mine, mine, wall_send.at[0], wall_recv.at[0], "mesh", peer(o))

    def walled():
        span = wall.at[:, pl.ds(0, (nm - 1) * per), :]
        return remote(span, span, wall_send.at[0], wall_recv.at[0], "mesh", peer(1))

    def send_halo1(side):
        first = 0 if side else 2 * (cell_rows - halo)
        return remote(
            wave.at[pl.ds(first, 2 * halo)],
            halo1.at[side],
            halo_send.at[side],
            halo_recv.at[side],
            "mesh",
            peer(-1 if side else 1),
        )

    def send_halo2(side):
        first = halo if side else cell_rows
        return remote(
            ext.at[pl.ds(first, halo)],
            halo2.at[side],
            halo_send.at[2 + side],
            halo_recv.at[2 + side],
            "mesh",
            peer(-1 if side else 1),
        )

    inside = (me > 0, me < nm - 1)

    def halo_each(copy, method):
        for side in range(2):
            there = inside[side] if method == "wait_recv" else inside[1 - side]
            pl.when(there)(getattr(copy(side), method))

    def columns(c):
        return pl.ds(pl.multiple_of(c * width, width), width)

    load_wave = pltpu.make_async_copy(wave_hbm, wave, load_sem.at[0])
    load_coup = pltpu.make_async_copy(coup_hbm, coup, load_sem.at[1])
    load_weights = pltpu.make_async_copy(
        weights_hbm, weights.at[:, pl.ds(0, LANE), :], load_sem.at[2]
    )
    load_tw = pltpu.make_async_copy(tw_hbm, tw_own, load_sem.at[3])
    load_basis = pltpu.make_async_copy(basis_hbm.at[freq], basis_own, load_sem.at[4])
    load_neigh = pltpu.make_async_copy(neigh_hbm, neigh_smem, load_sem.at[5])
    load_block = pltpu.make_async_copy(block_hbm, block_smem, load_sem.at[6])

    load_tw.start()
    for c in (*range(summed, chunks), *range(summed)):
        load_spec(c).start()
    load_basis.start()
    load_wave.start()
    load_neigh.start()
    load_block.start()

    barrier = pltpu.get_barrier_semaphore()
    first_core, first_chip = core == 0, chip == 0
    other_core, other_chip = core == 1, chip != 0

    def signal(sem, axis, target):
        pl.semaphore_signal(
            sem, inc=1, device_id={axis: target}, device_id_type=pl.DeviceIdType.MESH
        )

    @pl.when(first_core)
    def _():
        for d in range(1, ny):
            signal(barrier, "freq", at_chip(d))

    @pl.when(first_core == other_chip)
    def _():
        signal(barrier, "freq", partner)

    @pl.when(first_core & first_chip)
    def _():
        pl.semaphore_wait(barrier, ny)
        signal(go, "freq", partner)

    @pl.when(first_core & other_chip)
    def _():
        pl.semaphore_wait(barrier, ny - 1)

    @pl.when(other_core & other_chip)
    def _():
        pl.semaphore_wait(barrier, 1)
        signal(go, "freq", partner)

    load_tw.wait()
    loaded(summed, RAW, 1).wait()

    def send_first():
        for d in range(1, ny):
            send_tw(d).start()
            send_raw(d).start()

    pl.when(first_core)(send_first)

    @pl.when(first_core == other_chip)
    def _():
        pl.semaphore_wait(go, 1)

    for c in range(chunks):
        swap(c).start()

    @pl.when(first_core)
    def _():
        for d in range(1, ny):
            signal(seen.at[d - 1], "freq", at_chip(d))
        for d in range(1, ny):
            pl.semaphore_wait(seen.at[d - 1], 1)
        signal(peers_in, "freq", partner)

    @pl.when(other_core)
    def _():
        pl.semaphore_wait(peers_in, 1)
        send_first()

    @pl.when(other_core & first_chip)
    def _():
        for o in range(1, nm):
            signal(barrier, "mesh", peer(o))

    load_coup.start()
    load_weights.start()

    staged[...] = jnp.zeros_like(staged)
    folded[...] = jnp.zeros_like(folded)
    load_basis.wait()
    for d in range(ny):
        high, low = split(basis_own[d * rp : (d + 1) * rp, :])
        lhs_high[d * rb : d * rb + rp, :] = high
        lhs_low[d * rb : d * rb + rp, :] = low
    for d in range(1, ny):
        high, low = split(basis_own[m1 + (d - 1) * rp : m1 + d * rp, :])
        cross_high[d - 1, 0:rp, :] = high
        cross_low[d - 1, 0:rp, :] = low
    for d in range(2 * ny - 1):
        if 0 < d < ny:
            send_tw(d).wait_recv()
        folded[16 * d : 16 * d + 2, :] = jnp.dot(
            tw_all[d - 1] if 0 < d < ny else tw_own[...],
            basis_own[d * rp : d * rp + rows, :],
            precision=HIGHEST,
            preferred_element_type=F32,
        )
        high, low = split(folded[16 * d : 16 * (d + 1), :])
        if d < ny:
            lhs_high[d * rb + fb : (d + 1) * rb, :] = high
            lhs_low[d * rb + fb : (d + 1) * rb, :] = low
        else:
            cross_high[d - ny, fb:rb, :] = high
            cross_low[d - ny, fb:rb, :] = low

    own_rows = own_spec.reshape(chunks * coefs * seg, LANE)
    peer_rows = peer_spec.reshape(chunks * coefs * seg, LANE)
    far = max(ny - 1, 1)
    raw_rows = raw.reshape(far * RAW * coefs * seg, LANE)
    raw_peer_rows = raw_peer.reshape(far * RAW * coefs * seg, LANE)

    def stage(sources, c):
        for p, source in enumerate(sources):
            for s in range(2):
                for j in range(BLOCKS_PER_CHUNK):
                    piece = source[pl.ds(c * (coefs * seg) + 2 * j + s, coefs, stride=seg), :]
                    base = (p * 2 + s) * kp
                    staged[base : base + coefs, j * LANE : (j + 1) * LANE] = piece
        return split(staged[...])

    def product(high, low, s_high, s_low):
        return dot(high, s_high) + dot(low, s_high) + dot(high, s_low)

    def keep_part(c, total, d):
        for s in range(2):
            row = d * rb + fb + s
            for j in range(BLOCKS_PER_CHUNK):
                part[d, s, pl.ds(c * BLOCKS_PER_CHUNK + j, 1), :] = total[
                    row : row + 1, j * LANE : (j + 1) * LANE
                ]

    def pieces(c):
        for j in range(BLOCKS_PER_CHUNK):
            lanes = pl.ds(pl.multiple_of(c * width + j * LANE, LANE), LANE)
            yield j, slice(0, whole_rows), slice(j * whole_rows, (j + 1) * whole_rows), lanes
            if rest:
                first = BLOCKS_PER_CHUNK * whole_rows + j * rest
                yield j, slice(whole_rows, rows), slice(first, first + rest), lanes

    def summed_chunk(c, carry):
        @pl.when(c % PAIR == 0)
        def _():
            swapped(c, PAIR).wait_recv()

        s_high, s_low = stage((own_rows, peer_rows), c)
        total = product(lhs_high[...], lhs_low[...], s_high, s_low)
        series[:, columns(c)] = total[0:rows]
        keep_part(c, total, 0)
        for d in range(1, ny):
            keep_part(c, total, d)
            for j, take, put, _ in pieces(c):
                outgoing[d - 1, c, put, :] = total[
                    d * rb + take.start : d * rb + take.stop, j * LANE : (j + 1) * LANE
                ]
        return carry

    loaded(0, summed, 0).wait()
    lax.fori_loop(0, summed, summed_chunk, 0)
    for d in range(1, ny):
        send_part(d).start()

    def send_chunk(c, carry):
        for d in range(1, ny):
            send_series(d, c, 1).start()
        return carry

    lax.fori_loop(0, summed, send_chunk, 0)

    def raw_chunk(c, carry):
        @pl.when(c % PAIR == 0)
        def _():
            swapped(c, PAIR).wait_recv()

        s_high, s_low = stage((own_rows, peer_rows), c)
        total = product(lhs_high[0:rb, :], lhs_low[0:rb, :], s_high, s_low)
        series[:, columns(c)] = total[0:rows]
        keep_part(c, total, 0)
        return carry

    lax.fori_loop(summed, chunks, raw_chunk, 0)

    @pl.when(other_core & first_chip)
    def _():
        pl.semaphore_wait(barrier, nm - 1)
        for d in range(ny):
            signal(all_in, "freq", d * CORES)
            if d:
                signal(all_in, "freq", d * CORES + 1)

    @pl.when(first_core | other_chip)
    def _():
        pl.semaphore_wait(all_in, 1)

    load_wave.wait()
    halo_each(send_halo1, "start")

    pitch = weights.shape[1]
    weight_rows = weights.reshape(groups * pitch, LANE)
    load_weights.wait()

    def line_up(t, carry):
        for i in range(4):
            f = t * 4 + i
            lined[pl.ds(pl.multiple_of(f * LANE, LANE), LANE), :] = weight_rows[
                pl.ds(f, groups, stride=pitch), :
            ].T
        return carry

    lax.fori_loop(0, LANE // 4, line_up, 0)

    for d in range(1, ny):
        send_raw(d).wait_recv()
        pass_raw(d).start()

    wave_rows = 64

    def stage_current(b, carry):
        at = b * wave_rows
        ext[pl.ds(halo + at, wave_rows), :] = wave[pl.ds(2 * at + 1, wave_rows, stride=2), :]
        return carry

    lax.fori_loop(0, cell_rows // wave_rows, stage_current, 0)

    load_neigh.wait()
    load_block.wait()

    def gather():
        def tile(t, carry):
            for n in range(4):
                for i in range(8):
                    u = t * 8 + i
                    gathered[n, pl.ds(u, 1), :] = ext[pl.ds(neigh_smem[n, u], 1), :]
            return carry

        lax.fori_loop(0, cell_rows // 8, tile, 0)

    def spread_of(at, center):
        total = jnp.zeros((wave_rows, LANE), F32)
        for n in range(4):
            factor = coup[pl.ds(4 * at + n, wave_rows, stride=4), :]
            total += factor * (gathered[n, pl.ds(at, wave_rows), :] - center)
        return total

    inside_low = (jnp.zeros((halo, LANE), jnp.int32) + me) > 0
    inside_high = (jnp.zeros((halo, LANE), jnp.int32) + me) < nm - 1

    halo_each(send_halo1, "wait_recv")
    ext[0:halo, :] = jnp.where(inside_low, halo1[0, pl.ds(1, halo, stride=2), :], 0.0)
    ext[halo + cell_rows :, :] = jnp.where(
        inside_high, halo1[1, pl.ds(1, halo, stride=2), :], 0.0
    )
    load_coup.wait()
    gather()

    def first_step(b, carry):
        at = b * wave_rows
        center = ext[pl.ds(halo + at, wave_rows), :]
        previous = wave[pl.ds(2 * at, wave_rows, stride=2), :]
        state[pl.ds(2 * at, wave_rows, stride=2), :] = (
            2.0 * center - previous + spread_of(at, center)
        )
        return carry

    lax.fori_loop(0, cell_rows // wave_rows, first_step, 0)

    for d in range(1, ny):
        pass_raw(d).wait_recv()
    for r in range(RAW):
        c = summed + r
        total = series[:, columns(c)]
        extra = None
        for d in range(1, ny):
            s_high, s_low = stage((raw_rows, raw_peer_rows), (d - 1) * RAW + r)
            cross = product(cross_high[d - 1], cross_low[d - 1], s_high, s_low)
            total += cross[0:rows]
            extra = cross[fb : fb + 2] if extra is None else extra + cross[fb : fb + 2]
        series[:, columns(c)] = total
        if extra is not None:
            for s in range(2):
                for j in range(BLOCKS_PER_CHUNK):
                    at = pl.ds(c * BLOCKS_PER_CHUNK + j, 1)
                    part[0, s, at, :] = (
                        part[0, s, at, :] + extra[s : s + 1, j * LANE : (j + 1) * LANE]
                    )

    for d in range(1, ny):
        send_part(d).wait_recv()
    first_blocks = summed * BLOCKS_PER_CHUNK
    base = pl.multiple_of(me * per, 8)
    for s in range(2):
        weighted = part[0, s, 0:first_blocks, :]
        for d in range(1, ny):
            weighted += part_in[d - 1, s]
        wall[s, pl.ds(base, first_blocks), :] = weighted
        wall[s, pl.ds(base + first_blocks, per - first_blocks), :] = part[0, s, first_blocks:, :]
    for o in range(1, nm):
        send_wall(o).start()
    walled().wait_recv()

    def pick(t, carry):
        for i in range(8):
            g = t * 8 + i
            block = block_smem[g]
            for s in range(2):
                picked[s, pl.ds(g, 1), :] = wall[s, pl.ds(block, 1), :]
        return carry

    lax.fori_loop(0, groups // 8, pick, 0)
    for s in range(2):
        asked[s] = picked[s].T

    def interpolate(t, carry):
        faces = lined[pl.ds(pl.multiple_of(t * 8 * LANE, 8 * LANE), 8 * LANE), :]
        faces = faces.reshape(8, LANE, groups)
        for s in range(2):
            turned[s, pl.ds(pl.multiple_of(t * 8, 8), 8), :] = jnp.sum(
                faces * asked[s][None], axis=1
            )
        return carry

    lax.fori_loop(0, LANE // 8, interpolate, 0)
    alive = lax.broadcasted_iota(jnp.int32, (groups, LANE), 0) < count_smem[0]
    push = [jnp.where(alive, turned[s].T, 0.0) for s in range(2)]

    top = pl.ds(0, groups, stride=2)
    state[top, :] = state[top, :] + push[0]

    def stage_stepped(b, carry):
        at = b * wave_rows
        ext[pl.ds(halo + at, wave_rows), :] = state[pl.ds(2 * at, wave_rows, stride=2), :]
        return carry

    lax.fori_loop(0, cell_rows // wave_rows, stage_stepped, 0)
    halo_each(send_halo2, "start")
    halo_each(send_halo2, "wait_recv")
    ext[0:halo, :] = jnp.where(inside_low, halo2[0], 0.0)
    ext[halo + cell_rows :, :] = jnp.where(inside_high, halo2[1], 0.0)
    gather()

    def second_step(b, carry):
        at = b * wave_rows
        center = ext[pl.ds(halo + at, wave_rows), :]
        previous = wave[pl.ds(2 * at + 1, wave_rows, stride=2), :]
        state[pl.ds(2 * at + 1, wave_rows, stride=2), :] = (
            2.0 * center - previous + spread_of(at, center)
        )
        return carry

    lax.fori_loop(0, cell_rows // wave_rows, second_step, 0)
    bottom = pl.ds(1, groups, stride=2)
    state[bottom, :] = state[bottom, :] + push[1]

    swapped(0, chunks).wait_send()
    walled().wait_send()
    for d in range(1, ny):
        send_raw(d).wait_send()
        pass_raw(d).wait_send()
        send_tw(d).wait_send()
        send_part(d).wait_send()
    halo_each(send_halo1, "wait_send")
    halo_each(send_halo2, "wait_send")

    def finish(c, carry):
        for d in range(1, ny):
            for _, take, put, lanes in pieces(c):
                series[take, lanes] = series[take, lanes] + incoming[d - 1, c, put, :]
        return carry

    last = summed - 1
    for d in range(1, ny):
        send_series(d, 0, last).wait_recv()
    lax.fori_loop(0, last, finish, 0)
    for d in range(1, ny):
        send_series(d, 0, summed).wait_send()
        send_series(d, last, 1).wait_recv()
    finish(last, 0)


def store(series, state, series_hbm, state_hbm, sem):
    copies = [
        pltpu.make_async_copy(series, series_hbm, sem.at[0]),
        pltpu.make_async_copy(state, state_hbm, sem.at[1]),
    ]
    for copy in copies:
        copy.start()
    for copy in copies:
        copy.wait()


def chip_basis(ny, coefs, rows, horizon):
    kp, rp = pad(coefs, 8), pad(rows, 8)
    freq = np.arange(ny * CORES).reshape(-1, 1, 1, 1, 1, 1)
    d, r, p, s, k = np.indices((2 * ny - 1, rp, CORES, 2, kp), sparse=True)
    chip, core = freq // CORES, freq % CORES
    source = chip - np.where(d < ny, 0, d - ny + 1)
    window = ((chip + np.where(d < ny, d, 0)) % ny) * CORES + core
    wave_number = (source % ny * CORES + (core + p) % CORES) * coefs + k
    angle = ((window * rows + r) * wave_number) % horizon * (2.0 * math.pi / horizon)
    scale = np.where(wave_number == 0, 1.0, 2.0) / horizon
    value = np.where(s == 0, np.cos(angle), -np.sin(angle)) * scale
    value = np.where((r < rows) & (k < coefs), value, 0.0)
    return value.reshape(ny * CORES, (2 * ny - 1) * rp, CORES * 2 * kp).astype(np.float32)


def local(
    ny,
    nm,
    spectrum,
    time_weights,
    interp_weights,
    group_block,
    group_count,
    wave_state,
    neighbors,
    coupling,
):
    coefs, points = spectrum.shape[1:]
    rows = time_weights.shape[1]
    horizon = rows * ny * CORES
    groups = interp_weights.shape[0]
    cell_rows = neighbors.shape[1]
    halo = HALO_CELLS // LANE
    blocks = points // LANE
    chunks = blocks // BLOCKS_PER_CHUNK
    kp, rp = pad(coefs, 8), pad(rows, 8)
    k_all, rb = CORES * 2 * kp, pad(rows, 16) + 16
    summed = chunks - RAW
    seg = 2 * BLOCKS_PER_CHUNK
    width = BLOCKS_PER_CHUNK * LANE

    spec = spectrum.reshape(2, coefs, blocks, LANE).transpose(1, 2, 0, 3)
    spec = spec.reshape(coefs, 2 * blocks, LANE)
    wave = wave_state.reshape(2, cell_rows, LANE).transpose(1, 0, 2).reshape(2 * cell_rows, LANE)
    coup = coupling.reshape(4, cell_rows, LANE).transpose(1, 0, 2).reshape(4 * cell_rows, LANE)
    basis = jnp.asarray(chip_basis(ny, coefs, rows, horizon))

    vmem = lambda *shape: pltpu.VMEM(shape, F32)
    dma = lambda *shape: pltpu.SemaphoreType.DMA(shape)
    smem = pl.BlockSpec(memory_space=pltpu.SMEM)
    hbm = pl.BlockSpec(memory_space=pltpu.HBM)
    on_chip = pl.BlockSpec(memory_space=pltpu.VMEM)
    far = max(ny - 1, 1)
    pinned = [
        pltpu.with_memory_space_constraint(x, pltpu.HBM)
        for x in (
            group_block,
            neighbors,
            time_weights,
            basis,
            spec,
            interp_weights,
            wave,
            coup,
        )
    ]
    outs = (
        jax.ShapeDtypeStruct((rows, points), F32),
        jax.ShapeDtypeStruct((2 * cell_rows, LANE), F32),
    )
    series, state = pl.pallas_call(
        functools.partial(kernel, (ny, nm, coefs, rows, chunks)),
        out_shape=outs,
        in_specs=[smem] + [hbm] * 8,
        out_specs=(on_chip, on_chip),
        scratch_shapes=[
            pltpu.SMEM(group_block.shape, jnp.int32),
            pltpu.SMEM(neighbors.shape, jnp.int32),
            vmem(2, rows),
            vmem((2 * ny - 1) * rp, k_all),
            vmem(16 * (2 * ny - 1), k_all),
            vmem(chunks, coefs, seg, LANE),
            vmem(chunks, coefs, seg, LANE),
            vmem(k_all, width),
            pltpu.VMEM((ny * rb, k_all), BF16),
            pltpu.VMEM((ny * rb, k_all), BF16),
            pltpu.VMEM((far, rb, k_all), BF16),
            pltpu.VMEM((far, rb, k_all), BF16),
            vmem(far, RAW, coefs, seg, LANE),
            vmem(far, RAW, coefs, seg, LANE),
            vmem(far, 2, rows),
            vmem(far, summed, BLOCKS_PER_CHUNK * rows, LANE),
            vmem(far, summed, BLOCKS_PER_CHUNK * rows, LANE),
            vmem(ny, 2, blocks, LANE),
            vmem(far, 2, summed * BLOCKS_PER_CHUNK, LANE),
            vmem(2, nm * blocks, LANE),
            vmem(2, groups, LANE),
            vmem(2, LANE, groups),
            vmem(2, LANE, groups),
            vmem(groups, LANE + 8, LANE),
            vmem(LANE * LANE, groups),
            vmem(2 * cell_rows, LANE),
            vmem(4 * cell_rows, LANE),
            vmem(2, 2 * halo, LANE),
            vmem(2, halo, LANE),
            vmem(cell_rows + 2 * halo, LANE),
            vmem(4, cell_rows, LANE),
            dma(2),
            dma(1),
            dma(chunks // PAIR),
            dma(7),
            dma(far),
            dma(far),
            dma(far),
            dma(far),
            dma(far),
            dma(far),
            dma(far),
            dma(far, 2),
            dma(far),
            dma(far),
            dma(1),
            dma(1),
            dma(4),
            dma(4),
            pltpu.SemaphoreType.REGULAR,
            pltpu.SemaphoreType.REGULAR((far,)),
            pltpu.SemaphoreType.REGULAR,
            pltpu.SemaphoreType.REGULAR,
        ],
        compiler_params=pltpu.CompilerParams(
            collective_id=0, has_side_effects=True, vmem_limit_bytes=50000 * 1024
        ),
        name="adjoint",
    )(group_count, *pinned)
    series, state = pl.pallas_call(
        store,
        out_shape=outs,
        in_specs=[pl.BlockSpec(memory_space=pl.ANY)] * 2,
        out_specs=(hbm, hbm),
        scratch_shapes=[dma(2)],
        compiler_params=pltpu.CompilerParams(vmem_limit_bytes=1024 * 1024),
        name="store",
    )(series, state)
    new_state = state.reshape(cell_rows, 2, LANE).transpose(1, 0, 2)
    return series, new_state.reshape(1, 2, cell_rows * LANE)


def solution(mesh):
    placed = (
        P(None, "freq", "mesh"),
        P(None, "freq"),
        P("mesh", None, None),
        P("mesh"),
        P("mesh"),
        P("freq", None, "mesh"),
        P(None, "mesh"),
        P(None, "mesh"),
    )
    ny = mesh.shape["freq"] // CORES
    return jax.shard_map(
        functools.partial(local, ny, mesh.shape["mesh"]),
        mesh=mesh,
        in_specs=placed,
        out_specs=(P("freq", "mesh"), P("freq", None, "mesh")),
        check_vma=False,
    )
```

```python
import functools
import math

import jax
import jax.numpy as jnp
import numpy as np
from jax import lax
from jax.experimental import pallas as pl
from jax.experimental.pallas import tpu as pltpu
from jax.sharding import PartitionSpec as P

LANE = 128
CORES = 2
HALO_CELLS = 4096
BLOCKS_PER_CHUNK = 4
RAW = 2
PAIR = 2
HIGHEST = lax.Precision.HIGHEST
F32 = jnp.float32
BF16 = jnp.bfloat16


def pad(n, to):
    return (n + to - 1) // to * to


def split(x):
    high = x.astype(BF16)
    return high, (x - high.astype(F32)).astype(BF16)


def dot(a, b):
    return jnp.dot(a, b, preferred_element_type=F32)


def kernel(
    dims,
    count_smem,
    block_hbm,
    neigh_hbm,
    tw_hbm,
    basis_hbm,
    spec_hbm,
    weights_hbm,
    wave_hbm,
    coup_hbm,
    series,
    state,
    block_smem,
    neigh_smem,
    tw_own,
    basis_own,
    folded,
    own_spec,
    peer_spec,
    staged,
    lhs_high,
    lhs_low,
    cross_high,
    cross_low,
    raw,
    raw_peer,
    tw_all,
    outgoing,
    incoming,
    part,
    part_in,
    wall,
    picked,
    asked,
    turned,
    weights,
    lined,
    wave,
    coup,
    halo1,
    halo2,
    ext,
    gathered,
    ser_send,
    ser_recv,
):
    ny, nm, coefs, rows, chunks = dims
    groups = weights.shape[0]
    kp, rp, fb = pad(coefs, 8), pad(rows, 8), pad(rows, 16)
    rb = fb + 16
    m1 = ny * rp
    per = part.shape[2]
    cell_rows = ext.shape[0] - 2 * halo1.shape[1] // 2
    halo = halo1.shape[1] // 2
    width = BLOCKS_PER_CHUNK * LANE
    seg = 2 * BLOCKS_PER_CHUNK
    summed = chunks - RAW
    whole_rows = rows // 8 * 8
    rest = rows - whole_rows

    freq = lax.axis_index("freq")
    me = lax.axis_index("mesh")
    chip, core = freq // CORES, freq % CORES
    partner = chip * CORES + (1 - core)

    def at_chip(d):
        return ((chip + d + ny) % ny) * CORES + core

    def peer(d):
        return (me + d + nm) % nm

    def remote(src, dst, send, recv, axis, target):
        return pltpu.make_async_remote_copy(
            src_ref=src,
            dst_ref=dst,
            send_sem=send,
            recv_sem=recv,
            device_id={axis: target},
            device_id_type=pl.DeviceIdType.MESH,
        )

    def send_series(d, first, count):
        span = pl.ds(first, count)
        return remote(
            outgoing.at[d - 1, span],
            incoming.at[d - 1, span],
            ser_send.at[d - 1],
            ser_recv.at[d - 1, jnp.where(first == summed - 1, 1, 0)],
            "freq",
            at_chip(d),
        )

    def pieces(c):
        for j in range(BLOCKS_PER_CHUNK):
            lanes = pl.ds(pl.multiple_of(c * width + j * LANE, LANE), LANE)
            yield j, slice(0, whole_rows), slice(j * whole_rows, (j + 1) * whole_rows), lanes
            if rest:
                first = BLOCKS_PER_CHUNK * whole_rows + j * rest
                yield j, slice(whole_rows, rows), slice(first, first + rest), lanes

    def exchange(
        spec_sem,
        swap_send,
        swap_recv,
        load_sem,
        tw_send,
        tw_recv,
        raw_send,
        raw_recv,
        pass_send,
        pass_recv,
        part_send,
        part_recv,
        wall_send,
        wall_recv,
        halo_send,
        halo_recv,
        go,
        seen,
        peers_in,
        all_in,
    ):
        def load_spec(c):
            return pltpu.make_async_copy(
                spec_hbm.at[:, pl.ds(c * seg, seg), :],
                own_spec.at[c],
                spec_sem.at[1 if c >= summed else 0],
            )

        def loaded(first, count, sem):
            span = own_spec.at[pl.ds(first, count)]
            return pltpu.make_async_copy(span, span, spec_sem.at[sem])

        def swap(c):
            return remote(
                spec_hbm.at[:, pl.ds(c * seg, seg), :],
                peer_spec.at[c],
                swap_send.at[0],
                swap_recv.at[c // PAIR],
                "freq",
                partner,
            )

        def swapped(first, count):
            span = peer_spec.at[pl.ds(first, count)]
            return remote(span, span, swap_send.at[0], swap_recv.at[first // PAIR], "freq", partner)

        def send_tw(d):
            return remote(
                tw_own, tw_all.at[d - 1], tw_send.at[d - 1], tw_recv.at[d - 1], "freq", at_chip(-d)
            )

        def send_raw(d):
            return remote(
                own_spec.at[pl.ds(summed, RAW)],
                raw.at[d - 1],
                raw_send.at[d - 1],
                raw_recv.at[d - 1],
                "freq",
                at_chip(d),
            )

        def pass_raw(d):
            return remote(
                raw.at[d - 1],
                raw_peer.at[d - 1],
                pass_send.at[d - 1],
                pass_recv.at[d - 1],
                "freq",
                partner,
            )

        def send_part(d):
            return remote(
                part.at[d, :, pl.ds(0, summed * BLOCKS_PER_CHUNK), :],
                part_in.at[d - 1],
                part_send.at[d - 1],
                part_recv.at[d - 1],
                "freq",
                at_chip(d),
            )

        def send_wall(o):
            mine = wall.at[:, pl.ds(pl.multiple_of(me * per, 8), per), :]
            return remote(mine, mine, wall_send.at[0], wall_recv.at[0], "mesh", peer(o))

        def walled():
            span = wall.at[:, pl.ds(0, (nm - 1) * per), :]
            return remote(span, span, wall_send.at[0], wall_recv.at[0], "mesh", peer(1))

        def send_halo1(side):
            first = 0 if side else 2 * (cell_rows - halo)
            return remote(
                wave.at[pl.ds(first, 2 * halo)],
                halo1.at[side],
                halo_send.at[side],
                halo_recv.at[side],
                "mesh",
                peer(-1 if side else 1),
            )

        def send_halo2(side):
            first = halo if side else cell_rows
            return remote(
                ext.at[pl.ds(first, halo)],
                halo2.at[side],
                halo_send.at[2 + side],
                halo_recv.at[2 + side],
                "mesh",
                peer(-1 if side else 1),
            )

        inside = (me > 0, me < nm - 1)

        def halo_each(copy, method):
            for side in range(2):
                there = inside[side] if method == "wait_recv" else inside[1 - side]
                pl.when(there)(getattr(copy(side), method))

        def columns(c):
            return pl.ds(pl.multiple_of(c * width, width), width)

        load_wave = pltpu.make_async_copy(wave_hbm, wave, load_sem.at[0])
        load_coup = pltpu.make_async_copy(coup_hbm, coup, load_sem.at[1])
        load_weights = pltpu.make_async_copy(
            weights_hbm, weights.at[:, pl.ds(0, LANE), :], load_sem.at[2]
        )
        load_tw = pltpu.make_async_copy(tw_hbm, tw_own, load_sem.at[3])
        load_basis = pltpu.make_async_copy(basis_hbm.at[freq], basis_own, load_sem.at[4])
        load_neigh = pltpu.make_async_copy(neigh_hbm, neigh_smem, load_sem.at[5])
        load_block = pltpu.make_async_copy(block_hbm, block_smem, load_sem.at[6])

        load_tw.start()
        for c in (*range(summed, chunks), *range(summed)):
            load_spec(c).start()
        load_basis.start()
        load_wave.start()
        load_neigh.start()
        load_block.start()

        barrier = pltpu.get_barrier_semaphore()
        first_core, first_chip = core == 0, chip == 0
        other_core, other_chip = core == 1, chip != 0

        def signal(sem, axis, target):
            pl.semaphore_signal(
                sem, inc=1, device_id={axis: target}, device_id_type=pl.DeviceIdType.MESH
            )

        @pl.when(first_core)
        def _():
            for d in range(1, ny):
                signal(barrier, "freq", at_chip(d))

        @pl.when(first_core == other_chip)
        def _():
            signal(barrier, "freq", partner)

        @pl.when(first_core & first_chip)
        def _():
            pl.semaphore_wait(barrier, ny)
            signal(go.at[0], "freq", partner)

        @pl.when(first_core & other_chip)
        def _():
            pl.semaphore_wait(barrier, ny - 1)

        @pl.when(other_core & other_chip)
        def _():
            pl.semaphore_wait(barrier, 1)
            signal(go.at[0], "freq", partner)

        load_tw.wait()
        loaded(summed, RAW, 1).wait()

        def send_first():
            for d in range(1, ny):
                send_tw(d).start()
                send_raw(d).start()

        pl.when(first_core)(send_first)

        @pl.when(first_core == other_chip)
        def _():
            pl.semaphore_wait(go.at[0], 1)

        for c in range(chunks):
            swap(c).start()

        @pl.when(first_core)
        def _():
            for d in range(1, ny):
                signal(seen.at[d - 1], "freq", at_chip(d))
            for d in range(1, ny):
                pl.semaphore_wait(seen.at[d - 1], 1)
            signal(peers_in.at[0], "freq", partner)

        @pl.when(other_core)
        def _():
            pl.semaphore_wait(peers_in.at[0], 1)
            send_first()

        @pl.when(other_core & first_chip)
        def _():
            for o in range(1, nm):
                signal(barrier, "mesh", peer(o))

        load_coup.start()
        load_weights.start()

        staged[...] = jnp.zeros_like(staged)
        folded[...] = jnp.zeros_like(folded)
        load_basis.wait()
        for d in range(ny):
            high, low = split(basis_own[d * rp : (d + 1) * rp, :])
            lhs_high[d * rb : d * rb + rp, :] = high
            lhs_low[d * rb : d * rb + rp, :] = low
        for d in range(1, ny):
            high, low = split(basis_own[m1 + (d - 1) * rp : m1 + d * rp, :])
            cross_high[d - 1, 0:rp, :] = high
            cross_low[d - 1, 0:rp, :] = low
        for d in range(2 * ny - 1):
            if 0 < d < ny:
                send_tw(d).wait_recv()
            folded[16 * d : 16 * d + 2, :] = jnp.dot(
                tw_all[d - 1] if 0 < d < ny else tw_own[...],
                basis_own[d * rp : d * rp + rows, :],
                precision=HIGHEST,
                preferred_element_type=F32,
            )
            high, low = split(folded[16 * d : 16 * (d + 1), :])
            if d < ny:
                lhs_high[d * rb + fb : (d + 1) * rb, :] = high
                lhs_low[d * rb + fb : (d + 1) * rb, :] = low
            else:
                cross_high[d - ny, fb:rb, :] = high
                cross_low[d - ny, fb:rb, :] = low

        own_rows = own_spec.reshape(chunks * coefs * seg, LANE)
        peer_rows = peer_spec.reshape(chunks * coefs * seg, LANE)
        far = max(ny - 1, 1)
        raw_rows = raw.reshape(far * RAW * coefs * seg, LANE)
        raw_peer_rows = raw_peer.reshape(far * RAW * coefs * seg, LANE)

        def stage(sources, c):
            for p, source in enumerate(sources):
                for s in range(2):
                    for j in range(BLOCKS_PER_CHUNK):
                        piece = source[pl.ds(c * (coefs * seg) + 2 * j + s, coefs, stride=seg), :]
                        base = (p * 2 + s) * kp
                        staged[base : base + coefs, j * LANE : (j + 1) * LANE] = piece
            return split(staged[...])

        def product(high, low, s_high, s_low):
            return dot(high, s_high) + dot(low, s_high) + dot(high, s_low)

        def keep_part(c, total, d):
            for s in range(2):
                row = d * rb + fb + s
                for j in range(BLOCKS_PER_CHUNK):
                    part[d, s, pl.ds(c * BLOCKS_PER_CHUNK + j, 1), :] = total[
                        row : row + 1, j * LANE : (j + 1) * LANE
                    ]

        def summed_chunk(c, carry):
            @pl.when(c % PAIR == 0)
            def _():
                swapped(c, PAIR).wait_recv()

            s_high, s_low = stage((own_rows, peer_rows), c)
            total = product(lhs_high[...], lhs_low[...], s_high, s_low)
            series[:, columns(c)] = total[0:rows]
            keep_part(c, total, 0)
            for d in range(1, ny):
                keep_part(c, total, d)
                for j, take, put, _ in pieces(c):
                    outgoing[d - 1, c, put, :] = total[
                        d * rb + take.start : d * rb + take.stop, j * LANE : (j + 1) * LANE
                    ]
            return carry

        loaded(0, summed, 0).wait()
        lax.fori_loop(0, summed, summed_chunk, 0)
        for d in range(1, ny):
            send_part(d).start()

        def send_chunk(c, carry):
            for d in range(1, ny):
                send_series(d, c, 1).start()
            return carry

        lax.fori_loop(0, summed, send_chunk, 0)

        def raw_chunk(c, carry):
            @pl.when(c % PAIR == 0)
            def _():
                swapped(c, PAIR).wait_recv()

            s_high, s_low = stage((own_rows, peer_rows), c)
            total = product(lhs_high[0:rb, :], lhs_low[0:rb, :], s_high, s_low)
            series[:, columns(c)] = total[0:rows]
            keep_part(c, total, 0)
            return carry

        lax.fori_loop(summed, chunks, raw_chunk, 0)

        @pl.when(other_core & first_chip)
        def _():
            pl.semaphore_wait(barrier, nm - 1)
            for d in range(ny):
                signal(all_in.at[0], "freq", d * CORES)
                if d:
                    signal(all_in.at[0], "freq", d * CORES + 1)

        @pl.when(first_core | other_chip)
        def _():
            pl.semaphore_wait(all_in.at[0], 1)

        load_wave.wait()
        halo_each(send_halo1, "start")

        pitch = weights.shape[1]
        weight_rows = weights.reshape(groups * pitch, LANE)
        load_weights.wait()

        def line_up(t, carry):
            for i in range(4):
                f = t * 4 + i
                lined[pl.ds(pl.multiple_of(f * LANE, LANE), LANE), :] = weight_rows[
                    pl.ds(f, groups, stride=pitch), :
                ].T
            return carry

        lax.fori_loop(0, LANE // 4, line_up, 0)

        for d in range(1, ny):
            send_raw(d).wait_recv()
            pass_raw(d).start()

        wave_rows = 64

        def stage_current(b, carry):
            at = b * wave_rows
            ext[pl.ds(halo + at, wave_rows), :] = wave[pl.ds(2 * at + 1, wave_rows, stride=2), :]
            return carry

        lax.fori_loop(0, cell_rows // wave_rows, stage_current, 0)

        load_neigh.wait()
        load_block.wait()

        def gather():
            def tile(t, carry):
                for n in range(4):
                    for i in range(8):
                        u = t * 8 + i
                        gathered[n, pl.ds(u, 1), :] = ext[pl.ds(neigh_smem[n, u], 1), :]
                return carry

            lax.fori_loop(0, cell_rows // 8, tile, 0)

        def spread_of(at, center):
            total = jnp.zeros((wave_rows, LANE), F32)
            for n in range(4):
                factor = coup[pl.ds(4 * at + n, wave_rows, stride=4), :]
                total += factor * (gathered[n, pl.ds(at, wave_rows), :] - center)
            return total

        inside_low = (jnp.zeros((halo, LANE), jnp.int32) + me) > 0
        inside_high = (jnp.zeros((halo, LANE), jnp.int32) + me) < nm - 1

        halo_each(send_halo1, "wait_recv")
        ext[0:halo, :] = jnp.where(inside_low, halo1[0, pl.ds(1, halo, stride=2), :], 0.0)
        ext[halo + cell_rows :, :] = jnp.where(
            inside_high, halo1[1, pl.ds(1, halo, stride=2), :], 0.0
        )
        load_coup.wait()
        gather()

        def first_step(b, carry):
            at = b * wave_rows
            center = ext[pl.ds(halo + at, wave_rows), :]
            previous = wave[pl.ds(2 * at, wave_rows, stride=2), :]
            state[pl.ds(2 * at, wave_rows, stride=2), :] = (
                2.0 * center - previous + spread_of(at, center)
            )
            return carry

        lax.fori_loop(0, cell_rows // wave_rows, first_step, 0)

        for d in range(1, ny):
            pass_raw(d).wait_recv()
        for r in range(RAW):
            c = summed + r
            total = series[:, columns(c)]
            extra = None
            for d in range(1, ny):
                s_high, s_low = stage((raw_rows, raw_peer_rows), (d - 1) * RAW + r)
                cross = product(cross_high[d - 1], cross_low[d - 1], s_high, s_low)
                total += cross[0:rows]
                extra = cross[fb : fb + 2] if extra is None else extra + cross[fb : fb + 2]
            series[:, columns(c)] = total
            if extra is not None:
                for s in range(2):
                    for j in range(BLOCKS_PER_CHUNK):
                        at = pl.ds(c * BLOCKS_PER_CHUNK + j, 1)
                        part[0, s, at, :] = (
                            part[0, s, at, :] + extra[s : s + 1, j * LANE : (j + 1) * LANE]
                        )

        for d in range(1, ny):
            send_part(d).wait_recv()
        first_blocks = summed * BLOCKS_PER_CHUNK
        base = pl.multiple_of(me * per, 8)
        for s in range(2):
            weighted = part[0, s, 0:first_blocks, :]
            for d in range(1, ny):
                weighted += part_in[d - 1, s]
            wall[s, pl.ds(base, first_blocks), :] = weighted
            wall[s, pl.ds(base + first_blocks, per - first_blocks), :] = part[0, s, first_blocks:, :]
        for o in range(1, nm):
            send_wall(o).start()
        walled().wait_recv()

        def pick(t, carry):
            for i in range(8):
                g = t * 8 + i
                block = block_smem[g]
                for s in range(2):
                    picked[s, pl.ds(g, 1), :] = wall[s, pl.ds(block, 1), :]
            return carry

        lax.fori_loop(0, groups // 8, pick, 0)
        for s in range(2):
            asked[s] = picked[s].T

        def interpolate(t, carry):
            faces = lined[pl.ds(pl.multiple_of(t * 8 * LANE, 8 * LANE), 8 * LANE), :]
            faces = faces.reshape(8, LANE, groups)
            for s in range(2):
                turned[s, pl.ds(pl.multiple_of(t * 8, 8), 8), :] = jnp.sum(
                    faces * asked[s][None], axis=1
                )
            return carry

        lax.fori_loop(0, LANE // 8, interpolate, 0)
        alive = lax.broadcasted_iota(jnp.int32, (groups, LANE), 0) < count_smem[0]
        push = [jnp.where(alive, turned[s].T, 0.0) for s in range(2)]

        top = pl.ds(0, groups, stride=2)
        state[top, :] = state[top, :] + push[0]

        def stage_stepped(b, carry):
            at = b * wave_rows
            ext[pl.ds(halo + at, wave_rows), :] = state[pl.ds(2 * at, wave_rows, stride=2), :]
            return carry

        lax.fori_loop(0, cell_rows // wave_rows, stage_stepped, 0)
        halo_each(send_halo2, "start")
        halo_each(send_halo2, "wait_recv")
        ext[0:halo, :] = jnp.where(inside_low, halo2[0], 0.0)
        ext[halo + cell_rows :, :] = jnp.where(inside_high, halo2[1], 0.0)
        gather()

        def second_step(b, carry):
            at = b * wave_rows
            center = ext[pl.ds(halo + at, wave_rows), :]
            previous = wave[pl.ds(2 * at + 1, wave_rows, stride=2), :]
            state[pl.ds(2 * at + 1, wave_rows, stride=2), :] = (
                2.0 * center - previous + spread_of(at, center)
            )
            return carry

        lax.fori_loop(0, cell_rows // wave_rows, second_step, 0)
        bottom = pl.ds(1, groups, stride=2)
        state[bottom, :] = state[bottom, :] + push[1]

        swapped(0, chunks).wait_send()
        walled().wait_send()
        for d in range(1, ny):
            send_raw(d).wait_send()
            pass_raw(d).wait_send()
            send_tw(d).wait_send()
            send_part(d).wait_send()
        halo_each(send_halo1, "wait_send")
        halo_each(send_halo2, "wait_send")

    dma = lambda *shape: pltpu.SemaphoreType.DMA(shape)
    regular = lambda *shape: pltpu.SemaphoreType.REGULAR(shape)
    far = max(ny - 1, 1)
    pl.run_scoped(
        exchange,
        dma(2),
        dma(1),
        dma(chunks // PAIR),
        dma(7),
        dma(far),
        dma(far),
        dma(far),
        dma(far),
        dma(far),
        dma(far),
        dma(far),
        dma(far),
        dma(1),
        dma(1),
        dma(4),
        dma(4),
        regular(1),
        regular(far),
        regular(1),
        regular(1),
    )

    def finish(c, carry):
        for d in range(1, ny):
            for _, take, put, lanes in pieces(c):
                series[take, lanes] = series[take, lanes] + incoming[d - 1, c, put, :]
        return carry

    last = summed - 1
    for d in range(1, ny):
        send_series(d, 0, last).wait_recv()
    lax.fori_loop(0, last, finish, 0)
    for d in range(1, ny):
        send_series(d, 0, summed).wait_send()
        send_series(d, last, 1).wait_recv()
    finish(last, 0)


def store(series, state, series_hbm, state_hbm, sem):
    copies = [
        pltpu.make_async_copy(series, series_hbm, sem.at[0]),
        pltpu.make_async_copy(state, state_hbm, sem.at[1]),
    ]
    for copy in copies:
        copy.start()
    for copy in copies:
        copy.wait()


def chip_basis(ny, coefs, rows, horizon):
    kp, rp = pad(coefs, 8), pad(rows, 8)
    freq = np.arange(ny * CORES).reshape(-1, 1, 1, 1, 1, 1)
    d, r, p, s, k = np.indices((2 * ny - 1, rp, CORES, 2, kp), sparse=True)
    chip, core = freq // CORES, freq % CORES
    source = chip - np.where(d < ny, 0, d - ny + 1)
    window = ((chip + np.where(d < ny, d, 0)) % ny) * CORES + core
    wave_number = (source % ny * CORES + (core + p) % CORES) * coefs + k
    angle = ((window * rows + r) * wave_number) % horizon * (2.0 * math.pi / horizon)
    scale = np.where(wave_number == 0, 1.0, 2.0) / horizon
    value = np.where(s == 0, np.cos(angle), -np.sin(angle)) * scale
    value = np.where((r < rows) & (k < coefs), value, 0.0)
    return value.reshape(ny * CORES, (2 * ny - 1) * rp, CORES * 2 * kp).astype(np.float32)


def local(
    ny,
    nm,
    spectrum,
    time_weights,
    interp_weights,
    group_block,
    group_count,
    wave_state,
    neighbors,
    coupling,
):
    coefs, points = spectrum.shape[1:]
    rows = time_weights.shape[1]
    horizon = rows * ny * CORES
    groups = interp_weights.shape[0]
    cell_rows = neighbors.shape[1]
    halo = HALO_CELLS // LANE
    blocks = points // LANE
    chunks = blocks // BLOCKS_PER_CHUNK
    kp, rp = pad(coefs, 8), pad(rows, 8)
    k_all, rb = CORES * 2 * kp, pad(rows, 16) + 16
    summed = chunks - RAW
    seg = 2 * BLOCKS_PER_CHUNK
    width = BLOCKS_PER_CHUNK * LANE

    spec = spectrum.reshape(2, coefs, blocks, LANE).transpose(1, 2, 0, 3)
    spec = spec.reshape(coefs, 2 * blocks, LANE)
    wave = wave_state.reshape(2, cell_rows, LANE).transpose(1, 0, 2).reshape(2 * cell_rows, LANE)
    coup = coupling.reshape(4, cell_rows, LANE).transpose(1, 0, 2).reshape(4 * cell_rows, LANE)
    basis = jnp.asarray(chip_basis(ny, coefs, rows, horizon))

    vmem = lambda *shape: pltpu.VMEM(shape, F32)
    dma = lambda *shape: pltpu.SemaphoreType.DMA(shape)
    smem = pl.BlockSpec(memory_space=pltpu.SMEM)
    hbm = pl.BlockSpec(memory_space=pltpu.HBM)
    on_chip = pl.BlockSpec(memory_space=pltpu.VMEM)
    far = max(ny - 1, 1)
    pinned = [
        pltpu.with_memory_space_constraint(x, pltpu.HBM)
        for x in (
            group_block,
            neighbors,
            time_weights,
            basis,
            spec,
            interp_weights,
            wave,
            coup,
        )
    ]
    outs = (
        jax.ShapeDtypeStruct((rows, points), F32),
        jax.ShapeDtypeStruct((2 * cell_rows, LANE), F32),
    )
    series, state = pl.pallas_call(
        functools.partial(kernel, (ny, nm, coefs, rows, chunks)),
        out_shape=outs,
        in_specs=[smem] + [hbm] * 8,
        out_specs=(on_chip, on_chip),
        scratch_shapes=[
            pltpu.SMEM(group_block.shape, jnp.int32),
            pltpu.SMEM(neighbors.shape, jnp.int32),
            vmem(2, rows),
            vmem((2 * ny - 1) * rp, k_all),
            vmem(16 * (2 * ny - 1), k_all),
            vmem(chunks, coefs, seg, LANE),
            vmem(chunks, coefs, seg, LANE),
            vmem(k_all, width),
            pltpu.VMEM((ny * rb, k_all), BF16),
            pltpu.VMEM((ny * rb, k_all), BF16),
            pltpu.VMEM((far, rb, k_all), BF16),
            pltpu.VMEM((far, rb, k_all), BF16),
            vmem(far, RAW, coefs, seg, LANE),
            vmem(far, RAW, coefs, seg, LANE),
            vmem(far, 2, rows),
            vmem(far, summed, BLOCKS_PER_CHUNK * rows, LANE),
            vmem(far, summed, BLOCKS_PER_CHUNK * rows, LANE),
            vmem(ny, 2, blocks, LANE),
            vmem(far, 2, summed * BLOCKS_PER_CHUNK, LANE),
            vmem(2, nm * blocks, LANE),
            vmem(2, groups, LANE),
            vmem(2, LANE, groups),
            vmem(2, LANE, groups),
            vmem(groups, LANE + 8, LANE),
            vmem(LANE * LANE, groups),
            vmem(2 * cell_rows, LANE),
            vmem(4 * cell_rows, LANE),
            vmem(2, 2 * halo, LANE),
            vmem(2, halo, LANE),
            vmem(cell_rows + 2 * halo, LANE),
            vmem(4, cell_rows, LANE),
            dma(far),
            dma(far, 2),
        ],
        compiler_params=pltpu.CompilerParams(
            collective_id=0, has_side_effects=True, vmem_limit_bytes=50000 * 1024
        ),
        name="adjoint",
    )(group_count, *pinned)
    series, state = pl.pallas_call(
        store,
        out_shape=outs,
        in_specs=[pl.BlockSpec(memory_space=pl.ANY)] * 2,
        out_specs=(hbm, hbm),
        scratch_shapes=[dma(2)],
        compiler_params=pltpu.CompilerParams(vmem_limit_bytes=1024 * 1024),
        name="store",
    )(series, state)
    new_state = state.reshape(cell_rows, 2, LANE).transpose(1, 0, 2)
    return series, new_state.reshape(1, 2, cell_rows * LANE)


def solution(mesh):
    placed = (
        P(None, "freq", "mesh"),
        P(None, "freq"),
        P("mesh", None, None),
        P("mesh"),
        P("mesh"),
        P("freq", None, "mesh"),
        P(None, "mesh"),
        P(None, "mesh"),
    )
    ny = mesh.shape["freq"] // CORES
    return jax.shard_map(
        functools.partial(local, ny, mesh.shape["mesh"]),
        mesh=mesh,
        in_specs=placed,
        out_specs=(P("freq", "mesh"), P("freq", None, "mesh")),
        check_vma=False,
    )
```

```python
import functools
import math

import jax
import jax.numpy as jnp
import numpy as np
from jax import lax
from jax.experimental import pallas as pl
from jax.experimental.pallas import tpu as pltpu
from jax.sharding import PartitionSpec as P

LANE = 128
CORES = 2
HALO_CELLS = 4096
BLOCKS_PER_CHUNK = 4
RAW = 2
PAIR = 2
HIGHEST = lax.Precision.HIGHEST
F32 = jnp.float32
BF16 = jnp.bfloat16


def pad(n, to):
    return (n + to - 1) // to * to


def split(x):
    high = x.astype(BF16)
    return high, (x - high.astype(F32)).astype(BF16)


def dot(a, b):
    return jnp.dot(a, b, preferred_element_type=F32)


def kernel(
    dims,
    count_smem,
    block_hbm,
    neigh_hbm,
    tw_hbm,
    basis_hbm,
    spec_hbm,
    weights_hbm,
    wave_hbm,
    coup_hbm,
    series,
    state,
    block_smem,
    neigh_smem,
    tw_own,
    basis_own,
    folded,
    own_spec,
    peer_spec,
    staged,
    lhs_high,
    lhs_low,
    cross_high,
    cross_low,
    raw,
    raw_peer,
    tw_all,
    outgoing,
    incoming,
    part,
    part_in,
    wall,
    picked,
    asked,
    turned,
    weights,
    lined,
    wave,
    coup,
    halo1,
    halo2,
    ext,
    gathered,
    ser_send,
    ser_recv,
):
    ny, nm, coefs, rows, chunks = dims
    groups = weights.shape[0]
    kp, rp, fb = pad(coefs, 8), pad(rows, 8), pad(rows, 16)
    rb = fb + 16
    m1 = ny * rp
    per = part.shape[2]
    cell_rows = ext.shape[0] - 2 * halo1.shape[1] // 2
    halo = halo1.shape[1] // 2
    width = BLOCKS_PER_CHUNK * LANE
    seg = 2 * BLOCKS_PER_CHUNK
    summed = chunks - RAW
    whole_rows = rows // 8 * 8
    rest = rows - whole_rows

    freq = lax.axis_index("freq")
    me = lax.axis_index("mesh")
    chip, core = freq // CORES, freq % CORES
    partner = chip * CORES + (1 - core)

    def at_chip(d):
        return ((chip + d + ny) % ny) * CORES + core

    def peer(d):
        return (me + d + nm) % nm

    def remote(src, dst, send, recv, axis, target):
        return pltpu.make_async_remote_copy(
            src_ref=src,
            dst_ref=dst,
            send_sem=send,
            recv_sem=recv,
            device_id={axis: target},
            device_id_type=pl.DeviceIdType.MESH,
        )

    def send_series(d, first, count):
        span = pl.ds(first, count)
        return remote(
            outgoing.at[d - 1, span],
            incoming.at[d - 1, span],
            ser_send.at[d - 1],
            ser_recv.at[d - 1, jnp.where(first == summed - 1, 1, 0)],
            "freq",
            at_chip(d),
        )

    def pieces(c):
        for j in range(BLOCKS_PER_CHUNK):
            lanes = pl.ds(pl.multiple_of(c * width + j * LANE, LANE), LANE)
            yield j, slice(0, whole_rows), slice(j * whole_rows, (j + 1) * whole_rows), lanes
            if rest:
                first = BLOCKS_PER_CHUNK * whole_rows + j * rest
                yield j, slice(whole_rows, rows), slice(first, first + rest), lanes

    def exchange(
        spec_sem,
        swap_send,
        swap_recv,
        load_sem,
        tw_send,
        tw_recv,
        raw_send,
        raw_recv,
        pass_send,
        pass_recv,
        part_send,
        part_recv,
        wall_send,
        wall_recv,
        halo_send,
        halo_recv,
        go,
        seen,
        peers_in,
        all_in,
    ):
        def load_spec(c):
            return pltpu.make_async_copy(
                spec_hbm.at[:, pl.ds(c * seg, seg), :],
                own_spec.at[c],
                spec_sem.at[1 if c >= summed else 0],
            )

        def loaded(first, count, sem):
            span = own_spec.at[pl.ds(first, count)]
            return pltpu.make_async_copy(span, span, spec_sem.at[sem])

        def swap(c):
            return remote(
                spec_hbm.at[:, pl.ds(c * seg, seg), :],
                peer_spec.at[c],
                swap_send.at[0],
                swap_recv.at[c // PAIR],
                "freq",
                partner,
            )

        def swapped(first, count):
            span = peer_spec.at[pl.ds(first, count)]
            return remote(span, span, swap_send.at[0], swap_recv.at[first // PAIR], "freq", partner)

        def send_tw(d):
            return remote(
                tw_hbm, tw_all.at[d - 1], tw_send.at[d - 1], tw_recv.at[d - 1], "freq", at_chip(-d)
            )

        def send_raw(d):
            return remote(
                spec_hbm.at[:, pl.ds(summed * seg, RAW * seg), :],
                raw.at[d - 1],
                raw_send.at[d - 1],
                raw_recv.at[d - 1],
                "freq",
                at_chip(d),
            )

        def send_raw_chunk(d, r):
            return remote(
                own_spec.at[summed + r],
                raw.at[d - 1, :, pl.ds(r * seg, seg), :],
                raw_send.at[d - 1],
                raw_recv.at[d - 1],
                "freq",
                at_chip(d),
            )

        def pass_raw(d):
            return remote(
                raw.at[d - 1],
                raw_peer.at[d - 1],
                pass_send.at[d - 1],
                pass_recv.at[d - 1],
                "freq",
                partner,
            )

        def send_part(d):
            return remote(
                part.at[d, :, pl.ds(0, summed * BLOCKS_PER_CHUNK), :],
                part_in.at[d - 1],
                part_send.at[d - 1],
                part_recv.at[d - 1],
                "freq",
                at_chip(d),
            )

        def send_wall(o):
            mine = wall.at[:, pl.ds(pl.multiple_of(me * per, 8), per), :]
            return remote(mine, mine, wall_send.at[0], wall_recv.at[0], "mesh", peer(o))

        def walled():
            span = wall.at[:, pl.ds(0, (nm - 1) * per), :]
            return remote(span, span, wall_send.at[0], wall_recv.at[0], "mesh", peer(1))

        def send_halo1(side):
            first = 0 if side else 2 * (cell_rows - halo)
            return remote(
                wave.at[pl.ds(first, 2 * halo)],
                halo1.at[side],
                halo_send.at[side],
                halo_recv.at[side],
                "mesh",
                peer(-1 if side else 1),
            )

        def send_halo2(side):
            first = halo if side else cell_rows
            return remote(
                ext.at[pl.ds(first, halo)],
                halo2.at[side],
                halo_send.at[2 + side],
                halo_recv.at[2 + side],
                "mesh",
                peer(-1 if side else 1),
            )

        inside = (me > 0, me < nm - 1)

        def halo_each(copy, method):
            for side in range(2):
                there = inside[side] if method == "wait_recv" else inside[1 - side]
                pl.when(there)(getattr(copy(side), method))

        def columns(c):
            return pl.ds(pl.multiple_of(c * width, width), width)

        load_wave = pltpu.make_async_copy(wave_hbm, wave, load_sem.at[0])
        load_coup = pltpu.make_async_copy(coup_hbm, coup, load_sem.at[1])
        load_weights = pltpu.make_async_copy(
            weights_hbm, weights.at[:, pl.ds(0, LANE), :], load_sem.at[2]
        )
        load_tw = pltpu.make_async_copy(tw_hbm, tw_own, load_sem.at[3])
        load_basis = pltpu.make_async_copy(basis_hbm.at[freq], basis_own, load_sem.at[4])
        load_neigh = pltpu.make_async_copy(neigh_hbm, neigh_smem, load_sem.at[5])
        load_block = pltpu.make_async_copy(block_hbm, block_smem, load_sem.at[6])

        barrier = pltpu.get_barrier_semaphore()
        first_core, first_chip = core == 0, chip == 0
        other_core, other_chip = core == 1, chip != 0

        def signal(sem, axis, target):
            pl.semaphore_signal(
                sem, inc=1, device_id={axis: target}, device_id_type=pl.DeviceIdType.MESH
            )

        @pl.when(first_core)
        def _():
            for d in range(1, ny):
                signal(barrier, "freq", at_chip(d))

        @pl.when(first_core == other_chip)
        def _():
            signal(barrier, "freq", partner)

        @pl.when(first_core & other_chip)
        def _():
            pl.semaphore_wait(barrier, ny - 1)
            for d in range(1, ny):
                send_tw(d).start()
                send_raw(d).start()

        load_tw.start()
        for c in (*range(summed, chunks), *range(summed)):
            load_spec(c).start()
        load_basis.start()
        load_wave.start()
        load_neigh.start()
        load_block.start()

        @pl.when(first_core & first_chip)
        def _():
            pl.semaphore_wait(barrier, ny)
            signal(go.at[0], "freq", partner)

        @pl.when(other_core & other_chip)
        def _():
            pl.semaphore_wait(barrier, 1)
            signal(go.at[0], "freq", partner)

        def send_loaded():
            loaded(summed, RAW, 1).wait()
            for d in range(1, ny):
                send_tw(d).start()
                for r in range(RAW):
                    send_raw_chunk(d, r).start()

        pl.when(first_core & first_chip)(send_loaded)

        @pl.when(first_core == other_chip)
        def _():
            pl.semaphore_wait(go.at[0], 1)

        for c in range(chunks):
            swap(c).start()

        @pl.when(first_core)
        def _():
            for d in range(1, ny):
                signal(seen.at[d - 1], "freq", at_chip(d))
            for d in range(1, ny):
                pl.semaphore_wait(seen.at[d - 1], 1)
            signal(peers_in.at[0], "freq", partner)

        @pl.when(other_core)
        def _():
            pl.semaphore_wait(peers_in.at[0], 1)
            send_loaded()

        @pl.when(other_core & first_chip)
        def _():
            for o in range(1, nm):
                signal(barrier, "mesh", peer(o))

        load_coup.start()
        load_weights.start()

        staged[...] = jnp.zeros_like(staged)
        folded[...] = jnp.zeros_like(folded)
        load_tw.wait()
        load_basis.wait()
        for d in range(ny):
            high, low = split(basis_own[d * rp : (d + 1) * rp, :])
            lhs_high[d * rb : d * rb + rp, :] = high
            lhs_low[d * rb : d * rb + rp, :] = low
        for d in range(1, ny):
            high, low = split(basis_own[m1 + (d - 1) * rp : m1 + d * rp, :])
            cross_high[d - 1, 0:rp, :] = high
            cross_low[d - 1, 0:rp, :] = low
        for d in range(2 * ny - 1):
            if 0 < d < ny:
                send_tw(d).wait_recv()
            folded[16 * d : 16 * d + 2, :] = jnp.dot(
                tw_all[d - 1] if 0 < d < ny else tw_own[...],
                basis_own[d * rp : d * rp + rows, :],
                precision=HIGHEST,
                preferred_element_type=F32,
            )
            high, low = split(folded[16 * d : 16 * (d + 1), :])
            if d < ny:
                lhs_high[d * rb + fb : (d + 1) * rb, :] = high
                lhs_low[d * rb + fb : (d + 1) * rb, :] = low
            else:
                cross_high[d - ny, fb:rb, :] = high
                cross_low[d - ny, fb:rb, :] = low

        own_rows = own_spec.reshape(chunks * coefs * seg, LANE)
        peer_rows = peer_spec.reshape(chunks * coefs * seg, LANE)
        far = max(ny - 1, 1)
        raw_rows = raw.reshape(far * RAW * coefs * seg, LANE)
        raw_peer_rows = raw_peer.reshape(far * RAW * coefs * seg, LANE)

        def stage(sources, first, step=seg):
            for p, source in enumerate(sources):
                for s in range(2):
                    for j in range(BLOCKS_PER_CHUNK):
                        piece = source[pl.ds(first + 2 * j + s, coefs, stride=step), :]
                        base = (p * 2 + s) * kp
                        staged[base : base + coefs, j * LANE : (j + 1) * LANE] = piece
            return split(staged[...])

        def product(high, low, s_high, s_low):
            return dot(high, s_high) + dot(low, s_high) + dot(high, s_low)

        def keep_part(c, total, d):
            for s in range(2):
                row = d * rb + fb + s
                for j in range(BLOCKS_PER_CHUNK):
                    part[d, s, pl.ds(c * BLOCKS_PER_CHUNK + j, 1), :] = total[
                        row : row + 1, j * LANE : (j + 1) * LANE
                    ]

        def summed_chunk(c, carry):
            @pl.when(c % PAIR == 0)
            def _():
                swapped(c, PAIR).wait_recv()

            s_high, s_low = stage((own_rows, peer_rows), c * (coefs * seg))
            total = product(lhs_high[...], lhs_low[...], s_high, s_low)
            series[:, columns(c)] = total[0:rows]
            keep_part(c, total, 0)
            for d in range(1, ny):
                keep_part(c, total, d)
                for j, take, put, _ in pieces(c):
                    outgoing[d - 1, c, put, :] = total[
                        d * rb + take.start : d * rb + take.stop, j * LANE : (j + 1) * LANE
                    ]
            return carry

        loaded(0, summed, 0).wait()

        @pl.when(first_core & other_chip)
        def _():
            loaded(summed, RAW, 1).wait()

        lax.fori_loop(0, summed, summed_chunk, 0)
        for d in range(1, ny):
            send_part(d).start()

        def send_chunk(c, carry):
            for d in range(1, ny):
                send_series(d, c, 1).start()
            return carry

        lax.fori_loop(0, summed, send_chunk, 0)

        def raw_chunk(c, carry):
            @pl.when(c % PAIR == 0)
            def _():
                swapped(c, PAIR).wait_recv()

            s_high, s_low = stage((own_rows, peer_rows), c * (coefs * seg))
            total = product(lhs_high[0:rb, :], lhs_low[0:rb, :], s_high, s_low)
            series[:, columns(c)] = total[0:rows]
            keep_part(c, total, 0)
            return carry

        lax.fori_loop(summed, chunks, raw_chunk, 0)

        @pl.when(other_core & first_chip)
        def _():
            pl.semaphore_wait(barrier, nm - 1)
            for d in range(ny):
                signal(all_in.at[0], "freq", d * CORES)
                if d:
                    signal(all_in.at[0], "freq", d * CORES + 1)

        @pl.when(first_core | other_chip)
        def _():
            pl.semaphore_wait(all_in.at[0], 1)

        load_wave.wait()
        halo_each(send_halo1, "start")

        pitch = weights.shape[1]
        weight_rows = weights.reshape(groups * pitch, LANE)
        load_weights.wait()

        def line_up(t, carry):
            for i in range(4):
                f = t * 4 + i
                lined[pl.ds(pl.multiple_of(f * LANE, LANE), LANE), :] = weight_rows[
                    pl.ds(f, groups, stride=pitch), :
                ].T
            return carry

        lax.fori_loop(0, LANE // 4, line_up, 0)

        for d in range(1, ny):
            send_raw(d).wait_recv()
            pass_raw(d).start()

        wave_rows = 64

        def stage_current(b, carry):
            at = b * wave_rows
            ext[pl.ds(halo + at, wave_rows), :] = wave[pl.ds(2 * at + 1, wave_rows, stride=2), :]
            return carry

        lax.fori_loop(0, cell_rows // wave_rows, stage_current, 0)

        load_neigh.wait()
        load_block.wait()

        def gather():
            def tile(t, carry):
                for n in range(4):
                    for i in range(8):
                        u = t * 8 + i
                        gathered[n, pl.ds(u, 1), :] = ext[pl.ds(neigh_smem[n, u], 1), :]
                return carry

            lax.fori_loop(0, cell_rows // 8, tile, 0)

        def spread_of(at, center):
            total = jnp.zeros((wave_rows, LANE), F32)
            for n in range(4):
                factor = coup[pl.ds(4 * at + n, wave_rows, stride=4), :]
                total += factor * (gathered[n, pl.ds(at, wave_rows), :] - center)
            return total

        inside_low = (jnp.zeros((halo, LANE), jnp.int32) + me) > 0
        inside_high = (jnp.zeros((halo, LANE), jnp.int32) + me) < nm - 1

        halo_each(send_halo1, "wait_recv")
        ext[0:halo, :] = jnp.where(inside_low, halo1[0, pl.ds(1, halo, stride=2), :], 0.0)
        ext[halo + cell_rows :, :] = jnp.where(
            inside_high, halo1[1, pl.ds(1, halo, stride=2), :], 0.0
        )
        load_coup.wait()
        gather()

        def first_step(b, carry):
            at = b * wave_rows
            center = ext[pl.ds(halo + at, wave_rows), :]
            previous = wave[pl.ds(2 * at, wave_rows, stride=2), :]
            state[pl.ds(2 * at, wave_rows, stride=2), :] = (
                2.0 * center - previous + spread_of(at, center)
            )
            return carry

        lax.fori_loop(0, cell_rows // wave_rows, first_step, 0)

        for d in range(1, ny):
            pass_raw(d).wait_recv()
        for r in range(RAW):
            c = summed + r
            total = series[:, columns(c)]
            extra = None
            for d in range(1, ny):
                s_high, s_low = stage(
                    (raw_rows, raw_peer_rows), ((d - 1) * coefs * RAW + r) * seg, RAW * seg
                )
                cross = product(cross_high[d - 1], cross_low[d - 1], s_high, s_low)
                total += cross[0:rows]
                extra = cross[fb : fb + 2] if extra is None else extra + cross[fb : fb + 2]
            series[:, columns(c)] = total
            if extra is not None:
                for s in range(2):
                    for j in range(BLOCKS_PER_CHUNK):
                        at = pl.ds(c * BLOCKS_PER_CHUNK + j, 1)
                        part[0, s, at, :] = (
                            part[0, s, at, :] + extra[s : s + 1, j * LANE : (j + 1) * LANE]
                        )

        for d in range(1, ny):
            send_part(d).wait_recv()
        first_blocks = summed * BLOCKS_PER_CHUNK
        base = pl.multiple_of(me * per, 8)
        for s in range(2):
            weighted = part[0, s, 0:first_blocks, :]
            for d in range(1, ny):
                weighted += part_in[d - 1, s]
            wall[s, pl.ds(base, first_blocks), :] = weighted
            wall[s, pl.ds(base + first_blocks, per - first_blocks), :] = part[0, s, first_blocks:, :]
        for o in range(1, nm):
            send_wall(o).start()
        walled().wait_recv()

        def pick(t, carry):
            for i in range(8):
                g = t * 8 + i
                block = block_smem[g]
                for s in range(2):
                    picked[s, pl.ds(g, 1), :] = wall[s, pl.ds(block, 1), :]
            return carry

        lax.fori_loop(0, groups // 8, pick, 0)
        for s in range(2):
            asked[s] = picked[s].T

        def interpolate(t, carry):
            faces = lined[pl.ds(pl.multiple_of(t * 8 * LANE, 8 * LANE), 8 * LANE), :]
            faces = faces.reshape(8, LANE, groups)
            for s in range(2):
                turned[s, pl.ds(pl.multiple_of(t * 8, 8), 8), :] = jnp.sum(
                    faces * asked[s][None], axis=1
                )
            return carry

        lax.fori_loop(0, LANE // 8, interpolate, 0)
        alive = lax.broadcasted_iota(jnp.int32, (groups, LANE), 0) < count_smem[0]
        push = [jnp.where(alive, turned[s].T, 0.0) for s in range(2)]

        top = pl.ds(0, groups, stride=2)
        state[top, :] = state[top, :] + push[0]

        def stage_stepped(b, carry):
            at = b * wave_rows
            ext[pl.ds(halo + at, wave_rows), :] = state[pl.ds(2 * at, wave_rows, stride=2), :]
            return carry

        lax.fori_loop(0, cell_rows // wave_rows, stage_stepped, 0)
        halo_each(send_halo2, "start")
        halo_each(send_halo2, "wait_recv")
        ext[0:halo, :] = jnp.where(inside_low, halo2[0], 0.0)
        ext[halo + cell_rows :, :] = jnp.where(inside_high, halo2[1], 0.0)
        gather()

        def second_step(b, carry):
            at = b * wave_rows
            center = ext[pl.ds(halo + at, wave_rows), :]
            previous = wave[pl.ds(2 * at + 1, wave_rows, stride=2), :]
            state[pl.ds(2 * at + 1, wave_rows, stride=2), :] = (
                2.0 * center - previous + spread_of(at, center)
            )
            return carry

        lax.fori_loop(0, cell_rows // wave_rows, second_step, 0)
        bottom = pl.ds(1, groups, stride=2)
        state[bottom, :] = state[bottom, :] + push[1]

        swapped(0, chunks).wait_send()
        walled().wait_send()
        for d in range(1, ny):
            send_raw(d).wait_send()
            pass_raw(d).wait_send()
            send_tw(d).wait_send()
            send_part(d).wait_send()
        halo_each(send_halo1, "wait_send")
        halo_each(send_halo2, "wait_send")

    dma = lambda *shape: pltpu.SemaphoreType.DMA(shape)
    regular = lambda *shape: pltpu.SemaphoreType.REGULAR(shape)
    far = max(ny - 1, 1)
    pl.run_scoped(
        exchange,
        dma(2),
        dma(1),
        dma(chunks // PAIR),
        dma(7),
        dma(far),
        dma(far),
        dma(far),
        dma(far),
        dma(far),
        dma(far),
        dma(far),
        dma(far),
        dma(1),
        dma(1),
        dma(4),
        dma(4),
        regular(1),
        regular(far),
        regular(1),
        regular(1),
    )

    def finish(c, carry):
        for d in range(1, ny):
            for _, take, put, lanes in pieces(c):
                series[take, lanes] = series[take, lanes] + incoming[d - 1, c, put, :]
        return carry

    last = summed - 1
    for d in range(1, ny):
        send_series(d, 0, last).wait_recv()
    lax.fori_loop(0, last, finish, 0)
    for d in range(1, ny):
        send_series(d, 0, summed).wait_send()
        send_series(d, last, 1).wait_recv()
    finish(last, 0)


def store(series, state, series_hbm, state_hbm, sem):
    copies = [
        pltpu.make_async_copy(series, series_hbm, sem.at[0]),
        pltpu.make_async_copy(state, state_hbm, sem.at[1]),
    ]
    for copy in copies:
        copy.start()
    for copy in copies:
        copy.wait()


def chip_basis(ny, coefs, rows, horizon):
    kp, rp = pad(coefs, 8), pad(rows, 8)
    freq = np.arange(ny * CORES).reshape(-1, 1, 1, 1, 1, 1)
    d, r, p, s, k = np.indices((2 * ny - 1, rp, CORES, 2, kp), sparse=True)
    chip, core = freq // CORES, freq % CORES
    source = chip - np.where(d < ny, 0, d - ny + 1)
    window = ((chip + np.where(d < ny, d, 0)) % ny) * CORES + core
    wave_number = (source % ny * CORES + (core + p) % CORES) * coefs + k
    angle = ((window * rows + r) * wave_number) % horizon * (2.0 * math.pi / horizon)
    scale = np.where(wave_number == 0, 1.0, 2.0) / horizon
    value = np.where(s == 0, np.cos(angle), -np.sin(angle)) * scale
    value = np.where((r < rows) & (k < coefs), value, 0.0)
    return value.reshape(ny * CORES, (2 * ny - 1) * rp, CORES * 2 * kp).astype(np.float32)


def local(
    ny,
    nm,
    spectrum,
    time_weights,
    interp_weights,
    group_block,
    group_count,
    wave_state,
    neighbors,
    coupling,
):
    coefs, points = spectrum.shape[1:]
    rows = time_weights.shape[1]
    horizon = rows * ny * CORES
    groups = interp_weights.shape[0]
    cell_rows = neighbors.shape[1]
    halo = HALO_CELLS // LANE
    blocks = points // LANE
    chunks = blocks // BLOCKS_PER_CHUNK
    kp, rp = pad(coefs, 8), pad(rows, 8)
    k_all, rb = CORES * 2 * kp, pad(rows, 16) + 16
    summed = chunks - RAW
    seg = 2 * BLOCKS_PER_CHUNK
    width = BLOCKS_PER_CHUNK * LANE

    spec = spectrum.reshape(2, coefs, blocks, LANE).transpose(1, 2, 0, 3)
    spec = spec.reshape(coefs, 2 * blocks, LANE)
    wave = wave_state.reshape(2, cell_rows, LANE).transpose(1, 0, 2).reshape(2 * cell_rows, LANE)
    coup = coupling.reshape(4, cell_rows, LANE).transpose(1, 0, 2).reshape(4 * cell_rows, LANE)
    basis = jnp.asarray(chip_basis(ny, coefs, rows, horizon))

    vmem = lambda *shape: pltpu.VMEM(shape, F32)
    dma = lambda *shape: pltpu.SemaphoreType.DMA(shape)
    smem = pl.BlockSpec(memory_space=pltpu.SMEM)
    hbm = pl.BlockSpec(memory_space=pltpu.HBM)
    on_chip = pl.BlockSpec(memory_space=pltpu.VMEM)
    far = max(ny - 1, 1)
    pinned = [
        pltpu.with_memory_space_constraint(x, pltpu.HBM)
        for x in (
            group_block,
            neighbors,
            time_weights,
            basis,
            spec,
            interp_weights,
            wave,
            coup,
        )
    ]
    outs = (
        jax.ShapeDtypeStruct((rows, points), F32),
        jax.ShapeDtypeStruct((2 * cell_rows, LANE), F32),
    )
    series, state = pl.pallas_call(
        functools.partial(kernel, (ny, nm, coefs, rows, chunks)),
        out_shape=outs,
        in_specs=[smem] + [hbm] * 8,
        out_specs=(on_chip, on_chip),
        scratch_shapes=[
            pltpu.SMEM(group_block.shape, jnp.int32),
            pltpu.SMEM(neighbors.shape, jnp.int32),
            vmem(2, rows),
            vmem((2 * ny - 1) * rp, k_all),
            vmem(16 * (2 * ny - 1), k_all),
            vmem(chunks, coefs, seg, LANE),
            vmem(chunks, coefs, seg, LANE),
            vmem(k_all, width),
            pltpu.VMEM((ny * rb, k_all), BF16),
            pltpu.VMEM((ny * rb, k_all), BF16),
            pltpu.VMEM((far, rb, k_all), BF16),
            pltpu.VMEM((far, rb, k_all), BF16),
            vmem(far, coefs, RAW * seg, LANE),
            vmem(far, coefs, RAW * seg, LANE),
            vmem(far, 2, rows),
            vmem(far, summed, BLOCKS_PER_CHUNK * rows, LANE),
            vmem(far, summed, BLOCKS_PER_CHUNK * rows, LANE),
            vmem(ny, 2, blocks, LANE),
            vmem(far, 2, summed * BLOCKS_PER_CHUNK, LANE),
            vmem(2, nm * blocks, LANE),
            vmem(2, groups, LANE),
            vmem(2, LANE, groups),
            vmem(2, LANE, groups),
            vmem(groups, LANE + 8, LANE),
            vmem(LANE * LANE, groups),
            vmem(2 * cell_rows, LANE),
            vmem(4 * cell_rows, LANE),
            vmem(2, 2 * halo, LANE),
            vmem(2, halo, LANE),
            vmem(cell_rows + 2 * halo, LANE),
            vmem(4, cell_rows, LANE),
            dma(far),
            dma(far, 2),
        ],
        compiler_params=pltpu.CompilerParams(
            collective_id=0, has_side_effects=True, vmem_limit_bytes=50000 * 1024
        ),
        name="adjoint",
    )(group_count, *pinned)
    series, state = pl.pallas_call(
        store,
        out_shape=outs,
        in_specs=[pl.BlockSpec(memory_space=pl.ANY)] * 2,
        out_specs=(hbm, hbm),
        scratch_shapes=[dma(2)],
        compiler_params=pltpu.CompilerParams(vmem_limit_bytes=1024 * 1024),
        name="store",
    )(series, state)
    new_state = state.reshape(cell_rows, 2, LANE).transpose(1, 0, 2)
    return series, new_state.reshape(1, 2, cell_rows * LANE)


def solution(mesh):
    placed = (
        P(None, "freq", "mesh"),
        P(None, "freq"),
        P("mesh", None, None),
        P("mesh"),
        P("mesh"),
        P("freq", None, "mesh"),
        P(None, "mesh"),
        P(None, "mesh"),
    )
    ny = mesh.shape["freq"] // CORES
    return jax.shard_map(
        functools.partial(local, ny, mesh.shape["mesh"]),
        mesh=mesh,
        in_specs=placed,
        out_specs=(P("freq", "mesh"), P("freq", None, "mesh")),
        check_vma=False,
    )
```

```python
import functools
import math

import jax
import jax.numpy as jnp
import numpy as np
from jax import lax
from jax.experimental import pallas as pl
from jax.experimental.pallas import tpu as pltpu
from jax.sharding import PartitionSpec as P

LANE = 128
CORES = 2
HALO_CELLS = 4096
BLOCKS_PER_CHUNK = 4
RAW = 2
PAIR = 2
HIGHEST = lax.Precision.HIGHEST
F32 = jnp.float32
BF16 = jnp.bfloat16


def pad(n, to):
    return (n + to - 1) // to * to


def split(x):
    high = x.astype(BF16)
    return high, (x - high.astype(F32)).astype(BF16)


def dot(a, b):
    return jnp.dot(a, b, preferred_element_type=F32)


def kernel(
    dims,
    count_smem,
    block_hbm,
    neigh_hbm,
    tw_hbm,
    basis_hbm,
    spec_hbm,
    weights_hbm,
    wave_hbm,
    coup_hbm,
    series,
    state,
    block_smem,
    neigh_smem,
    tw_own,
    basis_own,
    folded,
    own_spec,
    peer_spec,
    staged,
    lhs_high,
    lhs_low,
    cross_high,
    cross_low,
    raw,
    raw_peer,
    tw_all,
    outgoing,
    incoming,
    part,
    part_in,
    wall,
    picked,
    asked,
    turned,
    weights,
    lined,
    wave,
    coup,
    halo1,
    halo2,
    ext,
    gathered,
    ser_send,
    ser_recv,
):
    ny, nm, coefs, rows, chunks = dims
    groups = weights.shape[0]
    kp, rp, fb = pad(coefs, 8), pad(rows, 8), pad(rows, 16)
    rb = fb + 16
    m1 = ny * rp
    per = part.shape[2]
    cell_rows = ext.shape[0] - 2 * halo1.shape[1] // 2
    halo = halo1.shape[1] // 2
    width = BLOCKS_PER_CHUNK * LANE
    seg = 2 * BLOCKS_PER_CHUNK
    summed = chunks - RAW
    whole_rows = rows // 8 * 8
    rest = rows - whole_rows

    freq = lax.axis_index("freq")
    me = lax.axis_index("mesh")
    chip, core = freq // CORES, freq % CORES
    partner = chip * CORES + (1 - core)

    def at_chip(d):
        return ((chip + d + ny) % ny) * CORES + core

    def peer(d):
        return (me + d + nm) % nm

    def remote(src, dst, send, recv, axis, target):
        return pltpu.make_async_remote_copy(
            src_ref=src,
            dst_ref=dst,
            send_sem=send,
            recv_sem=recv,
            device_id={axis: target},
            device_id_type=pl.DeviceIdType.MESH,
        )

    def send_series(d, first, count):
        span = pl.ds(first, count)
        return remote(
            outgoing.at[d - 1, span],
            incoming.at[d - 1, span],
            ser_send.at[d - 1],
            ser_recv.at[d - 1, jnp.where(first == summed - 1, 1, 0)],
            "freq",
            at_chip(d),
        )

    def pieces(c):
        for j in range(BLOCKS_PER_CHUNK):
            lanes = pl.ds(pl.multiple_of(c * width + j * LANE, LANE), LANE)
            yield j, slice(0, whole_rows), slice(j * whole_rows, (j + 1) * whole_rows), lanes
            if rest:
                first = BLOCKS_PER_CHUNK * whole_rows + j * rest
                yield j, slice(whole_rows, rows), slice(first, first + rest), lanes

    def exchange(
        spec_sem,
        swap_send,
        swap_recv,
        load_sem,
        tw_send,
        tw_recv,
        raw_send,
        raw_recv,
        pass_send,
        pass_recv,
        part_send,
        part_recv,
        wall_send,
        wall_recv,
        halo_send,
        halo_recv,
        go,
        seen,
        all_in,
    ):
        def load_spec(c):
            return pltpu.make_async_copy(
                spec_hbm.at[:, pl.ds(c * seg, seg), :],
                own_spec.at[c],
                spec_sem.at[1 if c >= summed else 0],
            )

        def loaded(first, count, sem):
            span = own_spec.at[pl.ds(first, count)]
            return pltpu.make_async_copy(span, span, spec_sem.at[sem])

        def swap(c):
            return remote(
                own_spec.at[c],
                peer_spec.at[c],
                swap_send.at[0],
                swap_recv.at[c // PAIR],
                "freq",
                partner,
            )

        def swapped(first, count):
            span = peer_spec.at[pl.ds(first, count)]
            return remote(span, span, swap_send.at[0], swap_recv.at[first // PAIR], "freq", partner)

        def send_tw(d):
            return remote(
                tw_hbm, tw_all.at[d - 1], tw_send.at[d - 1], tw_recv.at[d - 1], "freq", at_chip(-d)
            )

        def send_raw(d):
            return remote(
                spec_hbm.at[:, pl.ds(summed * seg, RAW * seg), :],
                raw.at[d - 1],
                raw_send.at[d - 1],
                raw_recv.at[d - 1],
                "freq",
                at_chip(d),
            )

        def send_raw_chunk(d, r):
            return remote(
                own_spec.at[summed + r],
                raw.at[d - 1, :, pl.ds(r * seg, seg), :],
                raw_send.at[d - 1],
                raw_recv.at[d - 1],
                "freq",
                at_chip(d),
            )

        def pass_raw(d):
            return remote(
                raw.at[d - 1],
                raw_peer.at[d - 1],
                pass_send.at[d - 1],
                pass_recv.at[d - 1],
                "freq",
                partner,
            )

        def send_part(d):
            return remote(
                part.at[d, :, pl.ds(0, summed * BLOCKS_PER_CHUNK), :],
                part_in.at[d - 1],
                part_send.at[d - 1],
                part_recv.at[d - 1],
                "freq",
                at_chip(d),
            )

        def send_wall(o):
            mine = wall.at[:, pl.ds(pl.multiple_of(me * per, 8), per), :]
            return remote(mine, mine, wall_send.at[0], wall_recv.at[0], "mesh", peer(o))

        def walled():
            span = wall.at[:, pl.ds(0, (nm - 1) * per), :]
            return remote(span, span, wall_send.at[0], wall_recv.at[0], "mesh", peer(1))

        def send_halo1(side):
            first = 0 if side else 2 * (cell_rows - halo)
            return remote(
                wave.at[pl.ds(first, 2 * halo)],
                halo1.at[side],
                halo_send.at[side],
                halo_recv.at[side],
                "mesh",
                peer(-1 if side else 1),
            )

        def send_halo2(side):
            first = halo if side else cell_rows
            return remote(
                ext.at[pl.ds(first, halo)],
                halo2.at[side],
                halo_send.at[2 + side],
                halo_recv.at[2 + side],
                "mesh",
                peer(-1 if side else 1),
            )

        inside = (me > 0, me < nm - 1)

        def halo_each(copy, method):
            for side in range(2):
                there = inside[side] if method == "wait_recv" else inside[1 - side]
                pl.when(there)(getattr(copy(side), method))

        def columns(c):
            return pl.ds(pl.multiple_of(c * width, width), width)

        load_wave = pltpu.make_async_copy(wave_hbm, wave, load_sem.at[0])
        load_coup = pltpu.make_async_copy(coup_hbm, coup, load_sem.at[1])
        load_weights = pltpu.make_async_copy(
            weights_hbm, weights.at[:, pl.ds(0, LANE), :], load_sem.at[2]
        )
        load_tw = pltpu.make_async_copy(tw_hbm, tw_own, load_sem.at[3])
        load_basis = pltpu.make_async_copy(basis_hbm.at[freq], basis_own, load_sem.at[4])
        load_neigh = pltpu.make_async_copy(neigh_hbm, neigh_smem, load_sem.at[5])
        load_block = pltpu.make_async_copy(block_hbm, block_smem, load_sem.at[6])

        barrier = pltpu.get_barrier_semaphore()
        first_core, first_chip = core == 0, chip == 0
        other_core, other_chip = core == 1, chip != 0

        def signal(sem, axis, target):
            pl.semaphore_signal(
                sem, inc=1, device_id={axis: target}, device_id_type=pl.DeviceIdType.MESH
            )

        for d in range(1, ny):
            at_first = at_chip(d) < CORES

            @pl.when(first_core | jnp.logical_not(at_first))
            def _():
                signal(barrier, "freq", at_chip(d))

        @pl.when(other_core)
        def _():
            signal(barrier, "freq", partner)

        @pl.when(other_chip)
        def _():
            pl.semaphore_wait(barrier, jnp.where(first_core, ny, ny - 1))
            for d in range(1, ny):
                send_tw(d).start()
                send_raw(d).start()

        @pl.when(other_core & other_chip)
        def _():
            signal(seen.at[chip - 1], "freq", 1)

        load_tw.start()
        for c in (*range(summed, chunks), *range(summed)):
            load_spec(c).start()
        load_basis.start()
        load_wave.start()
        load_neigh.start()
        load_block.start()

        @pl.when(first_chip)
        def _():
            @pl.when(first_core)
            def _():
                pl.semaphore_wait(barrier, ny)

            @pl.when(other_core)
            def _():
                for d in range(1, ny):
                    pl.semaphore_wait(seen.at[d - 1], 1)

            loaded(summed, RAW, 1).wait()
            for d in range(1, ny):
                send_tw(d).start()
                for r in range(RAW):
                    send_raw_chunk(d, r).start()

        @pl.when(first_core)
        def _():
            signal(go.at[0], "freq", partner)

        @pl.when(other_core)
        def _():
            pl.semaphore_wait(go.at[0], 1)

        loaded(0, summed, 0).wait()

        @pl.when(other_chip)
        def _():
            loaded(summed, RAW, 1).wait()

        for c in range(chunks):
            swap(c).start()

        @pl.when(other_core & first_chip)
        def _():
            for o in range(1, nm):
                signal(barrier, "mesh", peer(o))

        load_coup.start()
        load_weights.start()

        staged[...] = jnp.zeros_like(staged)
        folded[...] = jnp.zeros_like(folded)
        load_tw.wait()
        load_basis.wait()
        for d in range(ny):
            high, low = split(basis_own[d * rp : (d + 1) * rp, :])
            lhs_high[d * rb : d * rb + rp, :] = high
            lhs_low[d * rb : d * rb + rp, :] = low
        for d in range(1, ny):
            high, low = split(basis_own[m1 + (d - 1) * rp : m1 + d * rp, :])
            cross_high[d - 1, 0:rp, :] = high
            cross_low[d - 1, 0:rp, :] = low
        for d in range(2 * ny - 1):
            if 0 < d < ny:
                send_tw(d).wait_recv()
            folded[16 * d : 16 * d + 2, :] = jnp.dot(
                tw_all[d - 1] if 0 < d < ny else tw_own[...],
                basis_own[d * rp : d * rp + rows, :],
                precision=HIGHEST,
                preferred_element_type=F32,
            )
            high, low = split(folded[16 * d : 16 * (d + 1), :])
            if d < ny:
                lhs_high[d * rb + fb : (d + 1) * rb, :] = high
                lhs_low[d * rb + fb : (d + 1) * rb, :] = low
            else:
                cross_high[d - ny, fb:rb, :] = high
                cross_low[d - ny, fb:rb, :] = low

        own_rows = own_spec.reshape(chunks * coefs * seg, LANE)
        peer_rows = peer_spec.reshape(chunks * coefs * seg, LANE)
        far = max(ny - 1, 1)
        raw_rows = raw.reshape(far * RAW * coefs * seg, LANE)
        raw_peer_rows = raw_peer.reshape(far * RAW * coefs * seg, LANE)

        def stage(sources, first, step=seg):
            for p, source in enumerate(sources):
                for s in range(2):
                    for j in range(BLOCKS_PER_CHUNK):
                        piece = source[pl.ds(first + 2 * j + s, coefs, stride=step), :]
                        base = (p * 2 + s) * kp
                        staged[base : base + coefs, j * LANE : (j + 1) * LANE] = piece
            return split(staged[...])

        def product(high, low, s_high, s_low):
            return dot(high, s_high) + dot(low, s_high) + dot(high, s_low)

        def keep_part(c, total, d):
            for s in range(2):
                row = d * rb + fb + s
                for j in range(BLOCKS_PER_CHUNK):
                    part[d, s, pl.ds(c * BLOCKS_PER_CHUNK + j, 1), :] = total[
                        row : row + 1, j * LANE : (j + 1) * LANE
                    ]

        def summed_chunk(c, carry):
            @pl.when(c % PAIR == 0)
            def _():
                swapped(c, PAIR).wait_recv()

            s_high, s_low = stage((own_rows, peer_rows), c * (coefs * seg))
            total = product(lhs_high[...], lhs_low[...], s_high, s_low)
            series[:, columns(c)] = total[0:rows]
            keep_part(c, total, 0)
            for d in range(1, ny):
                keep_part(c, total, d)
                for j, take, put, _ in pieces(c):
                    outgoing[d - 1, c, put, :] = total[
                        d * rb + take.start : d * rb + take.stop, j * LANE : (j + 1) * LANE
                    ]
            return carry

        lax.fori_loop(0, summed, summed_chunk, 0)
        for d in range(1, ny):
            send_part(d).start()

        def send_chunk(c, carry):
            for d in range(1, ny):
                send_series(d, c, 1).start()
            return carry

        lax.fori_loop(0, summed, send_chunk, 0)

        def raw_chunk(c, carry):
            @pl.when(c % PAIR == 0)
            def _():
                swapped(c, PAIR).wait_recv()

            s_high, s_low = stage((own_rows, peer_rows), c * (coefs * seg))
            total = product(lhs_high[0:rb, :], lhs_low[0:rb, :], s_high, s_low)
            series[:, columns(c)] = total[0:rows]
            keep_part(c, total, 0)
            return carry

        lax.fori_loop(summed, chunks, raw_chunk, 0)

        @pl.when(other_core & first_chip)
        def _():
            pl.semaphore_wait(barrier, nm - 1)
            for d in range(ny):
                signal(all_in.at[0], "freq", d * CORES)
                if d:
                    signal(all_in.at[0], "freq", d * CORES + 1)

        @pl.when(first_core | other_chip)
        def _():
            pl.semaphore_wait(all_in.at[0], 1)

        load_wave.wait()
        halo_each(send_halo1, "start")

        pitch = weights.shape[1]
        weight_rows = weights.reshape(groups * pitch, LANE)
        load_weights.wait()

        def line_up(t, carry):
            for i in range(4):
                f = t * 4 + i
                lined[pl.ds(pl.multiple_of(f * LANE, LANE), LANE), :] = weight_rows[
                    pl.ds(f, groups, stride=pitch), :
                ].T
            return carry

        lax.fori_loop(0, LANE // 4, line_up, 0)

        for d in range(1, ny):
            send_raw(d).wait_recv()
            pass_raw(d).start()

        wave_rows = 64

        def stage_current(b, carry):
            at = b * wave_rows
            ext[pl.ds(halo + at, wave_rows), :] = wave[pl.ds(2 * at + 1, wave_rows, stride=2), :]
            return carry

        lax.fori_loop(0, cell_rows // wave_rows, stage_current, 0)

        load_neigh.wait()
        load_block.wait()

        def gather():
            def tile(t, carry):
                for n in range(4):
                    for i in range(8):
                        u = t * 8 + i
                        gathered[n, pl.ds(u, 1), :] = ext[pl.ds(neigh_smem[n, u], 1), :]
                return carry

            lax.fori_loop(0, cell_rows // 8, tile, 0)

        def spread_of(at, center):
            total = jnp.zeros((wave_rows, LANE), F32)
            for n in range(4):
                factor = coup[pl.ds(4 * at + n, wave_rows, stride=4), :]
                total += factor * (gathered[n, pl.ds(at, wave_rows), :] - center)
            return total

        inside_low = (jnp.zeros((halo, LANE), jnp.int32) + me) > 0
        inside_high = (jnp.zeros((halo, LANE), jnp.int32) + me) < nm - 1

        halo_each(send_halo1, "wait_recv")
        ext[0:halo, :] = jnp.where(inside_low, halo1[0, pl.ds(1, halo, stride=2), :], 0.0)
        ext[halo + cell_rows :, :] = jnp.where(
            inside_high, halo1[1, pl.ds(1, halo, stride=2), :], 0.0
        )
        load_coup.wait()
        gather()

        def first_step(b, carry):
            at = b * wave_rows
            center = ext[pl.ds(halo + at, wave_rows), :]
            previous = wave[pl.ds(2 * at, wave_rows, stride=2), :]
            state[pl.ds(2 * at, wave_rows, stride=2), :] = (
                2.0 * center - previous + spread_of(at, center)
            )
            return carry

        lax.fori_loop(0, cell_rows // wave_rows, first_step, 0)

        for d in range(1, ny):
            pass_raw(d).wait_recv()
        for r in range(RAW):
            c = summed + r
            total = series[:, columns(c)]
            extra = None
            for d in range(1, ny):
                s_high, s_low = stage(
                    (raw_rows, raw_peer_rows), ((d - 1) * coefs * RAW + r) * seg, RAW * seg
                )
                cross = product(cross_high[d - 1], cross_low[d - 1], s_high, s_low)
                total += cross[0:rows]
                extra = cross[fb : fb + 2] if extra is None else extra + cross[fb : fb + 2]
            series[:, columns(c)] = total
            if extra is not None:
                for s in range(2):
                    for j in range(BLOCKS_PER_CHUNK):
                        at = pl.ds(c * BLOCKS_PER_CHUNK + j, 1)
                        part[0, s, at, :] = (
                            part[0, s, at, :] + extra[s : s + 1, j * LANE : (j + 1) * LANE]
                        )

        for d in range(1, ny):
            send_part(d).wait_recv()
        first_blocks = summed * BLOCKS_PER_CHUNK
        base = pl.multiple_of(me * per, 8)
        for s in range(2):
            weighted = part[0, s, 0:first_blocks, :]
            for d in range(1, ny):
                weighted += part_in[d - 1, s]
            wall[s, pl.ds(base, first_blocks), :] = weighted
            wall[s, pl.ds(base + first_blocks, per - first_blocks), :] = part[0, s, first_blocks:, :]
        for o in range(1, nm):
            send_wall(o).start()
        walled().wait_recv()

        def pick(t, carry):
            for i in range(8):
                g = t * 8 + i
                block = block_smem[g]
                for s in range(2):
                    picked[s, pl.ds(g, 1), :] = wall[s, pl.ds(block, 1), :]
            return carry

        lax.fori_loop(0, groups // 8, pick, 0)
        for s in range(2):
            asked[s] = picked[s].T

        def interpolate(t, carry):
            faces = lined[pl.ds(pl.multiple_of(t * 8 * LANE, 8 * LANE), 8 * LANE), :]
            faces = faces.reshape(8, LANE, groups)
            for s in range(2):
                turned[s, pl.ds(pl.multiple_of(t * 8, 8), 8), :] = jnp.sum(
                    faces * asked[s][None], axis=1
                )
            return carry

        lax.fori_loop(0, LANE // 8, interpolate, 0)
        alive = lax.broadcasted_iota(jnp.int32, (groups, LANE), 0) < count_smem[0]
        push = [jnp.where(alive, turned[s].T, 0.0) for s in range(2)]

        top = pl.ds(0, groups, stride=2)
        state[top, :] = state[top, :] + push[0]

        def stage_stepped(b, carry):
            at = b * wave_rows
            ext[pl.ds(halo + at, wave_rows), :] = state[pl.ds(2 * at, wave_rows, stride=2), :]
            return carry

        lax.fori_loop(0, cell_rows // wave_rows, stage_stepped, 0)
        halo_each(send_halo2, "start")
        halo_each(send_halo2, "wait_recv")
        ext[0:halo, :] = jnp.where(inside_low, halo2[0], 0.0)
        ext[halo + cell_rows :, :] = jnp.where(inside_high, halo2[1], 0.0)
        gather()

        def second_step(b, carry):
            at = b * wave_rows
            center = ext[pl.ds(halo + at, wave_rows), :]
            previous = wave[pl.ds(2 * at + 1, wave_rows, stride=2), :]
            state[pl.ds(2 * at + 1, wave_rows, stride=2), :] = (
                2.0 * center - previous + spread_of(at, center)
            )
            return carry

        lax.fori_loop(0, cell_rows // wave_rows, second_step, 0)
        bottom = pl.ds(1, groups, stride=2)
        state[bottom, :] = state[bottom, :] + push[1]

        swapped(0, chunks).wait_send()
        walled().wait_send()
        for d in range(1, ny):
            send_raw(d).wait_send()
            pass_raw(d).wait_send()
            send_tw(d).wait_send()
            send_part(d).wait_send()
        halo_each(send_halo1, "wait_send")
        halo_each(send_halo2, "wait_send")

    dma = lambda *shape: pltpu.SemaphoreType.DMA(shape)
    regular = lambda *shape: pltpu.SemaphoreType.REGULAR(shape)
    far = max(ny - 1, 1)
    pl.run_scoped(
        exchange,
        dma(2),
        dma(1),
        dma(chunks // PAIR),
        dma(7),
        dma(far),
        dma(far),
        dma(far),
        dma(far),
        dma(far),
        dma(far),
        dma(far),
        dma(far),
        dma(1),
        dma(1),
        dma(4),
        dma(4),
        regular(1),
        regular(far),
        regular(1),
    )

    def finish(c, carry):
        for d in range(1, ny):
            for _, take, put, lanes in pieces(c):
                series[take, lanes] = series[take, lanes] + incoming[d - 1, c, put, :]
        return carry

    last = summed - 1
    for d in range(1, ny):
        send_series(d, 0, last).wait_recv()
    lax.fori_loop(0, last, finish, 0)
    for d in range(1, ny):
        send_series(d, 0, summed).wait_send()
        send_series(d, last, 1).wait_recv()
    finish(last, 0)


def store(series, state, series_hbm, state_hbm, sem):
    copies = [
        pltpu.make_async_copy(series, series_hbm, sem.at[0]),
        pltpu.make_async_copy(state, state_hbm, sem.at[1]),
    ]
    for copy in copies:
        copy.start()
    for copy in copies:
        copy.wait()


def chip_basis(ny, coefs, rows, horizon):
    kp, rp = pad(coefs, 8), pad(rows, 8)
    freq = np.arange(ny * CORES).reshape(-1, 1, 1, 1, 1, 1)
    d, r, p, s, k = np.indices((2 * ny - 1, rp, CORES, 2, kp), sparse=True)
    chip, core = freq // CORES, freq % CORES
    source = chip - np.where(d < ny, 0, d - ny + 1)
    window = ((chip + np.where(d < ny, d, 0)) % ny) * CORES + core
    wave_number = (source % ny * CORES + (core + p) % CORES) * coefs + k
    angle = ((window * rows + r) * wave_number) % horizon * (2.0 * math.pi / horizon)
    scale = np.where(wave_number == 0, 1.0, 2.0) / horizon
    value = np.where(s == 0, np.cos(angle), -np.sin(angle)) * scale
    value = np.where((r < rows) & (k < coefs), value, 0.0)
    return value.reshape(ny * CORES, (2 * ny - 1) * rp, CORES * 2 * kp).astype(np.float32)


def local(
    ny,
    nm,
    spectrum,
    time_weights,
    interp_weights,
    group_block,
    group_count,
    wave_state,
    neighbors,
    coupling,
):
    coefs, points = spectrum.shape[1:]
    rows = time_weights.shape[1]
    horizon = rows * ny * CORES
    groups = interp_weights.shape[0]
    cell_rows = neighbors.shape[1]
    halo = HALO_CELLS // LANE
    blocks = points // LANE
    chunks = blocks // BLOCKS_PER_CHUNK
    kp, rp = pad(coefs, 8), pad(rows, 8)
    k_all, rb = CORES * 2 * kp, pad(rows, 16) + 16
    summed = chunks - RAW
    seg = 2 * BLOCKS_PER_CHUNK
    width = BLOCKS_PER_CHUNK * LANE

    spec = spectrum.reshape(2, coefs, blocks, LANE).transpose(1, 2, 0, 3)
    spec = spec.reshape(coefs, 2 * blocks, LANE)
    wave = wave_state.reshape(2, cell_rows, LANE).transpose(1, 0, 2).reshape(2 * cell_rows, LANE)
    coup = coupling.reshape(4, cell_rows, LANE).transpose(1, 0, 2).reshape(4 * cell_rows, LANE)
    basis = jnp.asarray(chip_basis(ny, coefs, rows, horizon))

    vmem = lambda *shape: pltpu.VMEM(shape, F32)
    dma = lambda *shape: pltpu.SemaphoreType.DMA(shape)
    smem = pl.BlockSpec(memory_space=pltpu.SMEM)
    hbm = pl.BlockSpec(memory_space=pltpu.HBM)
    on_chip = pl.BlockSpec(memory_space=pltpu.VMEM)
    far = max(ny - 1, 1)
    pinned = [
        pltpu.with_memory_space_constraint(x, pltpu.HBM)
        for x in (
            group_block,
            neighbors,
            time_weights,
            basis,
            spec,
            interp_weights,
            wave,
            coup,
        )
    ]
    outs = (
        jax.ShapeDtypeStruct((rows, points), F32),
        jax.ShapeDtypeStruct((2 * cell_rows, LANE), F32),
    )
    series, state = pl.pallas_call(
        functools.partial(kernel, (ny, nm, coefs, rows, chunks)),
        out_shape=outs,
        in_specs=[smem] + [hbm] * 8,
        out_specs=(on_chip, on_chip),
        scratch_shapes=[
            pltpu.SMEM(group_block.shape, jnp.int32),
            pltpu.SMEM(neighbors.shape, jnp.int32),
            vmem(2, rows),
            vmem((2 * ny - 1) * rp, k_all),
            vmem(16 * (2 * ny - 1), k_all),
            vmem(chunks, coefs, seg, LANE),
            vmem(chunks, coefs, seg, LANE),
            vmem(k_all, width),
            pltpu.VMEM((ny * rb, k_all), BF16),
            pltpu.VMEM((ny * rb, k_all), BF16),
            pltpu.VMEM((far, rb, k_all), BF16),
            pltpu.VMEM((far, rb, k_all), BF16),
            vmem(far, coefs, RAW * seg, LANE),
            vmem(far, coefs, RAW * seg, LANE),
            vmem(far, 2, rows),
            vmem(far, summed, BLOCKS_PER_CHUNK * rows, LANE),
            vmem(far, summed, BLOCKS_PER_CHUNK * rows, LANE),
            vmem(ny, 2, blocks, LANE),
            vmem(far, 2, summed * BLOCKS_PER_CHUNK, LANE),
            vmem(2, nm * blocks, LANE),
            vmem(2, groups, LANE),
            vmem(2, LANE, groups),
            vmem(2, LANE, groups),
            vmem(groups, LANE + 8, LANE),
            vmem(LANE * LANE, groups),
            vmem(2 * cell_rows, LANE),
            vmem(4 * cell_rows, LANE),
            vmem(2, 2 * halo, LANE),
            vmem(2, halo, LANE),
            vmem(cell_rows + 2 * halo, LANE),
            vmem(4, cell_rows, LANE),
            dma(far),
            dma(far, 2),
        ],
        compiler_params=pltpu.CompilerParams(
            collective_id=0, has_side_effects=True, vmem_limit_bytes=50000 * 1024
        ),
        name="adjoint",
    )(group_count, *pinned)
    series, state = pl.pallas_call(
        store,
        out_shape=outs,
        in_specs=[pl.BlockSpec(memory_space=pl.ANY)] * 2,
        out_specs=(hbm, hbm),
        scratch_shapes=[dma(2)],
        compiler_params=pltpu.CompilerParams(vmem_limit_bytes=1024 * 1024),
        name="store",
    )(series, state)
    new_state = state.reshape(cell_rows, 2, LANE).transpose(1, 0, 2)
    return series, new_state.reshape(1, 2, cell_rows * LANE)


def solution(mesh):
    placed = (
        P(None, "freq", "mesh"),
        P(None, "freq"),
        P("mesh", None, None),
        P("mesh"),
        P("mesh"),
        P("freq", None, "mesh"),
        P(None, "mesh"),
        P(None, "mesh"),
    )
    ny = mesh.shape["freq"] // CORES
    return jax.shard_map(
        functools.partial(local, ny, mesh.shape["mesh"]),
        mesh=mesh,
        in_specs=placed,
        out_specs=(P("freq", "mesh"), P("freq", None, "mesh")),
        check_vma=False,
    )
```

```python
import functools
import math

import jax
import jax.numpy as jnp
import numpy as np
from jax import lax
from jax.experimental import pallas as pl
from jax.experimental.pallas import tpu as pltpu
from jax.sharding import PartitionSpec as P

LANE = 128
CORES = 2
HALO_CELLS = 4096
BLOCKS_PER_CHUNK = 4
RAW = 2
PAIR = 2
HIGHEST = lax.Precision.HIGHEST
F32 = jnp.float32
BF16 = jnp.bfloat16


def pad(n, to):
    return (n + to - 1) // to * to


def split(x):
    high = x.astype(BF16)
    return high, (x - high.astype(F32)).astype(BF16)


def dot(a, b):
    return jnp.dot(a, b, preferred_element_type=F32)


def kernel(
    dims,
    count_smem,
    block_hbm,
    neigh_hbm,
    tw_hbm,
    basis_hbm,
    spec_hbm,
    weights_hbm,
    wave_hbm,
    coup_hbm,
    series,
    state,
    block_smem,
    neigh_smem,
    tw_own,
    basis_own,
    folded,
    own_spec,
    peer_spec,
    staged,
    lhs_high,
    lhs_low,
    cross_high,
    cross_low,
    raw,
    raw_peer,
    tw_all,
    outgoing,
    incoming,
    part,
    part_in,
    aside,
    wall,
    picked,
    asked,
    turned,
    weights,
    lined,
    wave,
    coup,
    halo1,
    halo2,
    ext,
    gathered,
    ser_send,
    ser_recv,
):
    ny, nm, coefs, rows, chunks = dims
    groups = weights.shape[0]
    kp, rp, fb = pad(coefs, 8), pad(rows, 8), pad(rows, 16)
    rb = fb + 16
    m1 = ny * rp
    per = part.shape[2]
    cell_rows = ext.shape[0] - 2 * halo1.shape[1] // 2
    halo = halo1.shape[1] // 2
    width = BLOCKS_PER_CHUNK * LANE
    seg = 2 * BLOCKS_PER_CHUNK
    summed = chunks - RAW
    whole_rows = rows // 8 * 8
    rest = rows - whole_rows

    freq = lax.axis_index("freq")
    me = lax.axis_index("mesh")
    chip, core = freq // CORES, freq % CORES
    partner = chip * CORES + (1 - core)

    def at_chip(d):
        return ((chip + d + ny) % ny) * CORES + core

    def peer(d):
        return (me + d + nm) % nm

    def remote(src, dst, send, recv, axis, target):
        return pltpu.make_async_remote_copy(
            src_ref=src,
            dst_ref=dst,
            send_sem=send,
            recv_sem=recv,
            device_id={axis: target},
            device_id_type=pl.DeviceIdType.MESH,
        )

    def send_series(d, first, count):
        span = pl.ds(first, count)
        return remote(
            outgoing.at[d - 1, span],
            incoming.at[d - 1, span],
            ser_send.at[d - 1],
            ser_recv.at[d - 1, jnp.where(first == summed - 1, 1, 0)],
            "freq",
            at_chip(d),
        )

    def pieces(c):
        for j in range(BLOCKS_PER_CHUNK):
            lanes = pl.ds(pl.multiple_of(c * width + j * LANE, LANE), LANE)
            yield j, slice(0, whole_rows), slice(j * whole_rows, (j + 1) * whole_rows), lanes
            if rest:
                first = BLOCKS_PER_CHUNK * whole_rows + j * rest
                yield j, slice(whole_rows, rows), slice(first, first + rest), lanes

    def exchange(
        spec_sem,
        swap_send,
        swap_recv,
        load_sem,
        tw_send,
        tw_recv,
        raw_send,
        raw_recv,
        pass_send,
        pass_recv,
        part_send,
        part_recv,
        aside_send,
        aside_recv,
        on_send,
        wall_send,
        wall_recv,
        halo_send,
        halo_recv,
        go,
        seen,
        all_in,
    ):
        def load_spec(c):
            return pltpu.make_async_copy(
                spec_hbm.at[:, pl.ds(c * seg, seg), :],
                own_spec.at[c],
                spec_sem.at[1 if c >= summed else 0],
            )

        def loaded(first, count, sem):
            span = own_spec.at[pl.ds(first, count)]
            return pltpu.make_async_copy(span, span, spec_sem.at[sem])

        def swap(c):
            return remote(
                own_spec.at[c],
                peer_spec.at[c],
                swap_send.at[0],
                swap_recv.at[c // PAIR],
                "freq",
                partner,
            )

        def swapped(first, count):
            span = peer_spec.at[pl.ds(first, count)]
            return remote(span, span, swap_send.at[0], swap_recv.at[first // PAIR], "freq", partner)

        def send_tw(d):
            return remote(
                tw_hbm, tw_all.at[d - 1], tw_send.at[d - 1], tw_recv.at[d - 1], "freq", at_chip(-d)
            )

        def send_raw(d):
            return remote(
                spec_hbm.at[:, pl.ds(summed * seg, RAW * seg), :],
                raw.at[d - 1],
                raw_send.at[d - 1],
                raw_recv.at[d - 1],
                "freq",
                at_chip(d),
            )

        def send_raw_chunk(d, r):
            return remote(
                own_spec.at[summed + r],
                raw.at[d - 1, :, pl.ds(r * seg, seg), :],
                raw_send.at[d - 1],
                raw_recv.at[d - 1],
                "freq",
                at_chip(d),
            )

        def pass_raw(d):
            return remote(
                raw.at[d - 1],
                raw_peer.at[d - 1],
                pass_send.at[d - 1],
                pass_recv.at[d - 1],
                "freq",
                partner,
            )

        def send_part(d):
            return remote(
                part.at[d, :, pl.ds(0, summed * BLOCKS_PER_CHUNK), :],
                part_in.at[d - 1],
                part_send.at[d - 1],
                part_recv.at[d - 1],
                "freq",
                at_chip(d),
            )

        def detoured(d):
            return (me == 0) & ((chip + d) % ny == 0)

        def passes():
            return (me == 1 + core) & (chip == 0)

        def send_aside(d):
            return pltpu.make_async_remote_copy(
                src_ref=part.at[d, :, pl.ds(0, summed * BLOCKS_PER_CHUNK), :],
                dst_ref=aside.at[d - 1],
                send_sem=aside_send.at[d - 1],
                recv_sem=aside_recv.at[d - 1],
                device_id={"freq": at_chip(d), "mesh": 1 + core},
                device_id_type=pl.DeviceIdType.MESH,
            )

        def send_on(d):
            return remote(
                aside.at[d - 1],
                part_in.at[d - 1],
                on_send.at[d - 1],
                part_recv.at[d - 1],
                "mesh",
                0,
            )

        def send_wall(o):
            mine = wall.at[:, pl.ds(pl.multiple_of(me * per, 8), per), :]
            return remote(mine, mine, wall_send.at[0], wall_recv.at[0], "mesh", peer(o))

        def walled():
            span = wall.at[:, pl.ds(0, (nm - 1) * per), :]
            return remote(span, span, wall_send.at[0], wall_recv.at[0], "mesh", peer(1))

        def send_halo1(side):
            first = 0 if side else 2 * (cell_rows - halo)
            return remote(
                wave.at[pl.ds(first, 2 * halo)],
                halo1.at[side],
                halo_send.at[side],
                halo_recv.at[side],
                "mesh",
                peer(-1 if side else 1),
            )

        def send_halo2(side):
            first = halo if side else cell_rows
            return remote(
                ext.at[pl.ds(first, halo)],
                halo2.at[side],
                halo_send.at[2 + side],
                halo_recv.at[2 + side],
                "mesh",
                peer(-1 if side else 1),
            )

        inside = (me > 0, me < nm - 1)

        def halo_each(copy, method):
            for side in range(2):
                there = inside[side] if method == "wait_recv" else inside[1 - side]
                pl.when(there)(getattr(copy(side), method))

        def columns(c):
            return pl.ds(pl.multiple_of(c * width, width), width)

        load_wave = pltpu.make_async_copy(wave_hbm, wave, load_sem.at[0])
        load_coup = pltpu.make_async_copy(coup_hbm, coup, load_sem.at[1])
        load_weights = pltpu.make_async_copy(
            weights_hbm, weights.at[:, pl.ds(0, LANE), :], load_sem.at[2]
        )
        load_tw = pltpu.make_async_copy(tw_hbm, tw_own, load_sem.at[3])
        load_basis = pltpu.make_async_copy(basis_hbm.at[freq], basis_own, load_sem.at[4])
        load_neigh = pltpu.make_async_copy(neigh_hbm, neigh_smem, load_sem.at[5])
        load_block = pltpu.make_async_copy(block_hbm, block_smem, load_sem.at[6])

        barrier = pltpu.get_barrier_semaphore()
        first_core, first_chip = core == 0, chip == 0
        other_core, other_chip = core == 1, chip != 0

        def signal(sem, axis, target):
            pl.semaphore_signal(
                sem, inc=1, device_id={axis: target}, device_id_type=pl.DeviceIdType.MESH
            )

        for d in range(1, ny):
            at_first = at_chip(d) < CORES

            @pl.when(first_core | jnp.logical_not(at_first))
            def _():
                signal(barrier, "freq", at_chip(d))

        @pl.when(other_core)
        def _():
            signal(barrier, "freq", partner)

        @pl.when(other_chip)
        def _():
            pl.semaphore_wait(barrier, jnp.where(first_core, ny, ny - 1))
            for d in range(1, ny):
                send_tw(d).start()
                send_raw(d).start()

        @pl.when(other_core & other_chip)
        def _():
            signal(seen.at[chip - 1], "freq", 1)

        load_tw.start()
        for c in (*range(summed, chunks), *range(summed)):
            load_spec(c).start()
        load_basis.start()
        load_wave.start()
        load_neigh.start()
        load_block.start()

        @pl.when(first_chip)
        def _():
            @pl.when(first_core)
            def _():
                pl.semaphore_wait(barrier, ny)

            @pl.when(other_core)
            def _():
                for d in range(1, ny):
                    pl.semaphore_wait(seen.at[d - 1], 1)

            loaded(summed, RAW, 1).wait()
            for d in range(1, ny):
                send_tw(d).start()
                for r in range(RAW):
                    send_raw_chunk(d, r).start()

        @pl.when(first_core)
        def _():
            signal(go.at[0], "freq", partner)

        @pl.when(other_core)
        def _():
            pl.semaphore_wait(go.at[0], 1)

        loaded(0, summed, 0).wait()

        @pl.when(other_chip)
        def _():
            loaded(summed, RAW, 1).wait()

        for c in range(chunks):
            swap(c).start()

        @pl.when(other_core & first_chip)
        def _():
            for o in range(1, nm):
                signal(barrier, "mesh", peer(o))

        load_coup.start()
        load_weights.start()

        staged[...] = jnp.zeros_like(staged)
        folded[...] = jnp.zeros_like(folded)
        load_tw.wait()
        load_basis.wait()
        for d in range(ny):
            high, low = split(basis_own[d * rp : (d + 1) * rp, :])
            lhs_high[d * rb : d * rb + rp, :] = high
            lhs_low[d * rb : d * rb + rp, :] = low
        for d in range(1, ny):
            high, low = split(basis_own[m1 + (d - 1) * rp : m1 + d * rp, :])
            cross_high[d - 1, 0:rp, :] = high
            cross_low[d - 1, 0:rp, :] = low
        for d in range(2 * ny - 1):
            if 0 < d < ny:
                send_tw(d).wait_recv()
            folded[16 * d : 16 * d + 2, :] = jnp.dot(
                tw_all[d - 1] if 0 < d < ny else tw_own[...],
                basis_own[d * rp : d * rp + rows, :],
                precision=HIGHEST,
                preferred_element_type=F32,
            )
            high, low = split(folded[16 * d : 16 * (d + 1), :])
            if d < ny:
                lhs_high[d * rb + fb : (d + 1) * rb, :] = high
                lhs_low[d * rb + fb : (d + 1) * rb, :] = low
            else:
                cross_high[d - ny, fb:rb, :] = high
                cross_low[d - ny, fb:rb, :] = low

        own_rows = own_spec.reshape(chunks * coefs * seg, LANE)
        peer_rows = peer_spec.reshape(chunks * coefs * seg, LANE)
        far = max(ny - 1, 1)
        raw_rows = raw.reshape(far * RAW * coefs * seg, LANE)
        raw_peer_rows = raw_peer.reshape(far * RAW * coefs * seg, LANE)

        def stage(sources, first, step=seg):
            for p, source in enumerate(sources):
                for s in range(2):
                    for j in range(BLOCKS_PER_CHUNK):
                        piece = source[pl.ds(first + 2 * j + s, coefs, stride=step), :]
                        base = (p * 2 + s) * kp
                        staged[base : base + coefs, j * LANE : (j + 1) * LANE] = piece
            return split(staged[...])

        def product(high, low, s_high, s_low):
            return dot(high, s_high) + dot(low, s_high) + dot(high, s_low)

        def keep_part(c, total, d):
            for s in range(2):
                row = d * rb + fb + s
                for j in range(BLOCKS_PER_CHUNK):
                    part[d, s, pl.ds(c * BLOCKS_PER_CHUNK + j, 1), :] = total[
                        row : row + 1, j * LANE : (j + 1) * LANE
                    ]

        def summed_chunk(c, carry):
            @pl.when(c % PAIR == 0)
            def _():
                swapped(c, PAIR).wait_recv()

            s_high, s_low = stage((own_rows, peer_rows), c * (coefs * seg))
            total = product(lhs_high[...], lhs_low[...], s_high, s_low)
            series[:, columns(c)] = total[0:rows]
            keep_part(c, total, 0)
            for d in range(1, ny):
                keep_part(c, total, d)
                for j, take, put, _ in pieces(c):
                    outgoing[d - 1, c, put, :] = total[
                        d * rb + take.start : d * rb + take.stop, j * LANE : (j + 1) * LANE
                    ]
            return carry

        lax.fori_loop(0, summed, summed_chunk, 0)
        for d in range(1, ny):
            pl.when(jnp.logical_not(detoured(d)))(send_part(d).start)

        def send_chunk(c, carry):
            for d in range(1, ny):
                send_series(d, c, 1).start()
            return carry

        lax.fori_loop(0, summed, send_chunk, 0)

        def raw_chunk(c, carry):
            @pl.when(c % PAIR == 0)
            def _():
                swapped(c, PAIR).wait_recv()

            s_high, s_low = stage((own_rows, peer_rows), c * (coefs * seg))
            total = product(lhs_high[0:rb, :], lhs_low[0:rb, :], s_high, s_low)
            series[:, columns(c)] = total[0:rows]
            keep_part(c, total, 0)
            return carry

        lax.fori_loop(summed, chunks, raw_chunk, 0)

        @pl.when(other_core & first_chip)
        def _():
            pl.semaphore_wait(barrier, nm - 1)
            for d in range(ny):
                signal(all_in.at[0], "freq", d * CORES)
                if d:
                    signal(all_in.at[0], "freq", d * CORES + 1)

        @pl.when(first_core | other_chip)
        def _():
            pl.semaphore_wait(all_in.at[0], 1)

        for d in range(1, ny):
            pl.when(detoured(d))(send_aside(d).start)
        load_wave.wait()
        halo_each(send_halo1, "start")

        pitch = weights.shape[1]
        weight_rows = weights.reshape(groups * pitch, LANE)
        load_weights.wait()

        def line_up(t, carry):
            for i in range(4):
                f = t * 4 + i
                lined[pl.ds(pl.multiple_of(f * LANE, LANE), LANE), :] = weight_rows[
                    pl.ds(f, groups, stride=pitch), :
                ].T
            return carry

        lax.fori_loop(0, LANE // 4, line_up, 0)

        for d in range(1, ny):
            send_raw(d).wait_recv()
            pass_raw(d).start()

        wave_rows = 64

        def stage_current(b, carry):
            at = b * wave_rows
            ext[pl.ds(halo + at, wave_rows), :] = wave[pl.ds(2 * at + 1, wave_rows, stride=2), :]
            return carry

        lax.fori_loop(0, cell_rows // wave_rows, stage_current, 0)

        load_neigh.wait()
        load_block.wait()

        def gather():
            def tile(t, carry):
                for n in range(4):
                    for i in range(8):
                        u = t * 8 + i
                        gathered[n, pl.ds(u, 1), :] = ext[pl.ds(neigh_smem[n, u], 1), :]
                return carry

            lax.fori_loop(0, cell_rows // 8, tile, 0)

        def spread_of(at, center):
            total = jnp.zeros((wave_rows, LANE), F32)
            for n in range(4):
                factor = coup[pl.ds(4 * at + n, wave_rows, stride=4), :]
                total += factor * (gathered[n, pl.ds(at, wave_rows), :] - center)
            return total

        inside_low = (jnp.zeros((halo, LANE), jnp.int32) + me) > 0
        inside_high = (jnp.zeros((halo, LANE), jnp.int32) + me) < nm - 1

        halo_each(send_halo1, "wait_recv")
        ext[0:halo, :] = jnp.where(inside_low, halo1[0, pl.ds(1, halo, stride=2), :], 0.0)
        ext[halo + cell_rows :, :] = jnp.where(
            inside_high, halo1[1, pl.ds(1, halo, stride=2), :], 0.0
        )
        load_coup.wait()
        gather()

        def first_step(b, carry):
            at = b * wave_rows
            center = ext[pl.ds(halo + at, wave_rows), :]
            previous = wave[pl.ds(2 * at, wave_rows, stride=2), :]
            state[pl.ds(2 * at, wave_rows, stride=2), :] = (
                2.0 * center - previous + spread_of(at, center)
            )
            return carry

        lax.fori_loop(0, cell_rows // wave_rows, first_step, 0)

        for d in range(1, ny):
            pass_raw(d).wait_recv()
        for r in range(RAW):
            c = summed + r
            total = series[:, columns(c)]
            extra = None
            for d in range(1, ny):
                s_high, s_low = stage(
                    (raw_rows, raw_peer_rows), ((d - 1) * coefs * RAW + r) * seg, RAW * seg
                )
                cross = product(cross_high[d - 1], cross_low[d - 1], s_high, s_low)
                total += cross[0:rows]
                extra = cross[fb : fb + 2] if extra is None else extra + cross[fb : fb + 2]
            series[:, columns(c)] = total
            if extra is not None:
                for s in range(2):
                    for j in range(BLOCKS_PER_CHUNK):
                        at = pl.ds(c * BLOCKS_PER_CHUNK + j, 1)
                        part[0, s, at, :] = (
                            part[0, s, at, :] + extra[s : s + 1, j * LANE : (j + 1) * LANE]
                        )

        for d in range(1, ny):

            @pl.when(passes())
            def _():
                send_aside(d).wait_recv()
                send_on(d).start()

        for d in range(1, ny):
            send_part(d).wait_recv()
        first_blocks = summed * BLOCKS_PER_CHUNK
        base = pl.multiple_of(me * per, 8)
        for s in range(2):
            weighted = part[0, s, 0:first_blocks, :]
            for d in range(1, ny):
                weighted += part_in[d - 1, s]
            wall[s, pl.ds(base, first_blocks), :] = weighted
            wall[s, pl.ds(base + first_blocks, per - first_blocks), :] = part[0, s, first_blocks:, :]
        for o in range(1, nm):
            send_wall(o).start()
        walled().wait_recv()

        def pick(t, carry):
            for i in range(8):
                g = t * 8 + i
                block = block_smem[g]
                for s in range(2):
                    picked[s, pl.ds(g, 1), :] = wall[s, pl.ds(block, 1), :]
            return carry

        lax.fori_loop(0, groups // 8, pick, 0)
        for s in range(2):
            asked[s] = picked[s].T

        def interpolate(t, carry):
            faces = lined[pl.ds(pl.multiple_of(t * 8 * LANE, 8 * LANE), 8 * LANE), :]
            faces = faces.reshape(8, LANE, groups)
            for s in range(2):
                turned[s, pl.ds(pl.multiple_of(t * 8, 8), 8), :] = jnp.sum(
                    faces * asked[s][None], axis=1
                )
            return carry

        lax.fori_loop(0, LANE // 8, interpolate, 0)
        alive = lax.broadcasted_iota(jnp.int32, (groups, LANE), 0) < count_smem[0]
        push = [jnp.where(alive, turned[s].T, 0.0) for s in range(2)]

        top = pl.ds(0, groups, stride=2)
        state[top, :] = state[top, :] + push[0]

        def stage_stepped(b, carry):
            at = b * wave_rows
            ext[pl.ds(halo + at, wave_rows), :] = state[pl.ds(2 * at, wave_rows, stride=2), :]
            return carry

        lax.fori_loop(0, cell_rows // wave_rows, stage_stepped, 0)
        halo_each(send_halo2, "start")
        halo_each(send_halo2, "wait_recv")
        ext[0:halo, :] = jnp.where(inside_low, halo2[0], 0.0)
        ext[halo + cell_rows :, :] = jnp.where(inside_high, halo2[1], 0.0)
        gather()

        def second_step(b, carry):
            at = b * wave_rows
            center = ext[pl.ds(halo + at, wave_rows), :]
            previous = wave[pl.ds(2 * at + 1, wave_rows, stride=2), :]
            state[pl.ds(2 * at + 1, wave_rows, stride=2), :] = (
                2.0 * center - previous + spread_of(at, center)
            )
            return carry

        lax.fori_loop(0, cell_rows // wave_rows, second_step, 0)
        bottom = pl.ds(1, groups, stride=2)
        state[bottom, :] = state[bottom, :] + push[1]

        swapped(0, chunks).wait_send()
        walled().wait_send()
        for d in range(1, ny):
            send_raw(d).wait_send()
            pass_raw(d).wait_send()
            send_tw(d).wait_send()
            pl.when(jnp.logical_not(detoured(d)))(send_part(d).wait_send)
            pl.when(detoured(d))(send_aside(d).wait_send)
            pl.when(passes())(send_on(d).wait_send)
        halo_each(send_halo1, "wait_send")
        halo_each(send_halo2, "wait_send")

    dma = lambda *shape: pltpu.SemaphoreType.DMA(shape)
    regular = lambda *shape: pltpu.SemaphoreType.REGULAR(shape)
    far = max(ny - 1, 1)
    pl.run_scoped(
        exchange,
        dma(2),
        dma(1),
        dma(chunks // PAIR),
        dma(7),
        dma(far),
        dma(far),
        dma(far),
        dma(far),
        dma(far),
        dma(far),
        dma(far),
        dma(far),
        dma(far),
        dma(far),
        dma(far),
        dma(1),
        dma(1),
        dma(4),
        dma(4),
        regular(1),
        regular(far),
        regular(1),
    )

    def finish(c, carry):
        for d in range(1, ny):
            for _, take, put, lanes in pieces(c):
                series[take, lanes] = series[take, lanes] + incoming[d - 1, c, put, :]
        return carry

    last = summed - 1
    for d in range(1, ny):
        send_series(d, 0, last).wait_recv()
    lax.fori_loop(0, last, finish, 0)
    for d in range(1, ny):
        send_series(d, 0, summed).wait_send()
        send_series(d, last, 1).wait_recv()
    finish(last, 0)


def store(series, state, series_hbm, state_hbm, sem):
    copies = [
        pltpu.make_async_copy(series, series_hbm, sem.at[0]),
        pltpu.make_async_copy(state, state_hbm, sem.at[1]),
    ]
    for copy in copies:
        copy.start()
    for copy in copies:
        copy.wait()


def chip_basis(ny, coefs, rows, horizon):
    kp, rp = pad(coefs, 8), pad(rows, 8)
    freq = np.arange(ny * CORES).reshape(-1, 1, 1, 1, 1, 1)
    d, r, p, s, k = np.indices((2 * ny - 1, rp, CORES, 2, kp), sparse=True)
    chip, core = freq // CORES, freq % CORES
    source = chip - np.where(d < ny, 0, d - ny + 1)
    window = ((chip + np.where(d < ny, d, 0)) % ny) * CORES + core
    wave_number = (source % ny * CORES + (core + p) % CORES) * coefs + k
    angle = ((window * rows + r) * wave_number) % horizon * (2.0 * math.pi / horizon)
    scale = np.where(wave_number == 0, 1.0, 2.0) / horizon
    value = np.where(s == 0, np.cos(angle), -np.sin(angle)) * scale
    value = np.where((r < rows) & (k < coefs), value, 0.0)
    return value.reshape(ny * CORES, (2 * ny - 1) * rp, CORES * 2 * kp).astype(np.float32)


def local(
    ny,
    nm,
    spectrum,
    time_weights,
    interp_weights,
    group_block,
    group_count,
    wave_state,
    neighbors,
    coupling,
):
    coefs, points = spectrum.shape[1:]
    rows = time_weights.shape[1]
    horizon = rows * ny * CORES
    groups = interp_weights.shape[0]
    cell_rows = neighbors.shape[1]
    halo = HALO_CELLS // LANE
    blocks = points // LANE
    chunks = blocks // BLOCKS_PER_CHUNK
    kp, rp = pad(coefs, 8), pad(rows, 8)
    k_all, rb = CORES * 2 * kp, pad(rows, 16) + 16
    summed = chunks - RAW
    seg = 2 * BLOCKS_PER_CHUNK
    width = BLOCKS_PER_CHUNK * LANE

    spec = spectrum.reshape(2, coefs, blocks, LANE).transpose(1, 2, 0, 3)
    spec = spec.reshape(coefs, 2 * blocks, LANE)
    wave = wave_state.reshape(2, cell_rows, LANE).transpose(1, 0, 2).reshape(2 * cell_rows, LANE)
    coup = coupling.reshape(4, cell_rows, LANE).transpose(1, 0, 2).reshape(4 * cell_rows, LANE)
    basis = jnp.asarray(chip_basis(ny, coefs, rows, horizon))

    vmem = lambda *shape: pltpu.VMEM(shape, F32)
    dma = lambda *shape: pltpu.SemaphoreType.DMA(shape)
    smem = pl.BlockSpec(memory_space=pltpu.SMEM)
    hbm = pl.BlockSpec(memory_space=pltpu.HBM)
    on_chip = pl.BlockSpec(memory_space=pltpu.VMEM)
    far = max(ny - 1, 1)
    pinned = [
        pltpu.with_memory_space_constraint(x, pltpu.HBM)
        for x in (
            group_block,
            neighbors,
            time_weights,
            basis,
            spec,
            interp_weights,
            wave,
            coup,
        )
    ]
    outs = (
        jax.ShapeDtypeStruct((rows, points), F32),
        jax.ShapeDtypeStruct((2 * cell_rows, LANE), F32),
    )
    series, state = pl.pallas_call(
        functools.partial(kernel, (ny, nm, coefs, rows, chunks)),
        out_shape=outs,
        in_specs=[smem] + [hbm] * 8,
        out_specs=(on_chip, on_chip),
        scratch_shapes=[
            pltpu.SMEM(group_block.shape, jnp.int32),
            pltpu.SMEM(neighbors.shape, jnp.int32),
            vmem(2, rows),
            vmem((2 * ny - 1) * rp, k_all),
            vmem(16 * (2 * ny - 1), k_all),
            vmem(chunks, coefs, seg, LANE),
            vmem(chunks, coefs, seg, LANE),
            vmem(k_all, width),
            pltpu.VMEM((ny * rb, k_all), BF16),
            pltpu.VMEM((ny * rb, k_all), BF16),
            pltpu.VMEM((far, rb, k_all), BF16),
            pltpu.VMEM((far, rb, k_all), BF16),
            vmem(far, coefs, RAW * seg, LANE),
            vmem(far, coefs, RAW * seg, LANE),
            vmem(far, 2, rows),
            vmem(far, summed, BLOCKS_PER_CHUNK * rows, LANE),
            vmem(far, summed, BLOCKS_PER_CHUNK * rows, LANE),
            vmem(ny, 2, blocks, LANE),
            vmem(far, 2, summed * BLOCKS_PER_CHUNK, LANE),
            vmem(far, 2, summed * BLOCKS_PER_CHUNK, LANE),
            vmem(2, nm * blocks, LANE),
            vmem(2, groups, LANE),
            vmem(2, LANE, groups),
            vmem(2, LANE, groups),
            vmem(groups, LANE + 8, LANE),
            vmem(LANE * LANE, groups),
            vmem(2 * cell_rows, LANE),
            vmem(4 * cell_rows, LANE),
            vmem(2, 2 * halo, LANE),
            vmem(2, halo, LANE),
            vmem(cell_rows + 2 * halo, LANE),
            vmem(4, cell_rows, LANE),
            dma(far),
            dma(far, 2),
        ],
        compiler_params=pltpu.CompilerParams(
            collective_id=0, has_side_effects=True, vmem_limit_bytes=50000 * 1024
        ),
        name="adjoint",
    )(group_count, *pinned)
    series, state = pl.pallas_call(
        store,
        out_shape=outs,
        in_specs=[pl.BlockSpec(memory_space=pl.ANY)] * 2,
        out_specs=(hbm, hbm),
        scratch_shapes=[dma(2)],
        compiler_params=pltpu.CompilerParams(vmem_limit_bytes=1024 * 1024),
        name="store",
    )(series, state)
    new_state = state.reshape(cell_rows, 2, LANE).transpose(1, 0, 2)
    return series, new_state.reshape(1, 2, cell_rows * LANE)


def solution(mesh):
    placed = (
        P(None, "freq", "mesh"),
        P(None, "freq"),
        P("mesh", None, None),
        P("mesh"),
        P("mesh"),
        P("freq", None, "mesh"),
        P(None, "mesh"),
        P(None, "mesh"),
    )
    ny = mesh.shape["freq"] // CORES
    return jax.shard_map(
        functools.partial(local, ny, mesh.shape["mesh"]),
        mesh=mesh,
        in_specs=placed,
        out_specs=(P("freq", "mesh"), P("freq", None, "mesh")),
        check_vma=False,
    )
```

```python
import functools
import math

import jax
import jax.numpy as jnp
import numpy as np
from jax import lax
from jax.experimental import pallas as pl
from jax.experimental.pallas import tpu as pltpu
from jax.sharding import PartitionSpec as P

LANE = 128
CORES = 2
HALO_CELLS = 4096
BLOCKS_PER_CHUNK = 4
RAW = 3
PAIR = 2
HEAD = 32
HIGHEST = lax.Precision.HIGHEST
F32 = jnp.float32
BF16 = jnp.bfloat16


def pad(n, to):
    return (n + to - 1) // to * to


def split(x):
    high = x.astype(BF16)
    return high, (x - high.astype(F32)).astype(BF16)


def dot(a, b):
    return jnp.dot(a, b, preferred_element_type=F32)


def kernel(
    dims,
    count_smem,
    block_hbm,
    neigh_hbm,
    tw_hbm,
    basis_hbm,
    spec_hbm,
    weights_hbm,
    wave_hbm,
    coup_hbm,
    series,
    state,
    block_smem,
    neigh_smem,
    tw_own,
    basis_own,
    folded,
    own_spec,
    peer_spec,
    staged,
    lhs_high,
    lhs_low,
    cross_high,
    cross_low,
    raw,
    raw_peer,
    tw_all,
    outgoing,
    incoming,
    part,
    part_in,
    aside,
    aside_head,
    wall,
    picked,
    asked,
    turned,
    weights,
    lined,
    wave,
    coup,
    halo1,
    halo2,
    ext,
    gathered,
    ser_send,
    ser_recv,
):
    ny, nm, coefs, rows, chunks = dims
    groups = weights.shape[0]
    kp, rp, fb = pad(coefs, 8), pad(rows, 8), pad(rows, 16)
    rb = fb + 16
    m1 = ny * rp
    per = part.shape[2]
    cell_rows = ext.shape[0] - 2 * halo1.shape[1] // 2
    halo = halo1.shape[1] // 2
    width = BLOCKS_PER_CHUNK * LANE
    seg = 2 * BLOCKS_PER_CHUNK
    summed = chunks - RAW
    whole_rows = rows // 8 * 8
    rest = rows - whole_rows

    freq = lax.axis_index("freq")
    me = lax.axis_index("mesh")
    chip, core = freq // CORES, freq % CORES
    partner = chip * CORES + (1 - core)

    def at_chip(d):
        return ((chip + d + ny) % ny) * CORES + core

    def peer(d):
        return (me + d + nm) % nm

    def remote(src, dst, send, recv, axis, target):
        return pltpu.make_async_remote_copy(
            src_ref=src,
            dst_ref=dst,
            send_sem=send,
            recv_sem=recv,
            device_id={axis: target},
            device_id_type=pl.DeviceIdType.MESH,
        )

    last = summed - 1

    def send_series(d, first, count):
        span = pl.ds(first, count)
        return remote(
            outgoing.at[d - 1, span],
            incoming.at[d - 1, span],
            ser_send.at[d - 1, 0],
            ser_recv.at[d - 1, 0],
            "freq",
            at_chip(d),
        )

    def send_last(d):
        span = pl.ds(HEAD, outgoing.shape[2] - HEAD)
        return remote(
            outgoing.at[d - 1, last, span],
            incoming.at[d - 1, last, span],
            ser_send.at[d - 1, 1],
            ser_recv.at[d - 1, 1],
            "freq",
            at_chip(d),
        )

    def pieces(c):
        for j in range(BLOCKS_PER_CHUNK):
            lanes = pl.ds(pl.multiple_of(c * width + j * LANE, LANE), LANE)
            yield j, slice(0, whole_rows), slice(j * whole_rows, (j + 1) * whole_rows), lanes
            if rest:
                first = BLOCKS_PER_CHUNK * whole_rows + j * rest
                yield j, slice(whole_rows, rows), slice(first, first + rest), lanes

    def exchange(
        spec_sem,
        swap_send,
        swap_recv,
        load_sem,
        tw_send,
        tw_recv,
        raw_send,
        raw_recv,
        pass_send,
        pass_recv,
        part_send,
        part_recv,
        aside_send,
        aside_recv,
        on_send,
        head_send,
        head_recv,
        wall_send,
        wall_recv,
        halo_send,
        halo_recv,
        go,
        seen,
        all_in,
    ):
        def load_spec(c):
            return pltpu.make_async_copy(
                spec_hbm.at[:, pl.ds(c * seg, seg), :],
                own_spec.at[c],
                spec_sem.at[1 if c >= summed else 0],
            )

        def loaded(first, count, sem):
            span = own_spec.at[pl.ds(first, count)]
            return pltpu.make_async_copy(span, span, spec_sem.at[sem])

        def swap(c):
            return remote(
                own_spec.at[c],
                peer_spec.at[c],
                swap_send.at[0],
                swap_recv.at[c // PAIR],
                "freq",
                partner,
            )

        def swapped(first, count):
            span = peer_spec.at[pl.ds(first, count)]
            return remote(span, span, swap_send.at[0], swap_recv.at[first // PAIR], "freq", partner)

        def send_tw(d):
            return remote(
                tw_hbm, tw_all.at[d - 1], tw_send.at[d - 1], tw_recv.at[d - 1], "freq", at_chip(-d)
            )

        def send_raw(d):
            return remote(
                spec_hbm.at[:, pl.ds(summed * seg, RAW * seg), :],
                raw.at[d - 1],
                raw_send.at[d - 1],
                raw_recv.at[d - 1],
                "freq",
                at_chip(d),
            )

        def send_raw_chunk(d, r):
            return remote(
                own_spec.at[summed + r],
                raw.at[d - 1, :, pl.ds(r * seg, seg), :],
                raw_send.at[d - 1],
                raw_recv.at[d - 1],
                "freq",
                at_chip(d),
            )

        def pass_raw(d):
            return remote(
                raw.at[d - 1],
                raw_peer.at[d - 1],
                pass_send.at[d - 1],
                pass_recv.at[d - 1],
                "freq",
                partner,
            )

        def send_part(d):
            return remote(
                part.at[d, :, pl.ds(0, summed * BLOCKS_PER_CHUNK), :],
                part_in.at[d - 1],
                part_send.at[d - 1],
                part_recv.at[d - 1],
                "freq",
                at_chip(d),
            )

        def detoured(d):
            return (me == 0) & ((chip + d) % ny == 0)

        def passes():
            return (me == 1 + core) & (chip == 0)

        def head(ref, d):
            return ref.at[d - 1, last, pl.ds(0, HEAD)]

        def send_head(d):
            return remote(
                head(outgoing, d),
                head(incoming, d),
                head_send.at[d - 1],
                head_recv.at[d - 1],
                "freq",
                at_chip(d),
            )

        def send_aside(d):
            pairs = (
                (part.at[d, :, pl.ds(0, summed * BLOCKS_PER_CHUNK), :], aside),
                (head(outgoing, d), aside_head),
            )
            return [
                pltpu.make_async_remote_copy(
                    src_ref=source,
                    dst_ref=target.at[d - 1],
                    send_sem=aside_send.at[d - 1, i],
                    recv_sem=aside_recv.at[d - 1, i],
                    device_id={"freq": at_chip(d), "mesh": 1 + core},
                    device_id_type=pl.DeviceIdType.MESH,
                )
                for i, (source, target) in enumerate(pairs)
            ]

        def send_on(d):
            pairs = (
                (aside.at[d - 1], part_in.at[d - 1], part_recv),
                (aside_head.at[d - 1], head(incoming, d), head_recv),
            )
            return [
                remote(source, target, on_send.at[d - 1, i], recv.at[d - 1], "mesh", 0)
                for i, (source, target, recv) in enumerate(pairs)
            ]

        def send_wall(o):
            mine = wall.at[:, pl.ds(pl.multiple_of(me * per, 8), per), :]
            return remote(mine, mine, wall_send.at[0], wall_recv.at[0], "mesh", peer(o))

        def walled():
            span = wall.at[:, pl.ds(0, (nm - 1) * per), :]
            return remote(span, span, wall_send.at[0], wall_recv.at[0], "mesh", peer(1))

        def send_halo1(side):
            first = 0 if side else 2 * (cell_rows - halo)
            return remote(
                wave.at[pl.ds(first, 2 * halo)],
                halo1.at[side],
                halo_send.at[side],
                halo_recv.at[side],
                "mesh",
                peer(-1 if side else 1),
            )

        def send_halo2(side):
            first = halo if side else cell_rows
            return remote(
                ext.at[pl.ds(first, halo)],
                halo2.at[side],
                halo_send.at[2 + side],
                halo_recv.at[2 + side],
                "mesh",
                peer(-1 if side else 1),
            )

        inside = (me > 0, me < nm - 1)

        def halo_each(copy, method):
            for side in range(2):
                there = inside[side] if method == "wait_recv" else inside[1 - side]
                pl.when(there)(getattr(copy(side), method))

        def columns(c):
            return pl.ds(pl.multiple_of(c * width, width), width)

        load_wave = pltpu.make_async_copy(wave_hbm, wave, load_sem.at[0])
        load_coup = pltpu.make_async_copy(coup_hbm, coup, load_sem.at[1])
        load_weights = pltpu.make_async_copy(
            weights_hbm, weights.at[:, pl.ds(0, LANE), :], load_sem.at[2]
        )
        load_tw = pltpu.make_async_copy(tw_hbm, tw_own, load_sem.at[3])
        load_basis = pltpu.make_async_copy(basis_hbm.at[freq], basis_own, load_sem.at[4])
        load_neigh = pltpu.make_async_copy(neigh_hbm, neigh_smem, load_sem.at[5])
        load_block = pltpu.make_async_copy(block_hbm, block_smem, load_sem.at[6])

        barrier = pltpu.get_barrier_semaphore()
        first_core, first_chip = core == 0, chip == 0
        other_core, other_chip = core == 1, chip != 0

        def signal(sem, axis, target):
            pl.semaphore_signal(
                sem, inc=1, device_id={axis: target}, device_id_type=pl.DeviceIdType.MESH
            )

        for d in range(1, ny):
            at_first = at_chip(d) < CORES

            @pl.when(first_core | jnp.logical_not(at_first))
            def _():
                signal(barrier, "freq", at_chip(d))

        @pl.when(other_core)
        def _():
            signal(barrier, "freq", partner)

        @pl.when(other_chip)
        def _():
            pl.semaphore_wait(barrier, jnp.where(first_core, ny, ny - 1))
            for d in range(1, ny):
                send_tw(d).start()
                send_raw(d).start()

        @pl.when(other_core & other_chip)
        def _():
            signal(seen.at[chip - 1], "freq", 1)

        load_tw.start()
        for c in (*range(summed, chunks), *range(summed)):
            load_spec(c).start()
        load_basis.start()
        load_wave.start()
        load_neigh.start()
        load_block.start()

        @pl.when(first_chip)
        def _():
            @pl.when(first_core)
            def _():
                pl.semaphore_wait(barrier, ny)

            @pl.when(other_core)
            def _():
                for d in range(1, ny):
                    pl.semaphore_wait(seen.at[d - 1], 1)

            loaded(summed, RAW, 1).wait()
            for d in range(1, ny):
                send_tw(d).start()
                for r in range(RAW):
                    send_raw_chunk(d, r).start()

        @pl.when(first_core)
        def _():
            signal(go.at[0], "freq", partner)

        @pl.when(other_core)
        def _():
            pl.semaphore_wait(go.at[0], 1)

        loaded(0, summed, 0).wait()

        @pl.when(other_chip)
        def _():
            loaded(summed, RAW, 1).wait()

        for c in range(chunks):
            swap(c).start()

        @pl.when(other_core & first_chip)
        def _():
            for o in range(1, nm):
                signal(barrier, "mesh", peer(o))

        load_coup.start()
        load_weights.start()

        staged[...] = jnp.zeros_like(staged)
        folded[...] = jnp.zeros_like(folded)
        load_tw.wait()
        load_basis.wait()
        for d in range(ny):
            high, low = split(basis_own[d * rp : (d + 1) * rp, :])
            lhs_high[d * rb : d * rb + rp, :] = high
            lhs_low[d * rb : d * rb + rp, :] = low
        for d in range(1, ny):
            high, low = split(basis_own[m1 + (d - 1) * rp : m1 + d * rp, :])
            cross_high[d - 1, 0:rp, :] = high
            cross_low[d - 1, 0:rp, :] = low
        for d in range(2 * ny - 1):
            if 0 < d < ny:
                send_tw(d).wait_recv()
            folded[16 * d : 16 * d + 2, :] = jnp.dot(
                tw_all[d - 1] if 0 < d < ny else tw_own[...],
                basis_own[d * rp : d * rp + rows, :],
                precision=HIGHEST,
                preferred_element_type=F32,
            )
            high, low = split(folded[16 * d : 16 * (d + 1), :])
            if d < ny:
                lhs_high[d * rb + fb : (d + 1) * rb, :] = high
                lhs_low[d * rb + fb : (d + 1) * rb, :] = low
            else:
                cross_high[d - ny, fb:rb, :] = high
                cross_low[d - ny, fb:rb, :] = low

        own_rows = own_spec.reshape(chunks * coefs * seg, LANE)
        peer_rows = peer_spec.reshape(chunks * coefs * seg, LANE)
        far = max(ny - 1, 1)
        raw_rows = raw.reshape(far * RAW * coefs * seg, LANE)
        raw_peer_rows = raw_peer.reshape(far * RAW * coefs * seg, LANE)

        def stage(sources, first, step=seg):
            for p, source in enumerate(sources):
                for s in range(2):
                    for j in range(BLOCKS_PER_CHUNK):
                        piece = source[pl.ds(first + 2 * j + s, coefs, stride=step), :]
                        base = (p * 2 + s) * kp
                        staged[base : base + coefs, j * LANE : (j + 1) * LANE] = piece
            return split(staged[...])

        def product(high, low, s_high, s_low):
            return dot(high, s_high) + dot(low, s_high) + dot(high, s_low)

        def keep_part(c, total, d):
            for s in range(2):
                row = d * rb + fb + s
                for j in range(BLOCKS_PER_CHUNK):
                    part[d, s, pl.ds(c * BLOCKS_PER_CHUNK + j, 1), :] = total[
                        row : row + 1, j * LANE : (j + 1) * LANE
                    ]

        def summed_chunk(c, carry):
            @pl.when(c % PAIR == 0)
            def _():
                swapped(c, PAIR).wait_recv()

            s_high, s_low = stage((own_rows, peer_rows), c * (coefs * seg))
            total = product(lhs_high[...], lhs_low[...], s_high, s_low)
            series[:, columns(c)] = total[0:rows]
            keep_part(c, total, 0)
            for d in range(1, ny):
                keep_part(c, total, d)
                for j, take, put, _ in pieces(c):
                    outgoing[d - 1, c, put, :] = total[
                        d * rb + take.start : d * rb + take.stop, j * LANE : (j + 1) * LANE
                    ]
            return carry

        lax.fori_loop(0, summed, summed_chunk, 0)
        for d in range(1, ny):
            pl.when(jnp.logical_not(detoured(d)))(send_part(d).start)

        def send_chunk(c, carry):
            for d in range(1, ny):
                send_series(d, c, 1).start()
            return carry

        for d in range(1, ny):
            pl.when(jnp.logical_not(detoured(d)))(send_head(d).start)
        lax.fori_loop(0, last, send_chunk, 0)
        for d in range(1, ny):
            send_last(d).start()

        def raw_chunk(c, carry):
            @pl.when(c % PAIR == 0)
            def _():
                swapped(c, PAIR).wait_recv()

            s_high, s_low = stage((own_rows, peer_rows), c * (coefs * seg))
            total = product(lhs_high[0:rb, :], lhs_low[0:rb, :], s_high, s_low)
            series[:, columns(c)] = total[0:rows]
            keep_part(c, total, 0)
            return carry

        lax.fori_loop(summed, chunks, raw_chunk, 0)

        @pl.when(other_core & first_chip)
        def _():
            pl.semaphore_wait(barrier, nm - 1)
            for d in range(ny):
                signal(all_in.at[0], "freq", d * CORES)
                if d:
                    signal(all_in.at[0], "freq", d * CORES + 1)

        @pl.when(first_core | other_chip)
        def _():
            pl.semaphore_wait(all_in.at[0], 1)

        for d in range(1, ny):

            @pl.when(detoured(d))
            def _():
                for copy in send_aside(d):
                    copy.start()

        load_wave.wait()
        halo_each(send_halo1, "start")

        pitch = weights.shape[1]
        weight_rows = weights.reshape(groups * pitch, LANE)
        load_weights.wait()

        def line_up(t, carry):
            for i in range(4):
                f = t * 4 + i
                lined[pl.ds(pl.multiple_of(f * LANE, LANE), LANE), :] = weight_rows[
                    pl.ds(f, groups, stride=pitch), :
                ].T
            return carry

        lax.fori_loop(0, LANE // 4, line_up, 0)

        for d in range(1, ny):
            send_raw(d).wait_recv()
            pass_raw(d).start()

        wave_rows = 64

        def stage_current(b, carry):
            at = b * wave_rows
            ext[pl.ds(halo + at, wave_rows), :] = wave[pl.ds(2 * at + 1, wave_rows, stride=2), :]
            return carry

        lax.fori_loop(0, cell_rows // wave_rows, stage_current, 0)

        load_neigh.wait()
        load_block.wait()

        def gather():
            def tile(t, carry):
                for n in range(4):
                    for i in range(8):
                        u = t * 8 + i
                        gathered[n, pl.ds(u, 1), :] = ext[pl.ds(neigh_smem[n, u], 1), :]
                return carry

            lax.fori_loop(0, cell_rows // 8, tile, 0)

        def spread_of(at, center):
            total = jnp.zeros((wave_rows, LANE), F32)
            for n in range(4):
                factor = coup[pl.ds(4 * at + n, wave_rows, stride=4), :]
                total += factor * (gathered[n, pl.ds(at, wave_rows), :] - center)
            return total

        inside_low = (jnp.zeros((halo, LANE), jnp.int32) + me) > 0
        inside_high = (jnp.zeros((halo, LANE), jnp.int32) + me) < nm - 1

        halo_each(send_halo1, "wait_recv")
        ext[0:halo, :] = jnp.where(inside_low, halo1[0, pl.ds(1, halo, stride=2), :], 0.0)
        ext[halo + cell_rows :, :] = jnp.where(
            inside_high, halo1[1, pl.ds(1, halo, stride=2), :], 0.0
        )
        load_coup.wait()
        gather()

        def first_step(b, carry):
            at = b * wave_rows
            center = ext[pl.ds(halo + at, wave_rows), :]
            previous = wave[pl.ds(2 * at, wave_rows, stride=2), :]
            state[pl.ds(2 * at, wave_rows, stride=2), :] = (
                2.0 * center - previous + spread_of(at, center)
            )
            return carry

        lax.fori_loop(0, cell_rows // wave_rows, first_step, 0)

        for d in range(1, ny):
            pass_raw(d).wait_recv()
        for r in range(RAW):
            c = summed + r
            total = series[:, columns(c)]
            extra = None
            for d in range(1, ny):
                s_high, s_low = stage(
                    (raw_rows, raw_peer_rows), ((d - 1) * coefs * RAW + r) * seg, RAW * seg
                )
                cross = product(cross_high[d - 1], cross_low[d - 1], s_high, s_low)
                total += cross[0:rows]
                extra = cross[fb : fb + 2] if extra is None else extra + cross[fb : fb + 2]
            series[:, columns(c)] = total
            if extra is not None:
                for s in range(2):
                    for j in range(BLOCKS_PER_CHUNK):
                        at = pl.ds(c * BLOCKS_PER_CHUNK + j, 1)
                        part[0, s, at, :] = (
                            part[0, s, at, :] + extra[s : s + 1, j * LANE : (j + 1) * LANE]
                        )

        for d in range(1, ny):

            @pl.when(passes())
            def _():
                for copy in send_aside(d):
                    copy.wait_recv()
                for copy in send_on(d):
                    copy.start()

        for d in range(1, ny):
            send_part(d).wait_recv()
        first_blocks = summed * BLOCKS_PER_CHUNK
        base = pl.multiple_of(me * per, 8)
        for s in range(2):
            weighted = part[0, s, 0:first_blocks, :]
            for d in range(1, ny):
                weighted += part_in[d - 1, s]
            wall[s, pl.ds(base, first_blocks), :] = weighted
            wall[s, pl.ds(base + first_blocks, per - first_blocks), :] = part[0, s, first_blocks:, :]
        for o in range(1, nm):
            send_wall(o).start()
        walled().wait_recv()

        def pick(t, carry):
            for i in range(8):
                g = t * 8 + i
                block = block_smem[g]
                for s in range(2):
                    picked[s, pl.ds(g, 1), :] = wall[s, pl.ds(block, 1), :]
            return carry

        lax.fori_loop(0, groups // 8, pick, 0)
        for s in range(2):
            asked[s] = picked[s].T

        def interpolate(t, carry):
            faces = lined[pl.ds(pl.multiple_of(t * 8 * LANE, 8 * LANE), 8 * LANE), :]
            faces = faces.reshape(8, LANE, groups)
            for s in range(2):
                turned[s, pl.ds(pl.multiple_of(t * 8, 8), 8), :] = jnp.sum(
                    faces * asked[s][None], axis=1
                )
            return carry

        lax.fori_loop(0, LANE // 8, interpolate, 0)
        alive = lax.broadcasted_iota(jnp.int32, (groups, LANE), 0) < count_smem[0]
        push = [jnp.where(alive, turned[s].T, 0.0) for s in range(2)]

        top = pl.ds(0, groups, stride=2)
        state[top, :] = state[top, :] + push[0]

        def stage_stepped(b, carry):
            at = b * wave_rows
            ext[pl.ds(halo + at, wave_rows), :] = state[pl.ds(2 * at, wave_rows, stride=2), :]
            return carry

        lax.fori_loop(0, cell_rows // wave_rows, stage_stepped, 0)
        halo_each(send_halo2, "start")
        halo_each(send_halo2, "wait_recv")
        ext[0:halo, :] = jnp.where(inside_low, halo2[0], 0.0)
        ext[halo + cell_rows :, :] = jnp.where(inside_high, halo2[1], 0.0)
        gather()

        def second_step(b, carry):
            at = b * wave_rows
            center = ext[pl.ds(halo + at, wave_rows), :]
            previous = wave[pl.ds(2 * at + 1, wave_rows, stride=2), :]
            state[pl.ds(2 * at + 1, wave_rows, stride=2), :] = (
                2.0 * center - previous + spread_of(at, center)
            )
            return carry

        lax.fori_loop(0, cell_rows // wave_rows, second_step, 0)
        bottom = pl.ds(1, groups, stride=2)
        state[bottom, :] = state[bottom, :] + push[1]

        swapped(0, chunks).wait_send()
        walled().wait_send()
        for d in range(1, ny):
            send_raw(d).wait_send()
            pass_raw(d).wait_send()
            send_tw(d).wait_send()

            @pl.when(jnp.logical_not(detoured(d)))
            def _():
                send_part(d).wait_send()
                send_head(d).wait_send()

            @pl.when(detoured(d))
            def _():
                for copy in send_aside(d):
                    copy.wait_send()

            @pl.when(passes())
            def _():
                for copy in send_on(d):
                    copy.wait_send()

            send_head(d).wait_recv()
        halo_each(send_halo1, "wait_send")
        halo_each(send_halo2, "wait_send")

    dma = lambda *shape: pltpu.SemaphoreType.DMA(shape)
    regular = lambda *shape: pltpu.SemaphoreType.REGULAR(shape)
    far = max(ny - 1, 1)
    pl.run_scoped(
        exchange,
        dma(2),
        dma(1),
        dma(chunks // PAIR),
        dma(7),
        dma(far),
        dma(far),
        dma(far),
        dma(far),
        dma(far),
        dma(far),
        dma(far),
        dma(far),
        dma(far, 2),
        dma(far, 2),
        dma(far, 2),
        dma(far),
        dma(far),
        dma(1),
        dma(1),
        dma(4),
        dma(4),
        regular(1),
        regular(far),
        regular(1),
    )

    def finish(c, carry):
        for d in range(1, ny):
            for _, take, put, lanes in pieces(c):
                series[take, lanes] = series[take, lanes] + incoming[d - 1, c, put, :]
        return carry

    for d in range(1, ny):
        send_series(d, 0, last).wait_recv()
    lax.fori_loop(0, last, finish, 0)
    for d in range(1, ny):
        send_series(d, 0, last).wait_send()
        send_last(d).wait_send()
        send_last(d).wait_recv()
    finish(last, 0)


def store(series, state, series_hbm, state_hbm, sem):
    copies = [
        pltpu.make_async_copy(series, series_hbm, sem.at[0]),
        pltpu.make_async_copy(state, state_hbm, sem.at[1]),
    ]
    for copy in copies:
        copy.start()
    for copy in copies:
        copy.wait()


def chip_basis(ny, coefs, rows, horizon):
    kp, rp = pad(coefs, 8), pad(rows, 8)
    freq = np.arange(ny * CORES).reshape(-1, 1, 1, 1, 1, 1)
    d, r, p, s, k = np.indices((2 * ny - 1, rp, CORES, 2, kp), sparse=True)
    chip, core = freq // CORES, freq % CORES
    source = chip - np.where(d < ny, 0, d - ny + 1)
    window = ((chip + np.where(d < ny, d, 0)) % ny) * CORES + core
    wave_number = (source % ny * CORES + (core + p) % CORES) * coefs + k
    angle = ((window * rows + r) * wave_number) % horizon * (2.0 * math.pi / horizon)
    scale = np.where(wave_number == 0, 1.0, 2.0) / horizon
    value = np.where(s == 0, np.cos(angle), -np.sin(angle)) * scale
    value = np.where((r < rows) & (k < coefs), value, 0.0)
    return value.reshape(ny * CORES, (2 * ny - 1) * rp, CORES * 2 * kp).astype(np.float32)


def local(
    ny,
    nm,
    spectrum,
    time_weights,
    interp_weights,
    group_block,
    group_count,
    wave_state,
    neighbors,
    coupling,
):
    coefs, points = spectrum.shape[1:]
    rows = time_weights.shape[1]
    horizon = rows * ny * CORES
    groups = interp_weights.shape[0]
    cell_rows = neighbors.shape[1]
    halo = HALO_CELLS // LANE
    blocks = points // LANE
    chunks = blocks // BLOCKS_PER_CHUNK
    kp, rp = pad(coefs, 8), pad(rows, 8)
    k_all, rb = CORES * 2 * kp, pad(rows, 16) + 16
    summed = chunks - RAW
    seg = 2 * BLOCKS_PER_CHUNK
    width = BLOCKS_PER_CHUNK * LANE

    spec = spectrum.reshape(2, coefs, blocks, LANE).transpose(1, 2, 0, 3)
    spec = spec.reshape(coefs, 2 * blocks, LANE)
    wave = wave_state.reshape(2, cell_rows, LANE).transpose(1, 0, 2).reshape(2 * cell_rows, LANE)
    coup = coupling.reshape(4, cell_rows, LANE).transpose(1, 0, 2).reshape(4 * cell_rows, LANE)
    basis = jnp.asarray(chip_basis(ny, coefs, rows, horizon))

    vmem = lambda *shape: pltpu.VMEM(shape, F32)
    dma = lambda *shape: pltpu.SemaphoreType.DMA(shape)
    smem = pl.BlockSpec(memory_space=pltpu.SMEM)
    hbm = pl.BlockSpec(memory_space=pltpu.HBM)
    on_chip = pl.BlockSpec(memory_space=pltpu.VMEM)
    far = max(ny - 1, 1)
    pinned = [
        pltpu.with_memory_space_constraint(x, pltpu.HBM)
        for x in (
            group_block,
            neighbors,
            time_weights,
            basis,
            spec,
            interp_weights,
            wave,
            coup,
        )
    ]
    outs = (
        jax.ShapeDtypeStruct((rows, points), F32),
        jax.ShapeDtypeStruct((2 * cell_rows, LANE), F32),
    )
    series, state = pl.pallas_call(
        functools.partial(kernel, (ny, nm, coefs, rows, chunks)),
        out_shape=outs,
        in_specs=[smem] + [hbm] * 8,
        out_specs=(on_chip, on_chip),
        scratch_shapes=[
            pltpu.SMEM(group_block.shape, jnp.int32),
            pltpu.SMEM(neighbors.shape, jnp.int32),
            vmem(2, rows),
            vmem((2 * ny - 1) * rp, k_all),
            vmem(16 * (2 * ny - 1), k_all),
            vmem(chunks, coefs, seg, LANE),
            vmem(chunks, coefs, seg, LANE),
            vmem(k_all, width),
            pltpu.VMEM((ny * rb, k_all), BF16),
            pltpu.VMEM((ny * rb, k_all), BF16),
            pltpu.VMEM((far, rb, k_all), BF16),
            pltpu.VMEM((far, rb, k_all), BF16),
            vmem(far, coefs, RAW * seg, LANE),
            vmem(far, coefs, RAW * seg, LANE),
            vmem(far, 2, rows),
            vmem(far, summed, BLOCKS_PER_CHUNK * rows, LANE),
            vmem(far, summed, BLOCKS_PER_CHUNK * rows, LANE),
            vmem(ny, 2, blocks, LANE),
            vmem(far, 2, summed * BLOCKS_PER_CHUNK, LANE),
            vmem(far, 2, summed * BLOCKS_PER_CHUNK, LANE),
            vmem(far, HEAD, LANE),
            vmem(2, nm * blocks, LANE),
            vmem(2, groups, LANE),
            vmem(2, LANE, groups),
            vmem(2, LANE, groups),
            vmem(groups, LANE + 8, LANE),
            vmem(LANE * LANE, groups),
            vmem(2 * cell_rows, LANE),
            vmem(4 * cell_rows, LANE),
            vmem(2, 2 * halo, LANE),
            vmem(2, halo, LANE),
            vmem(cell_rows + 2 * halo, LANE),
            vmem(4, cell_rows, LANE),
            dma(far, 2),
            dma(far, 2),
        ],
        compiler_params=pltpu.CompilerParams(
            collective_id=0, has_side_effects=True, vmem_limit_bytes=50000 * 1024
        ),
        name="adjoint",
    )(group_count, *pinned)
    series, state = pl.pallas_call(
        store,
        out_shape=outs,
        in_specs=[pl.BlockSpec(memory_space=pl.ANY)] * 2,
        out_specs=(hbm, hbm),
        scratch_shapes=[dma(2)],
        compiler_params=pltpu.CompilerParams(vmem_limit_bytes=1024 * 1024),
        name="store",
    )(series, state)
    new_state = state.reshape(cell_rows, 2, LANE).transpose(1, 0, 2)
    return series, new_state.reshape(1, 2, cell_rows * LANE)


def solution(mesh):
    placed = (
        P(None, "freq", "mesh"),
        P(None, "freq"),
        P("mesh", None, None),
        P("mesh"),
        P("mesh"),
        P("freq", None, "mesh"),
        P(None, "mesh"),
        P(None, "mesh"),
    )
    ny = mesh.shape["freq"] // CORES
    return jax.shard_map(
        functools.partial(local, ny, mesh.shape["mesh"]),
        mesh=mesh,
        in_specs=placed,
        out_specs=(P("freq", "mesh"), P("freq", None, "mesh")),
        check_vma=False,
    )
```

```python
import functools
import math

import jax
import jax.numpy as jnp
import numpy as np
from jax import lax
from jax.experimental import pallas as pl
from jax.experimental.pallas import tpu as pltpu
from jax.sharding import PartitionSpec as P

LANE = 128
CORES = 2
HALO_CELLS = 4096
BLOCKS_PER_CHUNK = 4
RAW = 3
PAIR = 2
HEAD = 32
HIGHEST = lax.Precision.HIGHEST
F32 = jnp.float32
BF16 = jnp.bfloat16


def pad(n, to):
    return (n + to - 1) // to * to


def split(x):
    high = x.astype(BF16)
    return high, (x - high.astype(F32)).astype(BF16)


def dot(a, b):
    return jnp.dot(a, b, preferred_element_type=F32)


def kernel(
    dims,
    count_smem,
    block_hbm,
    neigh_hbm,
    tw_hbm,
    basis_hbm,
    spec_hbm,
    weights_hbm,
    wave_hbm,
    coup_hbm,
    series,
    state,
    block_smem,
    neigh_smem,
    tw_own,
    basis_own,
    folded,
    own_spec,
    peer_spec,
    staged,
    lhs_high,
    lhs_low,
    cross_high,
    cross_low,
    raw,
    raw_peer,
    tw_all,
    outgoing,
    incoming,
    part,
    part_in,
    aside,
    aside_head,
    wall,
    picked,
    asked,
    turned,
    weights,
    lined,
    wave,
    coup,
    halo1,
    halo2,
    ext,
    gathered,
    ser_send,
    ser_recv,
):
    ny, nm, coefs, rows, chunks = dims
    groups = weights.shape[0]
    kp, rp, fb = pad(coefs, 8), pad(rows, 8), pad(rows, 16)
    rb = fb + 16
    m1 = ny * rp
    per = part.shape[2]
    cell_rows = ext.shape[0] - 2 * halo1.shape[1] // 2
    halo = halo1.shape[1] // 2
    width = BLOCKS_PER_CHUNK * LANE
    seg = 2 * BLOCKS_PER_CHUNK
    summed = chunks - RAW
    whole_rows = rows // 8 * 8
    rest = rows - whole_rows

    freq = lax.axis_index("freq")
    me = lax.axis_index("mesh")
    chip, core = freq // CORES, freq % CORES
    partner = chip * CORES + (1 - core)

    def at_chip(d):
        return ((chip + d + ny) % ny) * CORES + core

    def peer(d):
        return (me + d + nm) % nm

    def remote(src, dst, send, recv, axis, target):
        return pltpu.make_async_remote_copy(
            src_ref=src,
            dst_ref=dst,
            send_sem=send,
            recv_sem=recv,
            device_id={axis: target},
            device_id_type=pl.DeviceIdType.MESH,
        )

    last = summed - 1

    def send_series(d, first, count):
        span = pl.ds(first, count)
        return remote(
            outgoing.at[d - 1, span],
            incoming.at[d - 1, span],
            ser_send.at[d - 1, 0],
            ser_recv.at[d - 1, 0],
            "freq",
            at_chip(d),
        )

    def send_last(d):
        span = pl.ds(HEAD, outgoing.shape[2] - HEAD)
        return remote(
            outgoing.at[d - 1, last, span],
            incoming.at[d - 1, last, span],
            ser_send.at[d - 1, 1],
            ser_recv.at[d - 1, 1],
            "freq",
            at_chip(d),
        )

    def pieces(c):
        for j in range(BLOCKS_PER_CHUNK):
            lanes = pl.ds(pl.multiple_of(c * width + j * LANE, LANE), LANE)
            yield j, slice(0, whole_rows), slice(j * whole_rows, (j + 1) * whole_rows), lanes
            if rest:
                first = BLOCKS_PER_CHUNK * whole_rows + j * rest
                yield j, slice(whole_rows, rows), slice(first, first + rest), lanes

    def exchange(
        spec_sem,
        swap_send,
        swap_recv,
        load_sem,
        tw_send,
        tw_recv,
        raw_send,
        raw_recv,
        pass_send,
        pass_recv,
        part_send,
        part_recv,
        aside_send,
        aside_recv,
        on_send,
        head_send,
        head_recv,
        wall_send,
        wall_recv,
        halo_send,
        halo_recv,
        go,
        seen,
        all_in,
    ):
        def load_spec(c):
            return pltpu.make_async_copy(
                spec_hbm.at[:, pl.ds(c * seg, seg), :],
                own_spec.at[c],
                spec_sem.at[1 if c >= summed else 0],
            )

        def loaded(first, count, sem):
            span = own_spec.at[pl.ds(first, count)]
            return pltpu.make_async_copy(span, span, spec_sem.at[sem])

        def swap(c):
            return remote(
                own_spec.at[c],
                peer_spec.at[c],
                swap_send.at[0],
                swap_recv.at[c // PAIR],
                "freq",
                partner,
            )

        def swapped(first, count):
            span = peer_spec.at[pl.ds(first, count)]
            return remote(span, span, swap_send.at[0], swap_recv.at[first // PAIR], "freq", partner)

        def send_tw(d):
            return remote(
                tw_hbm, tw_all.at[d - 1], tw_send.at[d - 1], tw_recv.at[d - 1], "freq", at_chip(-d)
            )

        def send_raw(d):
            return remote(
                spec_hbm.at[:, pl.ds(summed * seg, RAW * seg), :],
                raw.at[d - 1],
                raw_send.at[d - 1],
                raw_recv.at[d - 1],
                "freq",
                at_chip(d),
            )

        def send_raw_part(d, r):
            return remote(
                spec_hbm.at[:, pl.ds((summed + r) * seg, seg), :],
                raw.at[d - 1, :, pl.ds(r * seg, seg), :],
                raw_send.at[d - 1],
                raw_recv.at[d - 1],
                "freq",
                at_chip(d),
            )

        def send_raw_chunk(d, r):
            return remote(
                own_spec.at[summed + r],
                raw.at[d - 1, :, pl.ds(r * seg, seg), :],
                raw_send.at[d - 1],
                raw_recv.at[d - 1],
                "freq",
                at_chip(d),
            )

        def pass_raw(d):
            return remote(
                raw.at[d - 1],
                raw_peer.at[d - 1],
                pass_send.at[d - 1],
                pass_recv.at[d - 1],
                "freq",
                partner,
            )

        def send_part(d):
            return remote(
                part.at[d, :, pl.ds(0, summed * BLOCKS_PER_CHUNK), :],
                part_in.at[d - 1],
                part_send.at[d - 1],
                part_recv.at[d - 1],
                "freq",
                at_chip(d),
            )

        def detoured(d):
            return (me == 0) & ((chip + d) % ny == 0)

        def passes():
            return (me == 1 + core) & (chip == 0)

        def head(ref, d):
            return ref.at[d - 1, last, pl.ds(0, HEAD)]

        def send_head(d):
            return remote(
                head(outgoing, d),
                head(incoming, d),
                head_send.at[d - 1],
                head_recv.at[d - 1],
                "freq",
                at_chip(d),
            )

        def send_aside(d):
            pairs = (
                (part.at[d, :, pl.ds(0, summed * BLOCKS_PER_CHUNK), :], aside),
                (head(outgoing, d), aside_head),
            )
            return [
                pltpu.make_async_remote_copy(
                    src_ref=source,
                    dst_ref=target.at[d - 1],
                    send_sem=aside_send.at[d - 1, i],
                    recv_sem=aside_recv.at[d - 1, i],
                    device_id={"freq": at_chip(d), "mesh": 1 + core},
                    device_id_type=pl.DeviceIdType.MESH,
                )
                for i, (source, target) in enumerate(pairs)
            ]

        def send_on(d):
            pairs = (
                (aside.at[d - 1], part_in.at[d - 1], part_recv),
                (aside_head.at[d - 1], head(incoming, d), head_recv),
            )
            return [
                remote(source, target, on_send.at[d - 1, i], recv.at[d - 1], "mesh", 0)
                for i, (source, target, recv) in enumerate(pairs)
            ]

        def send_wall(o):
            mine = wall.at[:, pl.ds(pl.multiple_of(me * per, 8), per), :]
            return remote(mine, mine, wall_send.at[0], wall_recv.at[0], "mesh", peer(o))

        def walled():
            span = wall.at[:, pl.ds(0, (nm - 1) * per), :]
            return remote(span, span, wall_send.at[0], wall_recv.at[0], "mesh", peer(1))

        def send_halo1(side):
            first = 0 if side else 2 * (cell_rows - halo)
            return remote(
                wave.at[pl.ds(first, 2 * halo)],
                halo1.at[side],
                halo_send.at[side],
                halo_recv.at[side],
                "mesh",
                peer(-1 if side else 1),
            )

        def send_halo2(side):
            first = halo if side else cell_rows
            return remote(
                ext.at[pl.ds(first, halo)],
                halo2.at[side],
                halo_send.at[2 + side],
                halo_recv.at[2 + side],
                "mesh",
                peer(-1 if side else 1),
            )

        inside = (me > 0, me < nm - 1)

        def halo_each(copy, method):
            for side in range(2):
                there = inside[side] if method == "wait_recv" else inside[1 - side]
                pl.when(there)(getattr(copy(side), method))

        def columns(c):
            return pl.ds(pl.multiple_of(c * width, width), width)

        load_wave = pltpu.make_async_copy(wave_hbm, wave, load_sem.at[0])
        load_coup = pltpu.make_async_copy(coup_hbm, coup, load_sem.at[1])
        load_weights = pltpu.make_async_copy(
            weights_hbm, weights.at[:, pl.ds(0, LANE), :], load_sem.at[2]
        )
        load_tw = pltpu.make_async_copy(tw_hbm, tw_own, load_sem.at[3])
        load_basis = pltpu.make_async_copy(basis_hbm.at[freq], basis_own, load_sem.at[4])
        load_neigh = pltpu.make_async_copy(neigh_hbm, neigh_smem, load_sem.at[5])
        load_block = pltpu.make_async_copy(block_hbm, block_smem, load_sem.at[6])

        barrier = pltpu.get_barrier_semaphore()
        first_core, first_chip = core == 0, chip == 0
        other_core, other_chip = core == 1, chip != 0

        def signal(sem, axis, target):
            pl.semaphore_signal(
                sem, inc=1, device_id={axis: target}, device_id_type=pl.DeviceIdType.MESH
            )

        for d in range(1, ny):
            at_first = at_chip(d) < CORES

            @pl.when(first_core | jnp.logical_not(at_first))
            def _():
                signal(barrier, "freq", at_chip(d))

        @pl.when(other_core)
        def _():
            signal(barrier, "freq", partner)

        @pl.when(other_chip)
        def _():
            pl.semaphore_wait(barrier, jnp.where(first_core, ny, ny - 1))

            @pl.when(other_core)
            def _():
                signal(seen.at[chip - 1], "freq", 1)

            for d in range(1, ny):
                send_raw_part(d, 0).start()
                send_tw(d).start()
                for r in range(1, RAW):
                    send_raw_part(d, r).start()

        load_tw.start()
        for c in (*range(summed, chunks), *range(summed)):
            load_spec(c).start()
        load_basis.start()
        load_wave.start()
        load_neigh.start()
        load_block.start()

        @pl.when(first_chip)
        def _():
            @pl.when(first_core)
            def _():
                pl.semaphore_wait(barrier, ny)

            @pl.when(other_core)
            def _():
                for d in range(1, ny):
                    pl.semaphore_wait(seen.at[d - 1], 1)

            loaded(summed, RAW, 1).wait()
            for d in range(1, ny):
                send_tw(d).start()
                for r in range(RAW):
                    send_raw_chunk(d, r).start()

        @pl.when(first_core)
        def _():
            signal(go.at[0], "freq", partner)

        @pl.when(other_core)
        def _():
            pl.semaphore_wait(go.at[0], 1)

        loaded(0, summed, 0).wait()

        @pl.when(other_chip)
        def _():
            loaded(summed, RAW, 1).wait()

        for c in range(chunks):
            swap(c).start()

        @pl.when(other_core & first_chip)
        def _():
            for o in range(1, nm):
                signal(barrier, "mesh", peer(o))

        load_coup.start()
        load_weights.start()

        staged[...] = jnp.zeros_like(staged)
        folded[...] = jnp.zeros_like(folded)
        load_tw.wait()
        load_basis.wait()
        for d in range(ny):
            high, low = split(basis_own[d * rp : (d + 1) * rp, :])
            lhs_high[d * rb : d * rb + rp, :] = high
            lhs_low[d * rb : d * rb + rp, :] = low
        for d in range(1, ny):
            high, low = split(basis_own[m1 + (d - 1) * rp : m1 + d * rp, :])
            cross_high[d - 1, 0:rp, :] = high
            cross_low[d - 1, 0:rp, :] = low
        for d in range(2 * ny - 1):
            if 0 < d < ny:
                send_tw(d).wait_recv()
            folded[16 * d : 16 * d + 2, :] = jnp.dot(
                tw_all[d - 1] if 0 < d < ny else tw_own[...],
                basis_own[d * rp : d * rp + rows, :],
                precision=HIGHEST,
                preferred_element_type=F32,
            )
            high, low = split(folded[16 * d : 16 * (d + 1), :])
            if d < ny:
                lhs_high[d * rb + fb : (d + 1) * rb, :] = high
                lhs_low[d * rb + fb : (d + 1) * rb, :] = low
            else:
                cross_high[d - ny, fb:rb, :] = high
                cross_low[d - ny, fb:rb, :] = low

        own_rows = own_spec.reshape(chunks * coefs * seg, LANE)
        peer_rows = peer_spec.reshape(chunks * coefs * seg, LANE)
        far = max(ny - 1, 1)
        raw_rows = raw.reshape(far * RAW * coefs * seg, LANE)
        raw_peer_rows = raw_peer.reshape(far * RAW * coefs * seg, LANE)

        def stage(sources, first, step=seg):
            for p, source in enumerate(sources):
                for s in range(2):
                    for j in range(BLOCKS_PER_CHUNK):
                        piece = source[pl.ds(first + 2 * j + s, coefs, stride=step), :]
                        base = (p * 2 + s) * kp
                        staged[base : base + coefs, j * LANE : (j + 1) * LANE] = piece
            return split(staged[...])

        def product(high, low, s_high, s_low):
            return dot(high, s_high) + dot(low, s_high) + dot(high, s_low)

        def keep_part(c, total, d):
            for s in range(2):
                row = d * rb + fb + s
                for j in range(BLOCKS_PER_CHUNK):
                    part[d, s, pl.ds(c * BLOCKS_PER_CHUNK + j, 1), :] = total[
                        row : row + 1, j * LANE : (j + 1) * LANE
                    ]

        def summed_chunk(c, carry):
            @pl.when(c % PAIR == 0)
            def _():
                swapped(c, PAIR).wait_recv()

            s_high, s_low = stage((own_rows, peer_rows), c * (coefs * seg))
            total = product(lhs_high[...], lhs_low[...], s_high, s_low)
            series[:, columns(c)] = total[0:rows]
            keep_part(c, total, 0)
            for d in range(1, ny):
                keep_part(c, total, d)
                for j, take, put, _ in pieces(c):
                    outgoing[d - 1, c, put, :] = total[
                        d * rb + take.start : d * rb + take.stop, j * LANE : (j + 1) * LANE
                    ]
            return carry

        lax.fori_loop(0, summed, summed_chunk, 0)
        for d in range(1, ny):
            pl.when(jnp.logical_not(detoured(d)))(send_part(d).start)

        def send_chunk(c, carry):
            for d in range(1, ny):
                send_series(d, c, 1).start()
            return carry

        for d in range(1, ny):
            pl.when(jnp.logical_not(detoured(d)))(send_head(d).start)
        lax.fori_loop(0, last, send_chunk, 0)
        for d in range(1, ny):
            send_last(d).start()

        def raw_chunk(c, carry):
            @pl.when(c % PAIR == 0)
            def _():
                swapped(c, PAIR).wait_recv()

            s_high, s_low = stage((own_rows, peer_rows), c * (coefs * seg))
            total = product(lhs_high[0:rb, :], lhs_low[0:rb, :], s_high, s_low)
            series[:, columns(c)] = total[0:rows]
            keep_part(c, total, 0)
            return carry

        lax.fori_loop(summed, chunks, raw_chunk, 0)

        @pl.when(other_core & first_chip)
        def _():
            pl.semaphore_wait(barrier, nm - 1)
            for d in range(ny):
                signal(all_in.at[0], "freq", d * CORES)
                if d:
                    signal(all_in.at[0], "freq", d * CORES + 1)

        @pl.when(first_core | other_chip)
        def _():
            pl.semaphore_wait(all_in.at[0], 1)

        for d in range(1, ny):

            @pl.when(detoured(d))
            def _():
                for copy in send_aside(d):
                    copy.start()

        load_wave.wait()
        halo_each(send_halo1, "start")

        pitch = weights.shape[1]
        weight_rows = weights.reshape(groups * pitch, LANE)
        load_weights.wait()

        def line_up(t, carry):
            for i in range(4):
                f = t * 4 + i
                lined[pl.ds(pl.multiple_of(f * LANE, LANE), LANE), :] = weight_rows[
                    pl.ds(f, groups, stride=pitch), :
                ].T
            return carry

        lax.fori_loop(0, LANE // 4, line_up, 0)

        for d in range(1, ny):
            send_raw(d).wait_recv()
            pass_raw(d).start()

        wave_rows = 64

        def stage_current(b, carry):
            at = b * wave_rows
            ext[pl.ds(halo + at, wave_rows), :] = wave[pl.ds(2 * at + 1, wave_rows, stride=2), :]
            return carry

        lax.fori_loop(0, cell_rows // wave_rows, stage_current, 0)

        load_neigh.wait()
        load_block.wait()

        def gather():
            def tile(t, carry):
                for n in range(4):
                    for i in range(8):
                        u = t * 8 + i
                        gathered[n, pl.ds(u, 1), :] = ext[pl.ds(neigh_smem[n, u], 1), :]
                return carry

            lax.fori_loop(0, cell_rows // 8, tile, 0)

        def spread_of(at, center):
            total = jnp.zeros((wave_rows, LANE), F32)
            for n in range(4):
                factor = coup[pl.ds(4 * at + n, wave_rows, stride=4), :]
                total += factor * (gathered[n, pl.ds(at, wave_rows), :] - center)
            return total

        inside_low = (jnp.zeros((halo, LANE), jnp.int32) + me) > 0
        inside_high = (jnp.zeros((halo, LANE), jnp.int32) + me) < nm - 1

        halo_each(send_halo1, "wait_recv")
        ext[0:halo, :] = jnp.where(inside_low, halo1[0, pl.ds(1, halo, stride=2), :], 0.0)
        ext[halo + cell_rows :, :] = jnp.where(
            inside_high, halo1[1, pl.ds(1, halo, stride=2), :], 0.0
        )
        load_coup.wait()
        gather()

        def first_step(b, carry):
            at = b * wave_rows
            center = ext[pl.ds(halo + at, wave_rows), :]
            previous = wave[pl.ds(2 * at, wave_rows, stride=2), :]
            state[pl.ds(2 * at, wave_rows, stride=2), :] = (
                2.0 * center - previous + spread_of(at, center)
            )
            return carry

        lax.fori_loop(0, cell_rows // wave_rows, first_step, 0)

        for d in range(1, ny):
            pass_raw(d).wait_recv()
        for r in range(RAW):
            c = summed + r
            total = series[:, columns(c)]
            extra = None
            for d in range(1, ny):
                s_high, s_low = stage(
                    (raw_rows, raw_peer_rows), ((d - 1) * coefs * RAW + r) * seg, RAW * seg
                )
                cross = product(cross_high[d - 1], cross_low[d - 1], s_high, s_low)
                total += cross[0:rows]
                extra = cross[fb : fb + 2] if extra is None else extra + cross[fb : fb + 2]
            series[:, columns(c)] = total
            if extra is not None:
                for s in range(2):
                    for j in range(BLOCKS_PER_CHUNK):
                        at = pl.ds(c * BLOCKS_PER_CHUNK + j, 1)
                        part[0, s, at, :] = (
                            part[0, s, at, :] + extra[s : s + 1, j * LANE : (j + 1) * LANE]
                        )

        for d in range(1, ny):

            @pl.when(passes())
            def _():
                for copy in send_aside(d):
                    copy.wait_recv()
                for copy in send_on(d):
                    copy.start()

        for d in range(1, ny):
            send_part(d).wait_recv()
        first_blocks = summed * BLOCKS_PER_CHUNK
        base = pl.multiple_of(me * per, 8)
        for s in range(2):
            weighted = part[0, s, 0:first_blocks, :]
            for d in range(1, ny):
                weighted += part_in[d - 1, s]
            wall[s, pl.ds(base, first_blocks), :] = weighted
            wall[s, pl.ds(base + first_blocks, per - first_blocks), :] = part[0, s, first_blocks:, :]
        for o in range(1, nm):
            send_wall(o).start()
        walled().wait_recv()

        def pick(t, carry):
            for i in range(8):
                g = t * 8 + i
                block = block_smem[g]
                for s in range(2):
                    picked[s, pl.ds(g, 1), :] = wall[s, pl.ds(block, 1), :]
            return carry

        lax.fori_loop(0, groups // 8, pick, 0)
        for s in range(2):
            asked[s] = picked[s].T

        def interpolate(t, carry):
            faces = lined[pl.ds(pl.multiple_of(t * 8 * LANE, 8 * LANE), 8 * LANE), :]
            faces = faces.reshape(8, LANE, groups)
            for s in range(2):
                turned[s, pl.ds(pl.multiple_of(t * 8, 8), 8), :] = jnp.sum(
                    faces * asked[s][None], axis=1
                )
            return carry

        lax.fori_loop(0, LANE // 8, interpolate, 0)
        alive = lax.broadcasted_iota(jnp.int32, (groups, LANE), 0) < count_smem[0]
        push = [jnp.where(alive, turned[s].T, 0.0) for s in range(2)]

        top = pl.ds(0, groups, stride=2)
        state[top, :] = state[top, :] + push[0]

        def stage_stepped(b, carry):
            at = b * wave_rows
            ext[pl.ds(halo + at, wave_rows), :] = state[pl.ds(2 * at, wave_rows, stride=2), :]
            return carry

        lax.fori_loop(0, cell_rows // wave_rows, stage_stepped, 0)
        halo_each(send_halo2, "start")
        halo_each(send_halo2, "wait_recv")
        ext[0:halo, :] = jnp.where(inside_low, halo2[0], 0.0)
        ext[halo + cell_rows :, :] = jnp.where(inside_high, halo2[1], 0.0)
        gather()

        def second_step(b, carry):
            at = b * wave_rows
            center = ext[pl.ds(halo + at, wave_rows), :]
            previous = wave[pl.ds(2 * at + 1, wave_rows, stride=2), :]
            state[pl.ds(2 * at + 1, wave_rows, stride=2), :] = (
                2.0 * center - previous + spread_of(at, center)
            )
            return carry

        lax.fori_loop(0, cell_rows // wave_rows, second_step, 0)
        bottom = pl.ds(1, groups, stride=2)
        state[bottom, :] = state[bottom, :] + push[1]

        swapped(0, chunks).wait_send()
        walled().wait_send()
        for d in range(1, ny):
            send_raw(d).wait_send()
            pass_raw(d).wait_send()
            send_tw(d).wait_send()

            @pl.when(jnp.logical_not(detoured(d)))
            def _():
                send_part(d).wait_send()
                send_head(d).wait_send()

            @pl.when(detoured(d))
            def _():
                for copy in send_aside(d):
                    copy.wait_send()

            @pl.when(passes())
            def _():
                for copy in send_on(d):
                    copy.wait_send()

            send_head(d).wait_recv()
        halo_each(send_halo1, "wait_send")
        halo_each(send_halo2, "wait_send")

    dma = lambda *shape: pltpu.SemaphoreType.DMA(shape)
    regular = lambda *shape: pltpu.SemaphoreType.REGULAR(shape)
    far = max(ny - 1, 1)
    pl.run_scoped(
        exchange,
        dma(2),
        dma(1),
        dma(chunks // PAIR),
        dma(7),
        dma(far),
        dma(far),
        dma(far),
        dma(far),
        dma(far),
        dma(far),
        dma(far),
        dma(far),
        dma(far, 2),
        dma(far, 2),
        dma(far, 2),
        dma(far),
        dma(far),
        dma(1),
        dma(1),
        dma(4),
        dma(4),
        regular(1),
        regular(far),
        regular(1),
    )

    def finish(c, carry):
        for d in range(1, ny):
            for _, take, put, lanes in pieces(c):
                series[take, lanes] = series[take, lanes] + incoming[d - 1, c, put, :]
        return carry

    for d in range(1, ny):
        send_series(d, 0, last).wait_recv()
    lax.fori_loop(0, last, finish, 0)
    for d in range(1, ny):
        send_series(d, 0, last).wait_send()
        send_last(d).wait_send()
        send_last(d).wait_recv()
    finish(last, 0)


def store(series, state, series_hbm, state_hbm, sem):
    copies = [
        pltpu.make_async_copy(series, series_hbm, sem.at[0]),
        pltpu.make_async_copy(state, state_hbm, sem.at[1]),
    ]
    for copy in copies:
        copy.start()
    for copy in copies:
        copy.wait()


def chip_basis(ny, coefs, rows, horizon):
    kp, rp = pad(coefs, 8), pad(rows, 8)
    freq = np.arange(ny * CORES).reshape(-1, 1, 1, 1, 1, 1)
    d, r, p, s, k = np.indices((2 * ny - 1, rp, CORES, 2, kp), sparse=True)
    chip, core = freq // CORES, freq % CORES
    source = chip - np.where(d < ny, 0, d - ny + 1)
    window = ((chip + np.where(d < ny, d, 0)) % ny) * CORES + core
    wave_number = (source % ny * CORES + (core + p) % CORES) * coefs + k
    angle = ((window * rows + r) * wave_number) % horizon * (2.0 * math.pi / horizon)
    scale = np.where(wave_number == 0, 1.0, 2.0) / horizon
    value = np.where(s == 0, np.cos(angle), -np.sin(angle)) * scale
    value = np.where((r < rows) & (k < coefs), value, 0.0)
    return value.reshape(ny * CORES, (2 * ny - 1) * rp, CORES * 2 * kp).astype(np.float32)


def local(
    ny,
    nm,
    spectrum,
    time_weights,
    interp_weights,
    group_block,
    group_count,
    wave_state,
    neighbors,
    coupling,
):
    coefs, points = spectrum.shape[1:]
    rows = time_weights.shape[1]
    horizon = rows * ny * CORES
    groups = interp_weights.shape[0]
    cell_rows = neighbors.shape[1]
    halo = HALO_CELLS // LANE
    blocks = points // LANE
    chunks = blocks // BLOCKS_PER_CHUNK
    kp, rp = pad(coefs, 8), pad(rows, 8)
    k_all, rb = CORES * 2 * kp, pad(rows, 16) + 16
    summed = chunks - RAW
    seg = 2 * BLOCKS_PER_CHUNK
    width = BLOCKS_PER_CHUNK * LANE

    spec = spectrum.reshape(2, coefs, blocks, LANE).transpose(1, 2, 0, 3)
    spec = spec.reshape(coefs, 2 * blocks, LANE)
    wave = wave_state.reshape(2, cell_rows, LANE).transpose(1, 0, 2).reshape(2 * cell_rows, LANE)
    coup = coupling.reshape(4, cell_rows, LANE).transpose(1, 0, 2).reshape(4 * cell_rows, LANE)
    basis = jnp.asarray(chip_basis(ny, coefs, rows, horizon))

    vmem = lambda *shape: pltpu.VMEM(shape, F32)
    dma = lambda *shape: pltpu.SemaphoreType.DMA(shape)
    smem = pl.BlockSpec(memory_space=pltpu.SMEM)
    hbm = pl.BlockSpec(memory_space=pltpu.HBM)
    on_chip = pl.BlockSpec(memory_space=pltpu.VMEM)
    far = max(ny - 1, 1)
    pinned = [
        pltpu.with_memory_space_constraint(x, pltpu.HBM)
        for x in (
            group_block,
            neighbors,
            time_weights,
            basis,
            spec,
            interp_weights,
            wave,
            coup,
        )
    ]
    outs = (
        jax.ShapeDtypeStruct((rows, points), F32),
        jax.ShapeDtypeStruct((2 * cell_rows, LANE), F32),
    )
    series, state = pl.pallas_call(
        functools.partial(kernel, (ny, nm, coefs, rows, chunks)),
        out_shape=outs,
        in_specs=[smem] + [hbm] * 8,
        out_specs=(on_chip, on_chip),
        scratch_shapes=[
            pltpu.SMEM(group_block.shape, jnp.int32),
            pltpu.SMEM(neighbors.shape, jnp.int32),
            vmem(2, rows),
            vmem((2 * ny - 1) * rp, k_all),
            vmem(16 * (2 * ny - 1), k_all),
            vmem(chunks, coefs, seg, LANE),
            vmem(chunks, coefs, seg, LANE),
            vmem(k_all, width),
            pltpu.VMEM((ny * rb, k_all), BF16),
            pltpu.VMEM((ny * rb, k_all), BF16),
            pltpu.VMEM((far, rb, k_all), BF16),
            pltpu.VMEM((far, rb, k_all), BF16),
            vmem(far, coefs, RAW * seg, LANE),
            vmem(far, coefs, RAW * seg, LANE),
            vmem(far, 2, rows),
            vmem(far, summed, BLOCKS_PER_CHUNK * rows, LANE),
            vmem(far, summed, BLOCKS_PER_CHUNK * rows, LANE),
            vmem(ny, 2, blocks, LANE),
            vmem(far, 2, summed * BLOCKS_PER_CHUNK, LANE),
            vmem(far, 2, summed * BLOCKS_PER_CHUNK, LANE),
            vmem(far, HEAD, LANE),
            vmem(2, nm * blocks, LANE),
            vmem(2, groups, LANE),
            vmem(2, LANE, groups),
            vmem(2, LANE, groups),
            vmem(groups, LANE + 8, LANE),
            vmem(LANE * LANE, groups),
            vmem(2 * cell_rows, LANE),
            vmem(4 * cell_rows, LANE),
            vmem(2, 2 * halo, LANE),
            vmem(2, halo, LANE),
            vmem(cell_rows + 2 * halo, LANE),
            vmem(4, cell_rows, LANE),
            dma(far, 2),
            dma(far, 2),
        ],
        compiler_params=pltpu.CompilerParams(
            collective_id=0, has_side_effects=True, vmem_limit_bytes=50000 * 1024
        ),
        name="adjoint",
    )(group_count, *pinned)
    series, state = pl.pallas_call(
        store,
        out_shape=outs,
        in_specs=[pl.BlockSpec(memory_space=pl.ANY)] * 2,
        out_specs=(hbm, hbm),
        scratch_shapes=[dma(2)],
        compiler_params=pltpu.CompilerParams(vmem_limit_bytes=1024 * 1024),
        name="store",
    )(series, state)
    new_state = state.reshape(cell_rows, 2, LANE).transpose(1, 0, 2)
    return series, new_state.reshape(1, 2, cell_rows * LANE)


def solution(mesh):
    placed = (
        P(None, "freq", "mesh"),
        P(None, "freq"),
        P("mesh", None, None),
        P("mesh"),
        P("mesh"),
        P("freq", None, "mesh"),
        P(None, "mesh"),
        P(None, "mesh"),
    )
    ny = mesh.shape["freq"] // CORES
    return jax.shard_map(
        functools.partial(local, ny, mesh.shape["mesh"]),
        mesh=mesh,
        in_specs=placed,
        out_specs=(P("freq", "mesh"), P("freq", None, "mesh")),
        check_vma=False,
    )
```

```python
import functools
import math

import jax
import jax.numpy as jnp
import numpy as np
from jax import lax
from jax.experimental import pallas as pl
from jax.experimental.pallas import tpu as pltpu
from jax.sharding import PartitionSpec as P

LANE = 128
CORES = 2
HALO_CELLS = 4096
BLOCKS_PER_CHUNK = 4
RAW = 3
PAIR = 2
HEAD = 32
HIGHEST = lax.Precision.HIGHEST
F32 = jnp.float32
BF16 = jnp.bfloat16


def pad(n, to):
    return (n + to - 1) // to * to


def split(x):
    high = x.astype(BF16)
    return high, (x - high.astype(F32)).astype(BF16)


def dot(a, b):
    return jnp.dot(a, b, preferred_element_type=F32)


def kernel(
    dims,
    count_smem,
    block_hbm,
    neigh_hbm,
    tw_hbm,
    basis_hbm,
    spec_hbm,
    weights_hbm,
    wave_hbm,
    coup_hbm,
    series,
    state,
    block_smem,
    neigh_smem,
    tw_own,
    basis_own,
    folded,
    own_spec,
    peer_spec,
    staged,
    lhs_high,
    lhs_low,
    cross_high,
    cross_low,
    raw,
    raw_peer,
    tw_all,
    outgoing,
    incoming,
    part,
    part_in,
    aside,
    aside_head,
    wall,
    picked,
    asked,
    turned,
    weights,
    lined,
    wave,
    coup,
    halo1,
    halo2,
    ext,
    gathered,
    ser_send,
    ser_recv,
):
    ny, nm, coefs, rows, chunks = dims
    groups = weights.shape[0]
    kp, rp, fb = pad(coefs, 8), pad(rows, 8), pad(rows, 16)
    rb = fb + 16
    m1 = ny * rp
    per = part.shape[2]
    cell_rows = ext.shape[0] - 2 * halo1.shape[1] // 2
    halo = halo1.shape[1] // 2
    width = BLOCKS_PER_CHUNK * LANE
    seg = 2 * BLOCKS_PER_CHUNK
    summed = chunks - RAW
    whole_rows = rows // 8 * 8
    rest = rows - whole_rows

    freq = lax.axis_index("freq")
    me = lax.axis_index("mesh")
    chip, core = freq // CORES, freq % CORES
    partner = chip * CORES + (1 - core)

    def at_chip(d):
        return ((chip + d + ny) % ny) * CORES + core

    def peer(d):
        return (me + d + nm) % nm

    def remote(src, dst, send, recv, axis, target):
        return pltpu.make_async_remote_copy(
            src_ref=src,
            dst_ref=dst,
            send_sem=send,
            recv_sem=recv,
            device_id={axis: target},
            device_id_type=pl.DeviceIdType.MESH,
        )

    last = summed - 1

    def send_series(d, first, count):
        span = pl.ds(first, count)
        return remote(
            outgoing.at[d - 1, span],
            incoming.at[d - 1, span],
            ser_send.at[d - 1, 0],
            ser_recv.at[d - 1, 0],
            "freq",
            at_chip(d),
        )

    def send_last(d):
        span = pl.ds(HEAD, outgoing.shape[2] - HEAD)
        return remote(
            outgoing.at[d - 1, last, span],
            incoming.at[d - 1, last, span],
            ser_send.at[d - 1, 1],
            ser_recv.at[d - 1, 1],
            "freq",
            at_chip(d),
        )

    def pieces(c):
        for j in range(BLOCKS_PER_CHUNK):
            lanes = pl.ds(pl.multiple_of(c * width + j * LANE, LANE), LANE)
            yield j, slice(0, whole_rows), slice(j * whole_rows, (j + 1) * whole_rows), lanes
            if rest:
                first = BLOCKS_PER_CHUNK * whole_rows + j * rest
                yield j, slice(whole_rows, rows), slice(first, first + rest), lanes

    def exchange(
        spec_sem,
        swap_send,
        swap_recv,
        load_sem,
        tw_send,
        tw_recv,
        raw_send,
        raw_recv,
        pass_send,
        pass_recv,
        part_send,
        part_recv,
        aside_send,
        aside_recv,
        on_send,
        head_send,
        head_recv,
        wall_send,
        wall_recv,
        halo_send,
        halo_recv,
        go,
        seen,
        all_in,
    ):
        def load_spec(c):
            return pltpu.make_async_copy(
                spec_hbm.at[:, pl.ds(c * seg, seg), :],
                own_spec.at[c],
                spec_sem.at[1 if c >= summed else 0],
            )

        def loaded(first, count, sem):
            span = own_spec.at[pl.ds(first, count)]
            return pltpu.make_async_copy(span, span, spec_sem.at[sem])

        def swap(c):
            return remote(
                own_spec.at[c],
                peer_spec.at[c],
                swap_send.at[0],
                swap_recv.at[c // PAIR],
                "freq",
                partner,
            )

        def swapped(first, count):
            span = peer_spec.at[pl.ds(first, count)]
            return remote(span, span, swap_send.at[0], swap_recv.at[first // PAIR], "freq", partner)

        def send_tw(d):
            return remote(
                tw_hbm, tw_all.at[d - 1], tw_send.at[d - 1], tw_recv.at[d - 1], "freq", at_chip(-d)
            )

        def send_raw(d):
            return remote(
                spec_hbm.at[:, pl.ds(summed * seg, RAW * seg), :],
                raw.at[d - 1],
                raw_send.at[d - 1],
                raw_recv.at[d - 1],
                "freq",
                at_chip(d),
            )

        def send_raw_part(d, r):
            return remote(
                spec_hbm.at[:, pl.ds((summed + r) * seg, seg), :],
                raw.at[d - 1, :, pl.ds(r * seg, seg), :],
                raw_send.at[d - 1],
                raw_recv.at[d - 1],
                "freq",
                at_chip(d),
            )

        def send_raw_chunk(d, r):
            return remote(
                own_spec.at[summed + r],
                raw.at[d - 1, :, pl.ds(r * seg, seg), :],
                raw_send.at[d - 1],
                raw_recv.at[d - 1],
                "freq",
                at_chip(d),
            )

        def pass_raw(d):
            return remote(
                raw.at[d - 1],
                raw_peer.at[d - 1],
                pass_send.at[d - 1],
                pass_recv.at[d - 1],
                "freq",
                partner,
            )

        def send_part(d):
            return remote(
                part.at[d, :, pl.ds(0, summed * BLOCKS_PER_CHUNK), :],
                part_in.at[d - 1],
                part_send.at[d - 1],
                part_recv.at[d - 1],
                "freq",
                at_chip(d),
            )

        def detoured(d):
            return (me == 0) & ((chip + d) % ny == 0)

        def passes():
            return (me == 1 + core) & (chip == 0)

        def head(ref, d):
            return ref.at[d - 1, last, pl.ds(0, HEAD)]

        def send_head(d):
            return remote(
                head(outgoing, d),
                head(incoming, d),
                head_send.at[d - 1],
                head_recv.at[d - 1],
                "freq",
                at_chip(d),
            )

        def send_aside(d):
            pairs = (
                (part.at[d, :, pl.ds(0, summed * BLOCKS_PER_CHUNK), :], aside),
                (head(outgoing, d), aside_head),
            )
            return [
                pltpu.make_async_remote_copy(
                    src_ref=source,
                    dst_ref=target.at[d - 1],
                    send_sem=aside_send.at[d - 1, i],
                    recv_sem=aside_recv.at[d - 1, i],
                    device_id={"freq": at_chip(d), "mesh": 1 + core},
                    device_id_type=pl.DeviceIdType.MESH,
                )
                for i, (source, target) in enumerate(pairs)
            ]

        def send_on(d):
            pairs = (
                (aside.at[d - 1], part_in.at[d - 1], part_recv),
                (aside_head.at[d - 1], head(incoming, d), head_recv),
            )
            return [
                remote(source, target, on_send.at[d - 1, i], recv.at[d - 1], "mesh", 0)
                for i, (source, target, recv) in enumerate(pairs)
            ]

        def send_wall(o):
            mine = wall.at[:, pl.ds(pl.multiple_of(me * per, 8), per), :]
            return remote(mine, mine, wall_send.at[0], wall_recv.at[0], "mesh", peer(o))

        def walled():
            span = wall.at[:, pl.ds(0, (nm - 1) * per), :]
            return remote(span, span, wall_send.at[0], wall_recv.at[0], "mesh", peer(1))

        def send_halo1(side):
            first = 0 if side else 2 * (cell_rows - halo)
            return remote(
                wave.at[pl.ds(first, 2 * halo)],
                halo1.at[side],
                halo_send.at[side],
                halo_recv.at[side],
                "mesh",
                peer(-1 if side else 1),
            )

        def send_halo2(side):
            first = halo if side else cell_rows
            return remote(
                ext.at[pl.ds(first, halo)],
                halo2.at[side],
                halo_send.at[2 + side],
                halo_recv.at[2 + side],
                "mesh",
                peer(-1 if side else 1),
            )

        inside = (me > 0, me < nm - 1)

        def halo_each(copy, method):
            for side in range(2):
                there = inside[side] if method == "wait_recv" else inside[1 - side]
                pl.when(there)(getattr(copy(side), method))

        def columns(c):
            return pl.ds(pl.multiple_of(c * width, width), width)

        load_wave = pltpu.make_async_copy(wave_hbm, wave, load_sem.at[0])
        load_coup = pltpu.make_async_copy(coup_hbm, coup, load_sem.at[1])
        load_weights = pltpu.make_async_copy(
            weights_hbm, weights.at[:, pl.ds(0, LANE), :], load_sem.at[2]
        )
        load_tw = pltpu.make_async_copy(tw_hbm, tw_own, load_sem.at[3])
        load_basis = pltpu.make_async_copy(basis_hbm.at[freq], basis_own, load_sem.at[4])
        load_neigh = pltpu.make_async_copy(neigh_hbm, neigh_smem, load_sem.at[5])
        load_block = pltpu.make_async_copy(block_hbm, block_smem, load_sem.at[6])

        barrier = pltpu.get_barrier_semaphore()
        first_core, first_chip = core == 0, chip == 0
        other_core, other_chip = core == 1, chip != 0

        def signal(sem, axis, target):
            pl.semaphore_signal(
                sem, inc=1, device_id={axis: target}, device_id_type=pl.DeviceIdType.MESH
            )

        for d in range(1, ny):
            at_first = at_chip(d) < CORES

            @pl.when(first_core | jnp.logical_not(at_first))
            def _():
                signal(barrier, "freq", at_chip(d))

        @pl.when(other_core)
        def _():
            signal(barrier, "freq", partner)

        @pl.when(other_chip)
        def _():
            pl.semaphore_wait(barrier, jnp.where(first_core, ny, ny - 1))

            @pl.when(other_core)
            def _():
                signal(seen.at[chip - 1], "freq", 1)

            for d in range(1, ny):
                send_raw_part(d, 0).start()
                send_tw(d).start()
                for r in range(1, RAW):
                    send_raw_part(d, r).start()

        load_tw.start()
        for c in (*range(summed, chunks), *range(summed)):
            load_spec(c).start()
        load_basis.start()
        load_wave.start()
        load_neigh.start()
        load_block.start()

        @pl.when(first_chip)
        def _():
            @pl.when(first_core)
            def _():
                pl.semaphore_wait(barrier, ny)

            @pl.when(other_core)
            def _():
                for d in range(1, ny):
                    pl.semaphore_wait(seen.at[d - 1], 1)

            loaded(summed, RAW, 1).wait()
            for d in range(1, ny):
                send_tw(d).start()
                for r in range(RAW):
                    send_raw_chunk(d, r).start()

        @pl.when(first_core)
        def _():
            signal(go.at[0], "freq", partner)

        @pl.when(other_core)
        def _():
            pl.semaphore_wait(go.at[0], 1)

        loaded(0, summed, 0).wait()

        @pl.when(other_chip)
        def _():
            loaded(summed, RAW, 1).wait()

        for c in range(chunks):
            swap(c).start()

        @pl.when(other_core & first_chip)
        def _():
            for o in range(1, nm):
                signal(barrier, "mesh", peer(o))


        staged[...] = jnp.zeros_like(staged)
        folded[...] = jnp.zeros_like(folded)
        load_tw.wait()
        load_basis.wait()
        for d in range(ny):
            high, low = split(basis_own[d * rp : (d + 1) * rp, :])
            lhs_high[d * rb : d * rb + rp, :] = high
            lhs_low[d * rb : d * rb + rp, :] = low
        for d in range(1, ny):
            high, low = split(basis_own[m1 + (d - 1) * rp : m1 + d * rp, :])
            cross_high[d - 1, 0:rp, :] = high
            cross_low[d - 1, 0:rp, :] = low
        for d in range(2 * ny - 1):
            if 0 < d < ny:
                send_tw(d).wait_recv()
            folded[16 * d : 16 * d + 2, :] = jnp.dot(
                tw_all[d - 1] if 0 < d < ny else tw_own[...],
                basis_own[d * rp : d * rp + rows, :],
                precision=HIGHEST,
                preferred_element_type=F32,
            )
            high, low = split(folded[16 * d : 16 * (d + 1), :])
            if d < ny:
                lhs_high[d * rb + fb : (d + 1) * rb, :] = high
                lhs_low[d * rb + fb : (d + 1) * rb, :] = low
            else:
                cross_high[d - ny, fb:rb, :] = high
                cross_low[d - ny, fb:rb, :] = low

        own_rows = own_spec.reshape(chunks * coefs * seg, LANE)
        peer_rows = peer_spec.reshape(chunks * coefs * seg, LANE)
        far = max(ny - 1, 1)
        raw_rows = raw.reshape(far * RAW * coefs * seg, LANE)
        raw_peer_rows = raw_peer.reshape(far * RAW * coefs * seg, LANE)

        def stage(sources, first, step=seg):
            for p, source in enumerate(sources):
                for s in range(2):
                    for j in range(BLOCKS_PER_CHUNK):
                        piece = source[pl.ds(first + 2 * j + s, coefs, stride=step), :]
                        base = (p * 2 + s) * kp
                        staged[base : base + coefs, j * LANE : (j + 1) * LANE] = piece
            return split(staged[...])

        def product(high, low, s_high, s_low):
            return dot(high, s_high) + dot(low, s_high) + dot(high, s_low)

        def keep_part(c, total, d):
            for s in range(2):
                row = d * rb + fb + s
                for j in range(BLOCKS_PER_CHUNK):
                    part[d, s, pl.ds(c * BLOCKS_PER_CHUNK + j, 1), :] = total[
                        row : row + 1, j * LANE : (j + 1) * LANE
                    ]

        def summed_chunk(c, carry):
            @pl.when(c % PAIR == 0)
            def _():
                swapped(c, PAIR).wait_recv()

            s_high, s_low = stage((own_rows, peer_rows), c * (coefs * seg))
            total = product(lhs_high[...], lhs_low[...], s_high, s_low)
            series[:, columns(c)] = total[0:rows]
            keep_part(c, total, 0)
            for d in range(1, ny):
                keep_part(c, total, d)
                for j, take, put, _ in pieces(c):
                    outgoing[d - 1, c, put, :] = total[
                        d * rb + take.start : d * rb + take.stop, j * LANE : (j + 1) * LANE
                    ]
            return carry

        lax.fori_loop(0, summed, summed_chunk, 0)
        for d in range(1, ny):
            pl.when(jnp.logical_not(detoured(d)))(send_part(d).start)

        def send_chunk(c, carry):
            for d in range(1, ny):
                send_series(d, c, 1).start()
            return carry

        for d in range(1, ny):
            pl.when(jnp.logical_not(detoured(d)))(send_head(d).start)
        lax.fori_loop(0, last, send_chunk, 0)
        for d in range(1, ny):
            send_last(d).start()

        load_weights.start()
        load_coup.start()

        def raw_chunk(c, carry):
            @pl.when(c % PAIR == 0)
            def _():
                swapped(c, PAIR).wait_recv()

            s_high, s_low = stage((own_rows, peer_rows), c * (coefs * seg))
            total = product(lhs_high[0:rb, :], lhs_low[0:rb, :], s_high, s_low)
            series[:, columns(c)] = total[0:rows]
            keep_part(c, total, 0)
            return carry

        lax.fori_loop(summed, chunks, raw_chunk, 0)

        @pl.when(other_core & first_chip)
        def _():
            pl.semaphore_wait(barrier, nm - 1)
            for d in range(ny):
                signal(all_in.at[0], "freq", d * CORES)
                if d:
                    signal(all_in.at[0], "freq", d * CORES + 1)

        @pl.when(first_core | other_chip)
        def _():
            pl.semaphore_wait(all_in.at[0], 1)

        for d in range(1, ny):

            @pl.when(detoured(d))
            def _():
                for copy in send_aside(d):
                    copy.start()

        load_wave.wait()
        halo_each(send_halo1, "start")

        pitch = weights.shape[1]
        weight_rows = weights.reshape(groups * pitch, LANE)
        load_weights.wait()

        def line_up(t, carry):
            for i in range(4):
                f = t * 4 + i
                lined[pl.ds(pl.multiple_of(f * LANE, LANE), LANE), :] = weight_rows[
                    pl.ds(f, groups, stride=pitch), :
                ].T
            return carry

        lax.fori_loop(0, LANE // 4, line_up, 0)

        for d in range(1, ny):
            send_raw(d).wait_recv()
            pass_raw(d).start()

        wave_rows = 64

        def stage_current(b, carry):
            at = b * wave_rows
            ext[pl.ds(halo + at, wave_rows), :] = wave[pl.ds(2 * at + 1, wave_rows, stride=2), :]
            return carry

        lax.fori_loop(0, cell_rows // wave_rows, stage_current, 0)

        load_neigh.wait()
        load_block.wait()

        def gather():
            def tile(t, carry):
                for n in range(4):
                    for i in range(8):
                        u = t * 8 + i
                        gathered[n, pl.ds(u, 1), :] = ext[pl.ds(neigh_smem[n, u], 1), :]
                return carry

            lax.fori_loop(0, cell_rows // 8, tile, 0)

        def spread_of(at, center):
            total = jnp.zeros((wave_rows, LANE), F32)
            for n in range(4):
                factor = coup[pl.ds(4 * at + n, wave_rows, stride=4), :]
                total += factor * (gathered[n, pl.ds(at, wave_rows), :] - center)
            return total

        inside_low = (jnp.zeros((halo, LANE), jnp.int32) + me) > 0
        inside_high = (jnp.zeros((halo, LANE), jnp.int32) + me) < nm - 1

        halo_each(send_halo1, "wait_recv")
        ext[0:halo, :] = jnp.where(inside_low, halo1[0, pl.ds(1, halo, stride=2), :], 0.0)
        ext[halo + cell_rows :, :] = jnp.where(
            inside_high, halo1[1, pl.ds(1, halo, stride=2), :], 0.0
        )
        load_coup.wait()
        gather()

        def first_step(b, carry):
            at = b * wave_rows
            center = ext[pl.ds(halo + at, wave_rows), :]
            previous = wave[pl.ds(2 * at, wave_rows, stride=2), :]
            state[pl.ds(2 * at, wave_rows, stride=2), :] = (
                2.0 * center - previous + spread_of(at, center)
            )
            return carry

        lax.fori_loop(0, cell_rows // wave_rows, first_step, 0)

        for d in range(1, ny):
            pass_raw(d).wait_recv()
        for r in range(RAW):
            c = summed + r
            total = series[:, columns(c)]
            extra = None
            for d in range(1, ny):
                s_high, s_low = stage(
                    (raw_rows, raw_peer_rows), ((d - 1) * coefs * RAW + r) * seg, RAW * seg
                )
                cross = product(cross_high[d - 1], cross_low[d - 1], s_high, s_low)
                total += cross[0:rows]
                extra = cross[fb : fb + 2] if extra is None else extra + cross[fb : fb + 2]
            series[:, columns(c)] = total
            if extra is not None:
                for s in range(2):
                    for j in range(BLOCKS_PER_CHUNK):
                        at = pl.ds(c * BLOCKS_PER_CHUNK + j, 1)
                        part[0, s, at, :] = (
                            part[0, s, at, :] + extra[s : s + 1, j * LANE : (j + 1) * LANE]
                        )

        for d in range(1, ny):

            @pl.when(passes())
            def _():
                for copy in send_aside(d):
                    copy.wait_recv()
                for copy in send_on(d):
                    copy.start()

        for d in range(1, ny):
            send_part(d).wait_recv()
        first_blocks = summed * BLOCKS_PER_CHUNK
        base = pl.multiple_of(me * per, 8)
        for s in range(2):
            weighted = part[0, s, 0:first_blocks, :]
            for d in range(1, ny):
                weighted += part_in[d - 1, s]
            wall[s, pl.ds(base, first_blocks), :] = weighted
            wall[s, pl.ds(base + first_blocks, per - first_blocks), :] = part[0, s, first_blocks:, :]
        for o in range(1, nm):
            send_wall(o).start()
        walled().wait_recv()

        def pick(t, carry):
            for i in range(8):
                g = t * 8 + i
                block = block_smem[g]
                for s in range(2):
                    picked[s, pl.ds(g, 1), :] = wall[s, pl.ds(block, 1), :]
            return carry

        lax.fori_loop(0, groups // 8, pick, 0)
        for s in range(2):
            asked[s] = picked[s].T

        def interpolate(t, carry):
            faces = lined[pl.ds(pl.multiple_of(t * 8 * LANE, 8 * LANE), 8 * LANE), :]
            faces = faces.reshape(8, LANE, groups)
            for s in range(2):
                turned[s, pl.ds(pl.multiple_of(t * 8, 8), 8), :] = jnp.sum(
                    faces * asked[s][None], axis=1
                )
            return carry

        lax.fori_loop(0, LANE // 8, interpolate, 0)
        alive = lax.broadcasted_iota(jnp.int32, (groups, LANE), 0) < count_smem[0]
        push = [jnp.where(alive, turned[s].T, 0.0) for s in range(2)]

        top = pl.ds(0, groups, stride=2)
        state[top, :] = state[top, :] + push[0]

        def stage_stepped(b, carry):
            at = b * wave_rows
            ext[pl.ds(halo + at, wave_rows), :] = state[pl.ds(2 * at, wave_rows, stride=2), :]
            return carry

        lax.fori_loop(0, cell_rows // wave_rows, stage_stepped, 0)
        halo_each(send_halo2, "start")
        halo_each(send_halo2, "wait_recv")
        ext[0:halo, :] = jnp.where(inside_low, halo2[0], 0.0)
        ext[halo + cell_rows :, :] = jnp.where(inside_high, halo2[1], 0.0)
        gather()

        def second_step(b, carry):
            at = b * wave_rows
            center = ext[pl.ds(halo + at, wave_rows), :]
            previous = wave[pl.ds(2 * at + 1, wave_rows, stride=2), :]
            state[pl.ds(2 * at + 1, wave_rows, stride=2), :] = (
                2.0 * center - previous + spread_of(at, center)
            )
            return carry

        lax.fori_loop(0, cell_rows // wave_rows, second_step, 0)
        bottom = pl.ds(1, groups, stride=2)
        state[bottom, :] = state[bottom, :] + push[1]

        swapped(0, chunks).wait_send()
        walled().wait_send()
        for d in range(1, ny):
            send_raw(d).wait_send()
            pass_raw(d).wait_send()
            send_tw(d).wait_send()

            @pl.when(jnp.logical_not(detoured(d)))
            def _():
                send_part(d).wait_send()
                send_head(d).wait_send()

            @pl.when(detoured(d))
            def _():
                for copy in send_aside(d):
                    copy.wait_send()

            @pl.when(passes())
            def _():
                for copy in send_on(d):
                    copy.wait_send()

            send_head(d).wait_recv()
        halo_each(send_halo1, "wait_send")
        halo_each(send_halo2, "wait_send")

    dma = lambda *shape: pltpu.SemaphoreType.DMA(shape)
    regular = lambda *shape: pltpu.SemaphoreType.REGULAR(shape)
    far = max(ny - 1, 1)
    pl.run_scoped(
        exchange,
        dma(2),
        dma(1),
        dma(chunks // PAIR),
        dma(7),
        dma(far),
        dma(far),
        dma(far),
        dma(far),
        dma(far),
        dma(far),
        dma(far),
        dma(far),
        dma(far, 2),
        dma(far, 2),
        dma(far, 2),
        dma(far),
        dma(far),
        dma(1),
        dma(1),
        dma(4),
        dma(4),
        regular(1),
        regular(far),
        regular(1),
    )

    def finish(c, carry):
        for d in range(1, ny):
            for _, take, put, lanes in pieces(c):
                series[take, lanes] = series[take, lanes] + incoming[d - 1, c, put, :]
        return carry

    for d in range(1, ny):
        send_series(d, 0, last).wait_recv()
    lax.fori_loop(0, last, finish, 0)
    for d in range(1, ny):
        send_series(d, 0, last).wait_send()
        send_last(d).wait_send()
        send_last(d).wait_recv()
    finish(last, 0)


def store(series, state, series_hbm, state_hbm, sem):
    copies = [
        pltpu.make_async_copy(series, series_hbm, sem.at[0]),
        pltpu.make_async_copy(state, state_hbm, sem.at[1]),
    ]
    for copy in copies:
        copy.start()
    for copy in copies:
        copy.wait()


def chip_basis(ny, coefs, rows, horizon):
    kp, rp = pad(coefs, 8), pad(rows, 8)
    freq = np.arange(ny * CORES).reshape(-1, 1, 1, 1, 1, 1)
    d, r, p, s, k = np.indices((2 * ny - 1, rp, CORES, 2, kp), sparse=True)
    chip, core = freq // CORES, freq % CORES
    source = chip - np.where(d < ny, 0, d - ny + 1)
    window = ((chip + np.where(d < ny, d, 0)) % ny) * CORES + core
    wave_number = (source % ny * CORES + (core + p) % CORES) * coefs + k
    angle = ((window * rows + r) * wave_number) % horizon * (2.0 * math.pi / horizon)
    scale = np.where(wave_number == 0, 1.0, 2.0) / horizon
    value = np.where(s == 0, np.cos(angle), -np.sin(angle)) * scale
    value = np.where((r < rows) & (k < coefs), value, 0.0)
    return value.reshape(ny * CORES, (2 * ny - 1) * rp, CORES * 2 * kp).astype(np.float32)


def local(
    ny,
    nm,
    spectrum,
    time_weights,
    interp_weights,
    group_block,
    group_count,
    wave_state,
    neighbors,
    coupling,
):
    coefs, points = spectrum.shape[1:]
    rows = time_weights.shape[1]
    horizon = rows * ny * CORES
    groups = interp_weights.shape[0]
    cell_rows = neighbors.shape[1]
    halo = HALO_CELLS // LANE
    blocks = points // LANE
    chunks = blocks // BLOCKS_PER_CHUNK
    kp, rp = pad(coefs, 8), pad(rows, 8)
    k_all, rb = CORES * 2 * kp, pad(rows, 16) + 16
    summed = chunks - RAW
    seg = 2 * BLOCKS_PER_CHUNK
    width = BLOCKS_PER_CHUNK * LANE

    spec = spectrum.reshape(2, coefs, blocks, LANE).transpose(1, 2, 0, 3)
    spec = spec.reshape(coefs, 2 * blocks, LANE)
    wave = wave_state.reshape(2, cell_rows, LANE).transpose(1, 0, 2).reshape(2 * cell_rows, LANE)
    coup = coupling.reshape(4, cell_rows, LANE).transpose(1, 0, 2).reshape(4 * cell_rows, LANE)
    basis = jnp.asarray(chip_basis(ny, coefs, rows, horizon))

    vmem = lambda *shape: pltpu.VMEM(shape, F32)
    dma = lambda *shape: pltpu.SemaphoreType.DMA(shape)
    smem = pl.BlockSpec(memory_space=pltpu.SMEM)
    hbm = pl.BlockSpec(memory_space=pltpu.HBM)
    on_chip = pl.BlockSpec(memory_space=pltpu.VMEM)
    far = max(ny - 1, 1)
    pinned = [
        pltpu.with_memory_space_constraint(x, pltpu.HBM)
        for x in (
            group_block,
            neighbors,
            time_weights,
            basis,
            spec,
            interp_weights,
            wave,
            coup,
        )
    ]
    outs = (
        jax.ShapeDtypeStruct((rows, points), F32),
        jax.ShapeDtypeStruct((2 * cell_rows, LANE), F32),
    )
    series, state = pl.pallas_call(
        functools.partial(kernel, (ny, nm, coefs, rows, chunks)),
        out_shape=outs,
        in_specs=[smem] + [hbm] * 8,
        out_specs=(on_chip, on_chip),
        scratch_shapes=[
            pltpu.SMEM(group_block.shape, jnp.int32),
            pltpu.SMEM(neighbors.shape, jnp.int32),
            vmem(2, rows),
            vmem((2 * ny - 1) * rp, k_all),
            vmem(16 * (2 * ny - 1), k_all),
            vmem(chunks, coefs, seg, LANE),
            vmem(chunks, coefs, seg, LANE),
            vmem(k_all, width),
            pltpu.VMEM((ny * rb, k_all), BF16),
            pltpu.VMEM((ny * rb, k_all), BF16),
            pltpu.VMEM((far, rb, k_all), BF16),
            pltpu.VMEM((far, rb, k_all), BF16),
            vmem(far, coefs, RAW * seg, LANE),
            vmem(far, coefs, RAW * seg, LANE),
            vmem(far, 2, rows),
            vmem(far, summed, BLOCKS_PER_CHUNK * rows, LANE),
            vmem(far, summed, BLOCKS_PER_CHUNK * rows, LANE),
            vmem(ny, 2, blocks, LANE),
            vmem(far, 2, summed * BLOCKS_PER_CHUNK, LANE),
            vmem(far, 2, summed * BLOCKS_PER_CHUNK, LANE),
            vmem(far, HEAD, LANE),
            vmem(2, nm * blocks, LANE),
            vmem(2, groups, LANE),
            vmem(2, LANE, groups),
            vmem(2, LANE, groups),
            vmem(groups, LANE + 8, LANE),
            vmem(LANE * LANE, groups),
            vmem(2 * cell_rows, LANE),
            vmem(4 * cell_rows, LANE),
            vmem(2, 2 * halo, LANE),
            vmem(2, halo, LANE),
            vmem(cell_rows + 2 * halo, LANE),
            vmem(4, cell_rows, LANE),
            dma(far, 2),
            dma(far, 2),
        ],
        compiler_params=pltpu.CompilerParams(
            collective_id=0, has_side_effects=True, vmem_limit_bytes=50000 * 1024
        ),
        name="adjoint",
    )(group_count, *pinned)
    series, state = pl.pallas_call(
        store,
        out_shape=outs,
        in_specs=[pl.BlockSpec(memory_space=pl.ANY)] * 2,
        out_specs=(hbm, hbm),
        scratch_shapes=[dma(2)],
        compiler_params=pltpu.CompilerParams(vmem_limit_bytes=1024 * 1024),
        name="store",
    )(series, state)
    new_state = state.reshape(cell_rows, 2, LANE).transpose(1, 0, 2)
    return series, new_state.reshape(1, 2, cell_rows * LANE)


def solution(mesh):
    placed = (
        P(None, "freq", "mesh"),
        P(None, "freq"),
        P("mesh", None, None),
        P("mesh"),
        P("mesh"),
        P("freq", None, "mesh"),
        P(None, "mesh"),
        P(None, "mesh"),
    )
    ny = mesh.shape["freq"] // CORES
    return jax.shard_map(
        functools.partial(local, ny, mesh.shape["mesh"]),
        mesh=mesh,
        in_specs=placed,
        out_specs=(P("freq", "mesh"), P("freq", None, "mesh")),
        check_vma=False,
    )
```
